32 devices in a mesh: dp: 8 (over z, core), fsdp: 4 (over y, x).
Axes of the slice: x: 2, y: 2, z: 4, core: 2. Of those that a mesh axis runs over, the one named last changes fastest.
Arguments:
- tokens: bfloat16 [8192, 1024], P(('dp', 'fsdp')), may hold values from -6 to 6
- cotangent: bfloat16 [8192, 1024], P(('dp', 'fsdp')), may hold values from -6 to 6
- seq_lengths: int32 [32], replicated, may hold values from 1 to 256, 5120 in all
- seq_device: int32 [32], replicated, may hold values from 0 to 31, each once
- step_count: int32 [1], replicated, may hold values from 1 to 20
- attend_in: float32 [2, 1024, 3072], P(None, ('dp', 'fsdp'))
- attend_out: float32 [2, 1024, 1024], P(None, ('dp', 'fsdp')), may hold values from -0.75 to 0.75
- expand_weight: float32 [2, 1024, 4096], P(None, ('dp', 'fsdp')), may hold values from -0.1875 to 0.1875
- reduce_weight: float32 [2, 1024, 4096], P(None, ('dp', 'fsdp')), may hold values from -0.09375 to 0.09375
- layer_vectors: float32 [2, 13312], P(None, ('dp', 'fsdp'))
- attend_in_mean: float32 [2, 1024, 3072], P(None, ('dp', 'fsdp')), may hold values from -28 to 28
- attend_out_mean: float32 [2, 1024, 1024], P(None, ('dp', 'fsdp')), may hold values from -28 to 28
- expand_mean: float32 [2, 1024, 4096], P(None, ('dp', 'fsdp')), may hold values from -28 to 28
- reduce_mean: float32 [2, 1024, 4096], P(None, ('dp', 'fsdp')), may hold values from -28 to 28
- vectors_mean: float32 [2, 13312], P(None, ('dp', 'fsdp')), may hold values from -28 to 28
- attend_in_square: float32 [2, 1024, 3072], P(None, ('dp', 'fsdp')), may hold values from 16.384 to 245.76
- attend_out_square: float32 [2, 1024, 1024], P(None, ('dp', 'fsdp')), may hold values from 16.384 to 245.76
- expand_square: float32 [2, 1024, 4096], P(None, ('dp', 'fsdp')), may hold values from 16.384 to 245.76
- reduce_square: float32 [2, 1024, 4096], P(None, ('dp', 'fsdp')), may hold values from 16.384 to 245.76
- vectors_square: float32 [2, 13312], P(None, ('dp', 'fsdp')), may hold values from 819.2 to 16384
Outputs:
- hidden_states: bfloat16 [2, 8192, 1024], P(None, ('dp', 'fsdp'))
- input_grad: bfloat16 [8192, 1024], P(('dp', 'fsdp'))
- attend_in_grad: float32 [2, 1024, 3072], P(None, ('dp', 'fsdp'))
- attend_out_grad: float32 [2, 1024, 1024], P(None, ('dp', 'fsdp'))
- expand_grad: float32 [2, 1024, 4096], P(None, ('dp', 'fsdp'))
- reduce_grad: float32 [2, 1024, 4096], P(None, ('dp', 'fsdp'))
- vectors_grad: float32 [2, 13312], P(None, ('dp', 'fsdp'))
- attend_in_step: float32 [2, 1024, 3072], P(None, ('dp', 'fsdp'))
- attend_out_step: float32 [2, 1024, 1024], P(None, ('dp', 'fsdp'))
- expand_step: float32 [2, 1024, 4096], P(None, ('dp', 'fsdp'))
- reduce_step: float32 [2, 1024, 4096], P(None, ('dp', 'fsdp'))
- vectors_step: float32 [2, 13312], P(None, ('dp', 'fsdp'))
- attend_in_mean_new: float32 [2, 1024, 3072], P(None, ('dp', 'fsdp'))
- attend_out_mean_new: float32 [2, 1024, 1024], P(None, ('dp', 'fsdp'))
- expand_mean_new: float32 [2, 1024, 4096], P(None, ('dp', 'fsdp'))
- reduce_mean_new: float32 [2, 1024, 4096], P(None, ('dp', 'fsdp'))
- vectors_mean_new: float32 [2, 13312], P(None, ('dp', 'fsdp'))
- attend_in_square_new: float32 [2, 1024, 3072], P(None, ('dp', 'fsdp'))
- attend_out_square_new: float32 [2, 1024, 1024], P(None, ('dp', 'fsdp'))
- expand_square_new: float32 [2, 1024, 4096], P(None, ('dp', 'fsdp'))
- reduce_square_new: float32 [2, 1024, 4096], P(None, ('dp', 'fsdp'))
- vectors_square_new: float32 [2, 13312], P(None, ('dp', 'fsdp'))
The draws below stay inside these ranges and needn't reach their ends.
Inputs may be any that keep to these rules, and one draw needn't show every extreme that they name: `seq_device`: each device is dealt exactly one sequence. `seq_lengths`: the lengths add up to 32 * 256 * 5 // 8 and the longest has exactly 256.
All inputs are finite; a program needn't handle non-finite values.
Results may differ from the reference program's by a relative error of at most 0.02.
Values may be sent and summed in bfloat16 or wider, within the bound.
A program may use at most 256 MiB of HBM per device.

```python
import math
import jax
import jax.numpy as jnp
import numpy as np
from jax import lax

D = 1024
HEADS = 16
FF = 4096
HEAD_DIM = 64
ROT_DIM = 16
VEC = 13312
LAYERS = 2
ROWS_DEV = 256
TOKENS = 8192
DEVICES = 32


def draw_attend_in(key, part):
    return jax.random.truncated_normal(key, -4.0, 4.0, (LAYERS, D, 3 * D), jnp.float32) * D ** (-0.5)


def draw_layer_vectors(key, part):
    gain_key, shift_key = jax.random.split(key, 2)
    position = jnp.arange(9 * D + FF)
    gain_mask = (position < D) | (position >= 2 * D) & (position < 3 * D)
    gains = jax.random.uniform(gain_key, (LAYERS, 9 * D + FF), jnp.float32, 0.5, 1.5)
    shifts = jax.random.truncated_normal(shift_key, -4.0, 4.0, (LAYERS, 9 * D + FF), jnp.float32) * 0.3
    return jnp.where(gain_mask[None, :], gains, shifts)


def with_spikes(entries, key, source, target, shards_of, factor):
    def block_of(dim):
        return (jnp.arange(entries.shape[dim]) // (entries.shape[dim] // shards_of)).reshape((-1,) + (1,) * (entries.ndim - 1 - dim))

    first = jax.random.permutation(key, shards_of)[block_of(target)]
    second = (block_of(target) + shards_of // 2) % shards_of
    return jnp.where((block_of(source) == first) | (block_of(source) == second), factor * entries, entries)


def steps_of(key, shape, cuts, least, top_value):
    level = 1.0
    for dim, shards_of in cuts:
        draws = jax.random.uniform(jax.random.fold_in(jax.random.fold_in(key, 6), dim), (shards_of,), jnp.float32, least / len(cuts), top_value / len(cuts))
        level = level * jnp.repeat(jnp.exp(draws), shape[dim] // shards_of).reshape((-1,) + (1,) * (len(shape) - 1 - dim))
    return level


def profile(amount, total, bound, slope):
    weights = [(1 << 20) // math.isqrt(rank ** slope) + 1 for rank in range(2, amount + 1)]
    rest, holding = total - bound - (amount - 1), [1] * (amount - 1)
    while rest > 0:
        movable = [i for i in range(amount - 1) if holding[i] < bound]
        whole, left = sum([weights[i] for i in movable]), rest
        for i in movable:
            extra = min(bound - holding[i], max(1, left * weights[i] // whole), rest)
            holding[i] = holding[i] + extra
            rest = rest - extra
    return np.array([bound] + holding)


def uneven(stream_key, count, total, reach, slope):
    if count == 2:
        one = jax.random.randint(stream_key, (), max(1, total - reach), min(reach, total - 1) + 1)
        return jnp.stack([one, total - one])
    lengths = jnp.asarray(profile(count, total, reach, slope), jnp.int32)
    twos = (count - 1) // 2
    giver, taker = lengths[1:1 + 2 * twos:2], lengths[2:2 + 2 * twos:2]
    slack = jnp.minimum(giver - 1, reach - taker)
    moved = jax.random.randint(jax.random.fold_in(stream_key, 1), (twos,), 0, 1 << 20) % (slack + 1)
    lengths = lengths.at[1:1 + 2 * twos:2].set(giver - moved).at[2:2 + 2 * twos:2].set(taker + moved)
    return lengths[jax.random.permutation(jax.random.fold_in(stream_key, 2), count)]


def bell_draw(key, dims, scale, reach, cuts=(), kind=jnp.bfloat16):
    factor_of = steps_of(key, dims, cuts, -0.22, 0.18) if cuts else 1.0
    entries = jax.random.normal(key, dims, jnp.float32) * scale * factor_of
    return jnp.minimum(jnp.maximum(entries, -reach), reach).astype(kind)


def heavy_noise(own_key, extent, scale, bound, cuts, heavy, kind=jnp.bfloat16):
    entries = scale * jax.random.normal(own_key, extent, jnp.float32)
    if cuts:
        entries = entries * steps_of(own_key, extent, cuts, -0.22, 0.18)
    return jnp.clip(with_spikes(entries, jax.random.fold_in(own_key, 3), *heavy), -bound, bound).astype(kind)


def setup_inputs(seed: int = 0) -> dict:
    key_of = jax.random.split(jax.random.key(seed), 21)
    return {
        "tokens": bell_draw(key_of[0], (TOKENS, D), 1.0, 6.0, ((0, 32),)),
        "cotangent": heavy_noise(key_of[1], (TOKENS, D), 1.0, 6.0, ((0, 32),), (0, 1, 32, 2.75)),
        "seq_lengths": uneven(key_of[2], DEVICES, DEVICES * ROWS_DEV * 5 // 8, ROWS_DEV, 1).astype(jnp.int32),
        "seq_device": jax.random.permutation(key_of[3], DEVICES).astype(jnp.int32),
        "step_count": jax.random.randint(key_of[4], (1,), 1, 21).astype(jnp.int32),
        "attend_in": draw_attend_in(jax.random.fold_in(key_of[20], 71), 0),
        "attend_out": bell_draw(key_of[6], (LAYERS, D, D), (D // 16) ** -0.5, 0.75, ((1, 32),), jnp.float32),
        "expand_weight": bell_draw(key_of[7], (LAYERS, D, FF), D ** -0.5, 0.1875, ((1, 32),), jnp.float32),
        "reduce_weight": bell_draw(key_of[8], (LAYERS, D, FF), FF ** -0.5, 0.09375, ((1, 32),), jnp.float32),
        "layer_vectors": draw_layer_vectors(jax.random.fold_in(key_of[20], 71), 0),
        "attend_in_mean": bell_draw(key_of[10], (LAYERS, D, 3 * D), (0.05 * TOKENS ** 0.5), 28.0, ((1, 32),), jnp.float32),
        "attend_out_mean": bell_draw(key_of[11], (LAYERS, D, D), (0.05 * TOKENS ** 0.5), 28.0, ((1, 32),), jnp.float32),
        "expand_mean": bell_draw(key_of[12], (LAYERS, D, FF), (0.05 * TOKENS ** 0.5), 28.0, ((1, 32),), jnp.float32),
        "reduce_mean": bell_draw(key_of[13], (LAYERS, D, FF), (0.05 * TOKENS ** 0.5), 28.0, ((1, 32),), jnp.float32),
        "vectors_mean": bell_draw(key_of[14], (LAYERS, VEC), (0.05 * TOKENS ** 0.5), 28.0, ((1, 32),), jnp.float32),
        "attend_in_square": jnp.clip(jnp.exp(math.log(245.76) - 2.70805 * jax.random.uniform(key_of[15], (LAYERS, D, 3 * D), jnp.float32) ** steps_of(key_of[15], (LAYERS, D, 3 * D), ((1, 32),), -0.2, 0.2)), 16.384, 245.76),
        "attend_out_square": jnp.clip(jnp.exp(math.log(245.76) - 2.70805 * jax.random.uniform(key_of[16], (LAYERS, D, D), jnp.float32) ** steps_of(key_of[16], (LAYERS, D, D), ((1, 32),), -0.2, 0.2)), 16.384, 245.76),
        "expand_square": jnp.clip(jnp.exp(math.log(245.76) - 2.70805 * jax.random.uniform(key_of[17], (LAYERS, D, FF), jnp.float32) ** steps_of(key_of[17], (LAYERS, D, FF), ((1, 32),), -0.2, 0.2)), 16.384, 245.76),
        "reduce_square": jnp.clip(jnp.exp(math.log(245.76) - 2.70805 * jax.random.uniform(key_of[18], (LAYERS, D, FF), jnp.float32) ** steps_of(key_of[18], (LAYERS, D, FF), ((1, 32),), -0.2, 0.2)), 16.384, 245.76),
        "vectors_square": jnp.clip(jnp.exp(math.log(16384.0) - 2.9957323 * jax.random.uniform(key_of[19], (LAYERS, VEC), jnp.float32) ** steps_of(key_of[19], (LAYERS, VEC), ((1, 32),), -0.2, 0.2)), 819.2, 16384.0),
    }


NORM_EPSILON = 1e-05
ADAM_EPSILON = 1e-08
LEARNING = 0.02
BETA_FIRST = 0.9
BETA_SECOND = 0.95
DECAY_RATE = 0.1
MASKED_SCORE = -1e+30
PRECISE = lax.Precision.HIGHEST

@jax.custom_vjp
def low(v):
    return lax.optimization_barrier(v.astype(jnp.bfloat16)).astype(jnp.float32)

@jax.custom_vjp
def low_back(v):
    return v

def low_keep(v):
    return (low(v), None)

def low_pass(kept, grad):
    return (grad,)

def back_keep(v):
    return (v, None)

def back_low(kept, grad):
    return (low(grad),)
low.defvjp(low_keep, low_pass)
low_back.defvjp(back_keep, back_low)

def layer_norm(values, norm_gain, norm_shift):
    row_mean = lax.optimization_barrier(jnp.mean(values, -1, keepdims=True))
    centred = values - row_mean
    spread = lax.optimization_barrier(jnp.mean(centred * centred, -1, keepdims=True))
    return centred * lax.rsqrt(spread + NORM_EPSILON) * norm_gain + norm_shift

def split_vectors(vectors):
    return (vectors[0:D], vectors[D:2 * D], vectors[2 * D:3 * D], vectors[3 * D:4 * D], vectors[4 * D:7 * D], vectors[7 * D:8 * D], vectors[8 * D:8 * D + FF], vectors[8 * D + FF:])

def rotary_tables(row_count):
    half_rot = ROT_DIM // 2
    frequency = 10000.0 ** (-(jnp.arange(half_rot, dtype=jnp.float32) * 2.0) / ROT_DIM)
    angles = jnp.arange(row_count, dtype=jnp.float32)[:, None] * frequency[None, :]
    angles = jnp.concatenate([angles, angles], -1)[:, None, :]
    return (jnp.cos(angles), jnp.sin(angles))

def rotate(values, cosine, sine_table):
    half_rot = ROT_DIM // 2
    rotated = values[..., :ROT_DIM]
    turned = jnp.concatenate([-rotated[..., half_rot:], rotated[..., :half_rot]], -1)
    return jnp.concatenate([rotated * cosine + turned * sine_table, values[..., ROT_DIM:]], -1)

def attention(queries, keys, values, key_mask):
    score_scale = HEAD_DIM ** (-0.5)

    def one_head(pieces):
        query_head, key_head, value_head = pieces
        scores = low_back(jnp.einsum('gqd,gkd->gqk', query_head, key_head, precision=PRECISE) * score_scale)
        scores = jnp.where(key_mask, scores, MASKED_SCORE)
        top_score = lax.optimization_barrier(jnp.max(scores, -1, keepdims=True))
        weights = jnp.exp(scores - top_score)
        probability = weights / lax.optimization_barrier(jnp.sum(weights, -1, keepdims=True))
        return jnp.einsum('gqk,gkd->gqd', low(probability), value_head, precision=PRECISE)
    heads_out = lax.map(jax.checkpoint(one_head), (jnp.moveaxis(queries, 2, 0), jnp.moveaxis(keys, 2, 0), jnp.moveaxis(values, 2, 0)))
    return jnp.moveaxis(heads_out, 0, 2)

def layer(inputs, attend_in, attend_out, expand_weight, reduce_weight, vectors, key_mask, cosine, sine_table):
    group_size = inputs.shape[0]
    row_count = inputs.shape[1]
    pieces = split_vectors(vectors)
    normed_one = low(layer_norm(inputs, pieces[0], pieces[1]))
    mixed = low_back(jnp.einsum('grd,de->gre', normed_one, attend_in, precision=PRECISE) + pieces[4])
    shaped = mixed.reshape(group_size, row_count, 3, HEADS, HEAD_DIM)
    queries = low(rotate(shaped[:, :, 0], cosine, sine_table))
    keys = low(rotate(shaped[:, :, 1], cosine, sine_table))
    values = low(shaped[:, :, 2])
    context = attention(queries, keys, values, key_mask).reshape(group_size, row_count, D)
    context = low(low_back(context))
    attended = jnp.einsum('grd,de->gre', context, attend_out, precision=PRECISE) + pieces[5]
    normed_two = low(layer_norm(inputs, pieces[2], pieces[3]))
    expanded = low_back(jnp.einsum('grd,df->grf', normed_two, expand_weight, precision=PRECISE) + pieces[6])
    activated = low(jax.nn.gelu(expanded, approximate=False))
    reduced = jnp.einsum('grf,df->grd', activated, reduce_weight, precision=PRECISE) + pieces[7]
    return inputs + attended + reduced

def forward(token_values, params, key_mask, cosine, sine_table):
    rounded = tuple((low(param_array) for param_array in params))
    current = token_values
    results = []
    for layer_index in range(LAYERS):
        current = layer(current, rounded[0][layer_index], rounded[1][layer_index], rounded[2][layer_index], rounded[3][layer_index], rounded[4][layer_index], key_mask, cosine, sine_table)
        if layer_index + 1 < LAYERS:
            current = low_back(low(current))
        results.append(current)
    return tuple(results)

def adam_update(weight, moment, square, gradient, first_fix, second_fix):
    moment = BETA_FIRST * moment + (1.0 - BETA_FIRST) * gradient
    square = BETA_SECOND * square + (1.0 - BETA_SECOND) * gradient * gradient
    change = -LEARNING * (moment / first_fix / (jnp.sqrt(square / second_fix) + ADAM_EPSILON) + DECAY_RATE * weight)
    return (change, moment, square)

def reference(tokens, cotangent, seq_lengths, seq_device, step_count, attend_in, attend_out, expand_weight, reduce_weight, layer_vectors, attend_in_mean, attend_out_mean, expand_mean, reduce_mean, vectors_mean, attend_in_square, attend_out_square, expand_square, reduce_square, vectors_square):
    owners = jnp.arange(DEVICES, dtype=jnp.int32)
    device_length = lax.optimization_barrier(jnp.sum(jnp.where(seq_device[:, None] == owners[None, :], seq_lengths[:, None], 0), 0)).astype(jnp.int32)
    group_size = 1
    while group_size * 2 <= DEVICES and DEVICES % (group_size * 2) == 0 and (group_size * 2 * ROWS_DEV <= 4096):
        group_size = group_size * 2
    blocks = DEVICES // group_size
    token_blocks = tokens.reshape(blocks, group_size, ROWS_DEV, D)
    cot_blocks = cotangent.reshape(blocks, group_size, ROWS_DEV, D)
    length_blocks = device_length.reshape(blocks, group_size)
    params = (attend_in, attend_out, expand_weight, reduce_weight, layer_vectors)
    cosine, sine_table = rotary_tables(ROWS_DEV)
    row_ids = jnp.arange(ROWS_DEV, dtype=jnp.int32)

    def scan_step(carried, pieces):
        token_group, cot_group, length_group = pieces
        key_mask = (row_ids[None, None, :] <= row_ids[None, :, None]) & (row_ids[None, None, :] < length_group[:, None, None])
        valid_rows = (row_ids[None, :] < length_group[:, None]).astype(jnp.float32)[:, :, None]

        def run_layers(token_values, weights):
            return forward(token_values, weights, key_mask, cosine, sine_table)
        results, pull_back = jax.vjp(run_layers, token_group.astype(jnp.float32), params)
        cotangents = tuple((jnp.zeros_like(piece_out) for piece_out in results[:-1])) + (cot_group.astype(jnp.float32) * valid_rows,)
        token_grad, weight_grads = pull_back(cotangents)
        carried = jax.tree.map(lambda former, latter: former + latter, carried, weight_grads)
        return (carried, (jnp.stack(results).astype(jnp.bfloat16), token_grad.astype(jnp.bfloat16)))
    zero_grads = jax.tree.map(jnp.zeros_like, params)
    summed, (states, token_grads) = lax.scan(scan_step, zero_grads, (token_blocks, cot_blocks, length_blocks))
    hidden_states = jnp.moveaxis(states, 1, 0).reshape(LAYERS, TOKENS, D)
    input_grad = token_grads.reshape(TOKENS, D)
    step_float = step_count[0].astype(jnp.float32)
    first_fix = 1.0 - jnp.power(BETA_FIRST, step_float)
    second_fix = 1.0 - jnp.power(BETA_SECOND, step_float)
    new_in = adam_update(attend_in, attend_in_mean, attend_in_square, summed[0], first_fix, second_fix)
    new_out = adam_update(attend_out, attend_out_mean, attend_out_square, summed[1], first_fix, second_fix)
    new_expand = adam_update(expand_weight, expand_mean, expand_square, summed[2], first_fix, second_fix)
    new_reduce = adam_update(reduce_weight, reduce_mean, reduce_square, summed[3], first_fix, second_fix)
    new_vectors = adam_update(layer_vectors, vectors_mean, vectors_square, summed[4], first_fix, second_fix)
    return (hidden_states, input_grad, summed[0], summed[1], summed[2], summed[3], summed[4], new_in[0], new_out[0], new_expand[0], new_reduce[0], new_vectors[0], new_in[1], new_out[1], new_expand[1], new_reduce[1], new_vectors[1], new_in[2], new_out[2], new_expand[2], new_reduce[2], new_vectors[2])
```

```python
import functools

import jax
import jax.numpy as jnp
from jax import lax
from jax.experimental import pallas as pl
from jax.experimental.pallas import tpu as pltpu
from jax.sharding import Mesh
from jax.sharding import PartitionSpec as P

HEADS = 16
LAYERS = 2
NORM_EPSILON = 1e-05
ADAM_EPSILON = 1e-08
LEARNING = 0.02
BETA_FIRST = 0.9
BETA_SECOND = 0.95
DECAY_RATE = 0.1
MASKED_SCORE = -1e30

TP = 8
HALF = TP // 2
BF = jnp.bfloat16
F32 = jnp.float32
MESH = pl.DeviceIdType.MESH
NT = (((1,), (1,)), ((), ()))
TN = (((0,), (0,)), ((), ()))
ANY = pl.BlockSpec(memory_space=pl.ANY)
VMEM = pl.BlockSpec(memory_space=pltpu.VMEM)
SMEM = pl.BlockSpec(memory_space=pltpu.SMEM)
VMEM_BYTES = 60 * 1024 * 1024


def place():
    return lax.axis_index("grp"), lax.axis_index("tp")


def nn_dot(a, b):
    return jnp.dot(a, b, preferred_element_type=F32)


def nt_dot(a, b):
    return lax.dot_general(a, b, NT, preferred_element_type=F32)


def tn_dot(a, b):
    return lax.dot_general(a, b, TN, preferred_element_type=F32)


def remote(src, dst, send, recv, target):
    return pltpu.make_async_remote_copy(
        src_ref=src, dst_ref=dst, send_sem=send, recv_sem=recv, device_id=target, device_id_type=MESH
    )


def greet(targets):
    barrier = pltpu.get_barrier_semaphore()
    for target in targets:
        pl.semaphore_signal(barrier, inc=1, device_id=target, device_id_type=MESH)
    pl.semaphore_wait(barrier, len(targets))


def greet_all(groups):
    grp, tp = place()
    me = grp * TP + tp
    total = groups * TP
    barrier = pltpu.get_barrier_semaphore()

    def signal(step, carry):
        other = lax.rem(me + step, total)
        pl.semaphore_signal(
            barrier, inc=1, device_id=(other // TP, lax.rem(other, TP)), device_id_type=MESH
        )
        return carry

    lax.fori_loop(1, total, signal, 0)
    pl.semaphore_wait(barrier, total - 1)


def spread_kernel(groups, owners, xh, s0, s1, wo, vec, xg, w0, w1, wog, vecg,
                  xs, xr, ss, sr, ts, tr, os, orr, vs, vr, loc):
    grp, tp = place()
    me = grp * TP + tp
    total = groups * TP
    core, chip = tp // HALF, lax.rem(tp, HALF)
    partner = lax.rem(tp + HALF, TP)
    greet_all(groups)
    own = [
        pltpu.make_async_copy(xh, xg.at[tp], loc.at[0]),
        pltpu.make_async_copy(s0.at[tp], w0.at[me], loc.at[1]),
        pltpu.make_async_copy(s1.at[tp], w1.at[tp], loc.at[2]),
        pltpu.make_async_copy(vec, vecg.at[me], loc.at[3]),
    ]
    first = []
    for step in range(1, HALF):
        peer = core * HALF + lax.rem(chip + step, HALF)
        first.append(remote(xh, xg.at[tp], xs.at[step], xr.at[step], (grp, peer)))
    first.append(remote(xh, xg.at[tp], xs.at[0], xr.at[0], (grp, partner)))
    for copy in first:
        copy.start()

    def to(step):
        other = lax.rem(me + step, total)
        return other // TP, lax.rem(other, TP)

    def block_copy(step):
        g, t = to(step)
        return remote(s0.at[t], w0.at[me], ss.at[step], sr.at[step], (g, t))

    def vec_copy(step):
        return remote(vec, vecg.at[me], vs.at[step], vr.at[step], to(step))

    def plane_copy(step):
        peer = lax.rem(tp + step, TP)
        return remote(s1.at[peer], w1.at[tp], ts.at[step], tr.at[step], (grp, peer))

    def start_all(step, carry):
        vec_copy(step).start()
        block_copy(step).start()
        return carry

    lax.fori_loop(1, total, start_all, 0)

    def start_plane(step, carry):
        plane_copy(step).start()
        return carry

    lax.fori_loop(1, TP, start_plane, 0)
    for copy in own:
        copy.start()
    slot = lax.rem(me, owners)
    user = me // owners
    for g in range(groups):
        target_self = (user == tp) & (g == grp)

        @pl.when(jnp.logical_not(target_self))
        def _():
            remote(wo, wog.at[slot], os.at[g], orr.at[slot], (g, user)).start()

        @pl.when(target_self)
        def _():
            pltpu.make_async_copy(wo, wog.at[slot], orr.at[slot]).start()

    passed = []
    for step in range(1, HALF):
        source = core * HALF + lax.rem(chip + HALF - step, HALF)
        remote(xh, xg.at[source], xs.at[step], xr.at[step], (grp, tp)).wait_recv()
        copy = remote(xg.at[source], xg.at[source], xs.at[HALF + step], xr.at[HALF + step], (grp, partner))
        copy.start()
        passed.append(copy)
    for copy in first:
        copy.wait_send()
    first[-1].wait_recv()
    for copy in passed:
        copy.wait()
    for copy in own:
        copy.wait()

    def wait_all(step, carry):
        vec_copy(step).wait()
        block_copy(step).wait()
        return carry

    lax.fori_loop(1, total, wait_all, 0)

    def wait_plane(step, carry):
        plane_copy(step).wait()
        return carry

    lax.fori_loop(1, TP, wait_plane, 0)
    for g in range(groups):

        @pl.when(jnp.logical_not((user == tp) & (g == grp)))
        def _():
            remote(wo, wog.at[slot], os.at[g], orr.at[slot], (g, user)).wait_send()

    for j in range(owners):
        pltpu.make_async_copy(wo, wog.at[j], orr.at[j]).wait()


def spread(groups, xh, s0, s1, wo, vec):
    total = groups * TP
    rows = s0.shape[1]
    owners = wo.shape[2] // TP // rows
    dma = pltpu.SemaphoreType.DMA
    return pl.pallas_call(
        functools.partial(spread_kernel, groups, owners),
        out_shape=(
            jax.ShapeDtypeStruct((TP,) + xh.shape, BF),
            jax.ShapeDtypeStruct((total,) + s0.shape[1:], BF),
            jax.ShapeDtypeStruct(s1.shape, BF),
            jax.ShapeDtypeStruct((owners,) + wo.shape, BF),
            jax.ShapeDtypeStruct((total,) + vec.shape, F32),
        ),
        in_specs=[ANY] * 5,
        out_specs=(ANY,) * 5,
        scratch_shapes=[
            dma((TP,)), dma((TP,)), dma((total,)), dma((total,)), dma((TP,)), dma((TP,)),
            dma((groups,)), dma((owners,)), dma((total,)), dma((total,)), dma((4,)),
        ],
        compiler_params=pltpu.CompilerParams(collective_id=1, has_side_effects=True),
        name="spread",
    )(xh, s0, s1, wo, vec)


def turn(values, rot):
    return (
        values * rot[0]
        + pltpu.roll(values, values.shape[1] - 8, 1) * rot[1]
        + pltpu.roll(values, 8, 1) * rot[2]
    )


def turn_back(values, rot):
    return (
        values * rot[0]
        + pltpu.roll(values * rot[1], 8, 1)
        + pltpu.roll(values * rot[2], values.shape[1] - 8, 1)
    )


def head_parts(values, head_dim):
    lane = lax.broadcasted_iota(jnp.int32, values.shape, 1)
    zero = jnp.zeros_like(values)
    return [
        jnp.where((lane >= h * head_dim) & (lane < (h + 1) * head_dim), values, zero)
        for h in range(values.shape[1] // head_dim)
    ]


def forward_kernel(head_dim, lens, xh, w, wo, gains, b_in, b_up, rot, part, qkv, prob, ctx, act, slope):
    width = qkv.shape[2] // 3
    ff = act.shape[2]
    rows = xh.shape[1]
    values = xh[0].astype(F32)
    normed = (values * gains[0:1] + gains[1:2]).astype(BF)
    mixed = nn_dot(normed, w[:, : 3 * width]) + b_in[...]
    queries = (turn(mixed[:, :width], rot).astype(BF).astype(F32) * head_dim ** (-0.5)).astype(BF)
    keys = turn(mixed[:, width : 2 * width], rot).astype(BF)
    vals = mixed[:, 2 * width :].astype(BF)
    qkv[0, :, :width] = queries
    qkv[0, :, width : 2 * width] = keys
    qkv[0, :, 2 * width :] = vals
    length = lens[pl.program_id(0)]
    row = lax.broadcasted_iota(jnp.int32, (rows, rows), 0)
    col = lax.broadcasted_iota(jnp.int32, (rows, rows), 1)
    allowed = (col <= row) & (col < length)
    total = None
    for h, (q_h, v_h) in enumerate(zip(head_parts(queries, head_dim), head_parts(vals, head_dim))):
        scores = jnp.where(allowed, nt_dot(q_h, keys), MASKED_SCORE)
        weights = jnp.exp(scores - jnp.max(scores, -1, keepdims=True))
        probability = (weights / jnp.sum(weights, -1, keepdims=True)).astype(BF)
        prob[0, h] = probability
        term = nn_dot(probability, v_h)
        total = term if total is None else total + term
    context = total.astype(BF)
    ctx[0] = context
    normed = (values * gains[2:3] + gains[3:4]).astype(BF)
    expanded = nn_dot(normed, w[:, 3 * width : 3 * width + ff]) + b_up[...]
    spread_to = 0.5 * (1.0 + lax.erf(expanded * 0.7071067811865476))
    active = (expanded * spread_to).astype(BF)
    act[0] = active
    slope[0] = (spread_to + expanded * (0.3989422804014327 * jnp.exp(-0.5 * expanded * expanded))).astype(BF)
    part[0] = (nn_dot(context, wo[...]) + nt_dot(active, w[:, 3 * width + ff :])).astype(BF)


def block_of(shape):
    return pl.BlockSpec((1,) + shape, lambda s, *_: (s,) + (0,) * len(shape))


def whole_of(shape):
    return pl.BlockSpec(shape, lambda s, *_: (0,) * len(shape))


def forward_layer(head_dim, lens, xg, w, wo, gains, b_in, b_up, rot):
    seqs, rows, width = xg.shape
    local = b_in.shape[1] // 3
    ff = b_up.shape[1]
    heads = local // head_dim
    outs = ((rows, width), (rows, 3 * local), (heads, rows, rows), (rows, local), (rows, ff), (rows, ff))
    return pl.pallas_call(
        functools.partial(forward_kernel, head_dim),
        grid_spec=pltpu.PrefetchScalarGridSpec(
            num_scalar_prefetch=1,
            grid=(seqs,),
            in_specs=[block_of((rows, width))]
            + [whole_of(a.shape) for a in (w, wo, gains, b_in, b_up, rot)],
            out_specs=[block_of(shape) for shape in outs],
        ),
        out_shape=[jax.ShapeDtypeStruct((seqs,) + shape, BF) for shape in outs],
        compiler_params=pltpu.CompilerParams(vmem_limit_bytes=VMEM_BYTES),
        cost_estimate=pl.CostEstimate(
            flops=2 * seqs * rows * width * 12 * local, bytes_accessed=24 << 20, transcendentals=0
        ),
        name="forward_layer",
    )(lens, xg, w, wo, gains, b_in, b_up, rot)


def backward_kernel(head_dim, gg, qkv, prob, ctx_unused, slope, w, wo, gains, rot, part, mixes, sums):
    width = qkv.shape[2] // 3
    ff = slope.shape[2]
    grad = gg[0]
    active_grad = nn_dot(grad, w[:, 3 * width + ff :])
    expanded_grad = (slope[0].astype(F32) * active_grad).astype(BF)
    total = nt_dot(expanded_grad, w[:, 3 * width : 3 * width + ff]) * gains[2:3]
    context_grad = nt_dot(grad, wo[...]).astype(BF)
    queries = qkv[0, :, :width]
    keys = qkv[0, :, width : 2 * width]
    vals = qkv[0, :, 2 * width :]
    query_grad = key_grad = value_grad = 0.0
    for h, (c_h, q_h, k_h) in enumerate(
        zip(head_parts(context_grad, head_dim), head_parts(queries, head_dim), head_parts(keys, head_dim))
    ):
        prob_b = prob[0, h]
        probability = prob_b.astype(F32)
        prob_grad = nt_dot(c_h, vals)
        value_grad = value_grad + tn_dot(prob_b, c_h)
        inner = jnp.sum(probability * prob_grad, -1, keepdims=True)
        score_grad = (probability * (prob_grad - inner)).astype(BF)
        query_grad = query_grad + nn_dot(score_grad, k_h)
        key_grad = key_grad + tn_dot(score_grad, q_h)
    query_grad = query_grad * head_dim ** (-0.5)
    pieces = [turn_back(query_grad, rot).astype(BF), turn_back(key_grad, rot).astype(BF), value_grad.astype(BF)]
    for i, piece in enumerate(pieces):
        mixes[0, :, i * width : (i + 1) * width] = piece
    mixes[0, :, 3 * width :] = expanded_grad
    for i, piece in enumerate(pieces):
        total = total + nt_dot(piece, w[:, i * width : (i + 1) * width]) * gains[0:1]
    part[0] = total.astype(BF)

    @pl.when(pl.program_id(0) == 0)
    def _():
        sums[...] = jnp.zeros_like(sums)

    for i, piece in enumerate(pieces):
        sums[:, i * width : (i + 1) * width] += jnp.sum(
            piece.astype(F32).reshape(-1, 8, width), axis=0
        )
    sums[:, 3 * width :] += jnp.sum(expanded_grad.astype(F32).reshape(-1, 8, ff), axis=0)


def backward_layer(head_dim, gg, qkv, prob, ctx, slope, w, wo, gains, rot):
    seqs, rows, width = gg.shape
    local = ctx.shape[2]
    ff = slope.shape[2]
    mix = 3 * local + ff
    return pl.pallas_call(
        functools.partial(backward_kernel, head_dim),
        grid=(seqs,),
        in_specs=[block_of(a.shape[1:]) for a in (gg, qkv, prob, ctx, slope)]
        + [whole_of(a.shape) for a in (w, wo, gains, rot)],
        out_specs=[block_of((rows, width)), block_of((rows, mix)), whole_of((8, mix))],
        out_shape=[
            jax.ShapeDtypeStruct((seqs, rows, width), BF),
            jax.ShapeDtypeStruct((seqs, rows, mix), BF),
            jax.ShapeDtypeStruct((8, mix), F32),
        ],
        compiler_params=pltpu.CompilerParams(vmem_limit_bytes=VMEM_BYTES),
        cost_estimate=pl.CostEstimate(
            flops=2 * seqs * rows * width * 14 * local, bytes_accessed=24 << 20, transcendentals=0
        ),
        name="backward_layer",
    )(gg, qkv, prob, ctx, slope, w, wo, gains, rot)


CHUNK = 32


def exchange_kernel(forward, gather, part, own, extra, *refs):
    if gather:
        out, gathered, met, joined, landed, ps, pr, bs, br, gs, gr, loc = refs
    else:
        out, met, joined, landed, ps, pr, bs, br = refs
        gathered = None
    grp, tp = place()
    core, chip = tp // HALF, lax.rem(tp, HALF)
    partner = lax.rem(tp + HALF, TP)
    rows, width = own.shape
    peers = [core * HALF + lax.rem(chip + step, HALF) for step in range(HALF)]
    greet([(grp, partner)] + [(grp, peer) for peer in peers[1:]])
    other_core = 1 - core
    order = [1, 2, 3, 0]
    to_partner = []
    for step in order:
        block = lax.rem(chip + step, HALF)
        copy = remote(part.at[other_core * HALF + block], met.at[step], ps.at[step], pr.at[step], (grp, partner))
        copy.start()
        to_partner.append(copy)
    sends = []
    for index, step in enumerate(order):
        to_partner[index].wait_recv()
        block = core * HALF + lax.rem(chip + step, HALF)

        def join(i, carry):
            at = pl.ds(pl.multiple_of(i * CHUNK, CHUNK), CHUNK)
            joined[step, at] = (part[block, at].astype(F32) + met[step, at].astype(F32)).astype(BF)
            return carry

        lax.fori_loop(0, rows // CHUNK, join, 0)
        if step:
            copy = remote(joined.at[step], landed.at[step], bs.at[step], br.at[step], (grp, peers[step]))
            copy.start()
            sends.append(copy)
    for copy in sends:
        copy.wait_recv()

    def finish(i, carry):
        at = pl.ds(pl.multiple_of(i * CHUNK, CHUNK), CHUNK)
        total = joined[0, at].astype(F32)
        for step in range(1, HALF):
            total = total + landed[step, at].astype(F32)
        if forward:
            result = (own[at].astype(F32) + total + extra[...]).astype(BF)
            out[at] = result
            values = result.astype(F32)
        else:
            values = own[at].astype(F32)
        centred = values - jnp.mean(values, -1, keepdims=True)
        scale = lax.rsqrt(jnp.mean(centred * centred, -1, keepdims=True) + NORM_EPSILON)
        if forward:
            gathered[tp, at] = (centred * scale).astype(BF)
        else:
            xhat = centred * scale
            mean_one = jnp.mean(total, -1, keepdims=True)
            mean_two = jnp.mean(total * xhat, -1, keepdims=True)
            result = (extra[at].astype(F32) + scale * (total - mean_one - xhat * mean_two)).astype(BF)
            out[at] = result
            if gather:
                gathered[tp, at] = result
        return carry

    lax.fori_loop(0, rows // CHUNK, finish, 0)
    for copy in to_partner + sends:
        copy.wait_send()
    if not gather:
        return
    first = [remote(gathered.at[tp], gathered.at[tp], gs.at[0], gr.at[0], (grp, partner))]
    for step in range(1, HALF):
        first.append(remote(gathered.at[tp], gathered.at[tp], gs.at[step], gr.at[step], (grp, peers[step])))
    for copy in first[1:] + first[:1]:
        copy.start()
    passed = []
    for step in range(1, HALF):
        source = core * HALF + lax.rem(chip + HALF - step, HALF)
        remote(gathered.at[source], gathered.at[source], gs.at[step], gr.at[step], (grp, tp)).wait_recv()
        copy = remote(
            gathered.at[source], gathered.at[source], gs.at[HALF + step], gr.at[HALF + step], (grp, partner)
        )
        copy.start()
        passed.append(copy)
    first[0].wait_recv()
    for copy in passed:
        copy.wait()
    for copy in first:
        copy.wait_send()


def exchange(part, own, extra, forward, gather, ident):
    seqs, rows, width = part.shape
    dma = pltpu.SemaphoreType.DMA
    out_shape = [jax.ShapeDtypeStruct((rows, width), BF)]
    scratch = [pltpu.VMEM((HALF, rows, width), BF)] * 3 + [dma((HALF,))] * 4
    if gather:
        out_shape.append(jax.ShapeDtypeStruct((seqs, rows, width), BF))
        scratch += [dma((TP,)), dma((TP,)), dma((1,))]
    return pl.pallas_call(
        functools.partial(exchange_kernel, forward, gather),
        out_shape=out_shape,
        in_specs=[VMEM] * 3,
        out_specs=[VMEM] * len(out_shape),
        scratch_shapes=scratch,
        compiler_params=pltpu.CompilerParams(
            collective_id=ident, has_side_effects=True, vmem_limit_bytes=VMEM_BYTES
        ),
        name="exchange",
    )(part, own, extra)


def settle_kernel(groups, owners, g0, h1, go, vec, r0, r1, ro, rv,
                  ss, sr, ts, tr, os, orr, vs, vr, loc):
    grp, tp = place()
    me = grp * TP + tp
    total = groups * TP
    greet_all(groups)

    def to(step):
        other = lax.rem(me + step, total)
        return other // TP, lax.rem(other, TP)

    def block_copy(step):
        g, t = to(step)
        return remote(g0.at[g * TP + t], r0.at[me], ss.at[step], sr.at[step], (g, t))

    def vec_copy(step):
        g, t = to(step)
        return remote(vec.at[g * TP + t], rv.at[me], vs.at[step], vr.at[step], (g, t))

    def plane_copy(step):
        peer = lax.rem(tp + step, TP)
        return remote(h1.at[peer], r1.at[tp], ts.at[step], tr.at[step], (grp, peer))

    def start_all(step, carry):
        vec_copy(step).start()
        block_copy(step).start()
        return carry

    lax.fori_loop(1, total, start_all, 0)

    def start_plane(step, carry):
        plane_copy(step).start()
        return carry

    lax.fori_loop(1, TP, start_plane, 0)
    own = [
        pltpu.make_async_copy(g0.at[me], r0.at[me], loc.at[0]),
        pltpu.make_async_copy(h1.at[tp], r1.at[tp], loc.at[1]),
        pltpu.make_async_copy(vec.at[me], rv.at[me], loc.at[2]),
    ]
    for copy in own:
        copy.start()
    for j in range(owners):
        owner = tp * owners + j

        @pl.when(owner != me)
        def _():
            remote(go.at[j], ro.at[grp], os.at[j], orr.at[grp], (owner // TP, lax.rem(owner, TP))).start()

        @pl.when(owner == me)
        def _():
            pltpu.make_async_copy(go.at[j], ro.at[grp], orr.at[grp]).start()

    for copy in own:
        copy.wait()

    def wait_all(step, carry):
        vec_copy(step).wait()
        block_copy(step).wait()
        return carry

    lax.fori_loop(1, total, wait_all, 0)

    def wait_plane(step, carry):
        plane_copy(step).wait()
        return carry

    lax.fori_loop(1, TP, wait_plane, 0)
    for j in range(owners):
        owner = tp * owners + j

        @pl.when(owner != me)
        def _():
            remote(go.at[j], ro.at[grp], os.at[j], orr.at[grp], (owner // TP, lax.rem(owner, TP))).wait_send()

    for g in range(groups):
        pltpu.make_async_copy(go.at[0], ro.at[g], orr.at[g]).wait()


def settle(groups, g0, h1, go, vec):
    total = groups * TP
    owners = go.shape[0]
    dma = pltpu.SemaphoreType.DMA
    return pl.pallas_call(
        functools.partial(settle_kernel, groups, owners),
        out_shape=(
            jax.ShapeDtypeStruct(g0.shape, BF),
            jax.ShapeDtypeStruct(h1.shape, BF),
            jax.ShapeDtypeStruct((groups,) + go.shape[1:], BF),
            jax.ShapeDtypeStruct(vec.shape, F32),
        ),
        in_specs=[ANY] * 4,
        out_specs=(ANY,) * 4,
        scratch_shapes=[
            dma((total,)), dma((total,)), dma((TP,)), dma((TP,)),
            dma((owners,)), dma((groups,)), dma((total,)), dma((total,)), dma((3,)),
        ],
        compiler_params=pltpu.CompilerParams(collective_id=4, has_side_effects=True),
        name="settle",
    )(g0, h1, go, vec)


def rotary(row_count, width, head_dim):
    rot_dim = head_dim // 4
    half_rot = rot_dim // 2
    column = jnp.arange(width, dtype=jnp.int32) % head_dim
    freq_slot = (column % half_rot).astype(F32)
    frequency = 10000.0 ** (-(freq_slot * 2.0) / rot_dim)
    angles = jnp.arange(row_count, dtype=F32)[:, None] * frequency[None, :]
    inside = (column < rot_dim)[None, :]
    first_half = (column < half_rot)[None, :]
    sine = jnp.sin(angles)
    return jnp.stack(
        [
            jnp.where(inside, jnp.cos(angles), 1.0),
            jnp.where(first_half, -sine, 0.0),
            jnp.where(inside & jnp.logical_not(first_half), sine, 0.0),
        ]
    )


def standard(values):
    centred = values - jnp.mean(values, -1, keepdims=True)
    return centred * lax.rsqrt(jnp.mean(centred * centred, -1, keepdims=True) + NORM_EPSILON)


def adam_update(weight, moment, square, gradient, first_fix, second_fix):
    moment = BETA_FIRST * moment + (1.0 - BETA_FIRST) * gradient
    square = BETA_SECOND * square + (1.0 - BETA_SECOND) * gradient * gradient
    change = -LEARNING * (
        moment / first_fix / (jnp.sqrt(square / second_fix) + ADAM_EPSILON) + DECAY_RATE * weight
    )
    return (change, moment, square)


def per_device(
    groups,
    tokens,
    cotangent,
    seq_lengths,
    seq_device,
    step_count,
    *state,
):
    params, moments, squares = state[0:5], state[5:10], state[10:15]
    attend_in, attend_out, expand_weight, reduce_weight, layer_vectors = params
    grp, tp = place()
    me = grp * TP + tp
    total = groups * TP
    rows, width = tokens.shape
    shard = attend_in.shape[1]
    head_dim = width // HEADS
    local = width // TP
    ff = expand_weight.shape[2] // TP
    vec_part = layer_vectors.shape[1]
    owners = local // shard
    plane_ids = grp * TP + jnp.arange(TP, dtype=jnp.int32)
    lens = jnp.sum(jnp.where(plane_ids[:, None] == seq_device[None, :], seq_lengths[None, :], 0), 1)
    own_length = jnp.sum(jnp.where(seq_device == me, seq_lengths, 0))
    valid = jnp.arange(rows, dtype=jnp.int32)[:, None] < own_length
    rot = rotary(rows, local, head_dim)

    blocks = [
        jnp.concatenate(
            [
                attend_in[l].astype(BF).reshape(shard, 3, TP, local).transpose(2, 0, 1, 3).reshape(TP, shard, 3 * local),
                expand_weight[l].astype(BF).reshape(shard, TP, ff).transpose(1, 0, 2),
                reduce_weight[l].astype(BF).reshape(shard, TP, ff).transpose(1, 0, 2),
            ],
            2,
        )
        for l in range(LAYERS)
    ]
    vec = jnp.pad(layer_vectors.astype(BF).astype(F32).reshape(-1), (0, 8 * 128 - 2 * vec_part)).reshape(8, 128)
    xhat_own = standard(tokens.astype(F32)).astype(BF)
    grad_own = jnp.where(valid, cotangent, jnp.zeros_like(cotangent))
    xg, w0, w1, wog, vecg = spread(groups, xhat_own, blocks[0], blocks[1], attend_out.astype(BF), vec)
    grads_all = lax.all_gather(grad_own, "tp", axis=0)
    weights = [w0.reshape(width, -1), lax.all_gather(w1, "grp", axis=0).reshape(width, -1)]
    out_rows = wog.transpose(1, 0, 2, 3).reshape(LAYERS, local, width)
    vectors = vecg.reshape(total, -1)[:, : 2 * vec_part].reshape(total, LAYERS, vec_part)
    vectors = vectors.transpose(1, 0, 2).reshape(LAYERS, -1)
    gains, b_in, b_up, b_rest = [], [], [], []
    for l in range(LAYERS):
        v = vectors[l]
        gains.append(v[: 4 * width].reshape(4, width))
        b_in.append(
            lax.dynamic_slice_in_dim(v[4 * width : 7 * width].reshape(3, width), tp * local, local, 1).reshape(1, -1)
        )
        b_up.append(lax.dynamic_slice_in_dim(v[8 * width : -width].reshape(1, -1), tp * ff, ff, 1))
        b_rest.append((v[7 * width : 8 * width] + v[-width:])[None, :])

    part0, *kept0 = forward_layer(head_dim, lens, xg, weights[0], out_rows[0], gains[0], b_in[0], b_up[0], rot)
    hidden0, xg1 = exchange(part0, tokens, b_rest[0], True, True, 2)
    part1, *kept1 = forward_layer(head_dim, lens, xg1, weights[1], out_rows[1], gains[1], b_in[1], b_up[1], rot)
    summed1 = lax.psum_scatter(part1, "tp", scatter_dimension=0, tiled=True)[0]
    hidden1 = (hidden0.astype(F32) + summed1.astype(F32) + b_rest[1]).astype(BF)

    def layer_back(l, xhats, gg, grad_rows, kept):
        qkv, prob, ctx, act, slope = kept
        part, mixes, sums = backward_layer(
            head_dim, gg, qkv, prob, ctx, slope, weights[l], out_rows[l], gains[l], rot
        )
        flat = lambda a: a.reshape(-1, a.shape[-1])
        sums = jnp.sum(sums, 0)
        cross = tn_dot(flat(xhats), flat(mixes))
        gain_one, shift_one, gain_two, shift_two = (gains[l][i][:, None] for i in range(4))
        split = 3 * local
        w_in, w_up = weights[l][:, :split].astype(F32), weights[l][:, split : split + ff].astype(F32)
        in_grad = gain_one * cross[:, :split] + shift_one * sums[None, :split]
        up_grad = gain_two * cross[:, split:] + shift_two * sums[None, split:]
        down_grad = tn_dot(flat(gg), flat(act))
        out_grad = tn_dot(flat(ctx), flat(gg)).astype(BF)
        packed = jnp.concatenate([in_grad.astype(BF), up_grad.astype(BF), down_grad.astype(BF)], 1)
        norm_sums = [
            jnp.sum(w_in * cross[:, :split], 1),
            jnp.sum(w_in * sums[None, :split], 1),
            jnp.sum(w_up * cross[:, split:], 1),
            jnp.sum(w_up * sums[None, split:], 1),
        ]
        here = (jnp.arange(TP) == tp)
        in_bias = jnp.where(here[None, :, None], sums[:split].reshape(3, 1, local), 0.0).reshape(-1)
        up_bias = jnp.where(here[:, None], sums[None, split:], 0.0).reshape(-1)
        bias_sums = jnp.sum(grad_rows.astype(F32), 0)
        vector = jnp.concatenate(norm_sums + [in_bias, bias_sums, up_bias, bias_sums])
        return part, packed, out_grad, vector

    part, packed1, out_grad1, vector1 = layer_back(1, xg1, grads_all, grad_own, kept1)
    reduced1 = lax.psum_scatter(packed1, "grp", scatter_dimension=0, tiled=True).reshape(TP, shard, -1)
    grad0, gg0 = exchange(part, hidden0, grad_own, False, True, 3)
    part, packed0, out_grad0, vector0 = layer_back(0, xg, gg0, grad0, kept0)
    (input_grad,) = exchange(part, tokens, grad0, False, False, 5)
    out_grads = jnp.stack([out_grad0, out_grad1]).reshape(LAYERS, owners, shard, width).transpose(1, 0, 2, 3)
    vec_send = jnp.stack([vector0, vector1]).reshape(LAYERS, total, vec_part).transpose(1, 0, 2).reshape(total, -1)
    vec_send = jnp.pad(vec_send, ((0, 0), (0, 8 * 128 - 2 * vec_part))).reshape(total, 8, 128)
    r0, r1, ro, rv = settle(groups, packed0.reshape(total, shard, -1), reduced1, out_grads, vec_send)
    split = 3 * local
    sum0 = jnp.sum(r0.reshape(groups, TP, shard, -1).astype(F32), 0)
    sums = [sum0, r1.astype(F32)]
    grad_in = jnp.stack(
        [s[:, :, :split].reshape(TP, shard, 3, local).transpose(1, 2, 0, 3).reshape(shard, -1) for s in sums]
    )
    grad_up = jnp.stack([s[:, :, split : split + ff].transpose(1, 0, 2).reshape(shard, -1) for s in sums])
    grad_down = jnp.stack([s[:, :, split + ff :].transpose(1, 0, 2).reshape(shard, -1) for s in sums])
    grad_out = jnp.sum(ro.astype(F32), 0)
    grad_vec = jnp.sum(rv, 0).reshape(-1)[: 2 * vec_part].reshape(LAYERS, vec_part)
    grads = (grad_in, grad_out, grad_up, grad_down, grad_vec)
    step_float = step_count[0].astype(F32)
    first_fix = 1.0 - jnp.power(BETA_FIRST, step_float)
    second_fix = 1.0 - jnp.power(BETA_SECOND, step_float)
    updated = [
        adam_update(params[i], moments[i], squares[i], grads[i], first_fix, second_fix) for i in range(5)
    ]
    return (
        jnp.stack([hidden0, hidden1]),
        input_grad,
        *grads,
        *(u[0] for u in updated),
        *(u[1] for u in updated),
        *(u[2] for u in updated),
    )


def solution(mesh):
    devices = mesh.devices.reshape(-1, TP)
    groups = devices.shape[0]
    flat = Mesh(devices, ("grp", "tp"))
    axes = ("grp", "tp")
    by_row = P(axes, None)
    by_dim = [P(None, axes, None)] * 4 + [P(None, axes)]
    return jax.shard_map(
        functools.partial(per_device, groups),
        mesh=flat,
        in_specs=(by_row, by_row, P(), P(), P(), *(by_dim * 3)),
        out_specs=(P(None, axes, None), by_row, *(by_dim * 4)),
        check_vma=False,
    )
```

```python
import functools

import jax
import jax.numpy as jnp
from jax import lax
from jax.experimental import pallas as pl
from jax.experimental.pallas import tpu as pltpu
from jax.sharding import Mesh
from jax.sharding import PartitionSpec as P

HEADS = 16
LAYERS = 2
NORM_EPSILON = 1e-05
ADAM_EPSILON = 1e-08
LEARNING = 0.02
BETA_FIRST = 0.9
BETA_SECOND = 0.95
DECAY_RATE = 0.1
MASKED_SCORE = -1e30

TP = 8
HALF = TP // 2
BF = jnp.bfloat16
F32 = jnp.float32
MESH = pl.DeviceIdType.MESH
NT = (((1,), (1,)), ((), ()))
TN = (((0,), (0,)), ((), ()))
ANY = pl.BlockSpec(memory_space=pl.ANY)
VMEM = pl.BlockSpec(memory_space=pltpu.VMEM)
SMEM = pl.BlockSpec(memory_space=pltpu.SMEM)
VMEM_BYTES = 60 * 1024 * 1024


def place():
    return lax.axis_index("grp"), lax.axis_index("tp")


def nn_dot(a, b):
    return jnp.dot(a, b, preferred_element_type=F32)


def nt_dot(a, b):
    return lax.dot_general(a, b, NT, preferred_element_type=F32)


def tn_dot(a, b):
    return lax.dot_general(a, b, TN, preferred_element_type=F32)


def remote(src, dst, send, recv, target):
    return pltpu.make_async_remote_copy(
        src_ref=src, dst_ref=dst, send_sem=send, recv_sem=recv, device_id=target, device_id_type=MESH
    )


def greet(targets):
    barrier = pltpu.get_barrier_semaphore()
    for target in targets:
        pl.semaphore_signal(barrier, inc=1, device_id=target, device_id_type=MESH)
    pl.semaphore_wait(barrier, len(targets))


def greet_all(groups):
    grp, tp = place()
    me = grp * TP + tp
    total = groups * TP
    barrier = pltpu.get_barrier_semaphore()

    def signal(step, carry):
        other = lax.rem(me + step, total)
        pl.semaphore_signal(
            barrier, inc=1, device_id=(other // TP, lax.rem(other, TP)), device_id_type=MESH
        )
        return carry

    lax.fori_loop(1, total, signal, 0)
    pl.semaphore_wait(barrier, total - 1)


def spread_kernel(groups, owners, xh, s0, s1, wo, vec, xg, w0, w1, wog, vecg,
                  xs, xr, ss, sr, ts, tr, os, orr, vs, vr, loc):
    grp, tp = place()
    me = grp * TP + tp
    total = groups * TP
    core, chip = tp // HALF, lax.rem(tp, HALF)
    partner = lax.rem(tp + HALF, TP)
    greet_all(groups)
    own = [
        pltpu.make_async_copy(xh, xg.at[tp], loc.at[0]),
        pltpu.make_async_copy(s0.at[tp], w0.at[me], loc.at[1]),
        pltpu.make_async_copy(s1.at[tp], w1.at[tp], loc.at[2]),
        pltpu.make_async_copy(vec, vecg.at[me], loc.at[3]),
    ]
    first = []
    for step in range(1, HALF):
        peer = core * HALF + lax.rem(chip + step, HALF)
        first.append(remote(xh, xg.at[tp], xs.at[step], xr.at[step], (grp, peer)))
    first.append(remote(xh, xg.at[tp], xs.at[0], xr.at[0], (grp, partner)))
    for copy in first:
        copy.start()

    def to(step):
        other = lax.rem(me + step, total)
        return other // TP, lax.rem(other, TP)

    def block_copy(step):
        g, t = to(step)
        return remote(s0.at[t], w0.at[me], ss.at[step], sr.at[step], (g, t))

    def vec_copy(step):
        return remote(vec, vecg.at[me], vs.at[step], vr.at[step], to(step))

    def plane_copy(step):
        peer = lax.rem(tp + step, TP)
        return remote(s1.at[peer], w1.at[tp], ts.at[step], tr.at[step], (grp, peer))

    def start_all(step, carry):
        vec_copy(step).start()
        block_copy(step).start()
        return carry

    lax.fori_loop(1, total, start_all, 0)

    def start_plane(step, carry):
        plane_copy(step).start()
        return carry

    lax.fori_loop(1, TP, start_plane, 0)
    for copy in own:
        copy.start()
    slot = lax.rem(me, owners)
    user = me // owners
    for g in range(groups):
        target_self = (user == tp) & (g == grp)

        @pl.when(jnp.logical_not(target_self))
        def _():
            remote(wo, wog.at[slot], os.at[g], orr.at[slot], (g, user)).start()

        @pl.when(target_self)
        def _():
            pltpu.make_async_copy(wo, wog.at[slot], orr.at[slot]).start()

    passed = []
    for step in range(1, HALF):
        source = core * HALF + lax.rem(chip + HALF - step, HALF)
        remote(xh, xg.at[source], xs.at[step], xr.at[step], (grp, tp)).wait_recv()
        copy = remote(xg.at[source], xg.at[source], xs.at[HALF + step], xr.at[HALF + step], (grp, partner))
        copy.start()
        passed.append(copy)
    for copy in first:
        copy.wait_send()
    first[-1].wait_recv()
    for copy in passed:
        copy.wait()
    for copy in own:
        copy.wait()

    def wait_all(step, carry):
        vec_copy(step).wait()
        block_copy(step).wait()
        return carry

    lax.fori_loop(1, total, wait_all, 0)

    def wait_plane(step, carry):
        plane_copy(step).wait()
        return carry

    lax.fori_loop(1, TP, wait_plane, 0)
    for g in range(groups):

        @pl.when(jnp.logical_not((user == tp) & (g == grp)))
        def _():
            remote(wo, wog.at[slot], os.at[g], orr.at[slot], (g, user)).wait_send()

    for j in range(owners):
        pltpu.make_async_copy(wo, wog.at[j], orr.at[j]).wait()


def spread(groups, xh, s0, s1, wo, vec):
    total = groups * TP
    rows = s0.shape[1]
    owners = wo.shape[2] // TP // rows
    dma = pltpu.SemaphoreType.DMA
    return pl.pallas_call(
        functools.partial(spread_kernel, groups, owners),
        out_shape=(
            jax.ShapeDtypeStruct((TP,) + xh.shape, BF),
            jax.ShapeDtypeStruct((total,) + s0.shape[1:], BF),
            jax.ShapeDtypeStruct(s1.shape, BF),
            jax.ShapeDtypeStruct((owners,) + wo.shape, BF),
            jax.ShapeDtypeStruct((total,) + vec.shape, F32),
        ),
        in_specs=[ANY] * 5,
        out_specs=(ANY,) * 5,
        scratch_shapes=[
            dma((TP,)), dma((TP,)), dma((total,)), dma((total,)), dma((TP,)), dma((TP,)),
            dma((groups,)), dma((owners,)), dma((total,)), dma((total,)), dma((4,)),
        ],
        compiler_params=pltpu.CompilerParams(collective_id=1, has_side_effects=True),
        name="spread",
    )(xh, s0, s1, wo, vec)


def turn(values, rot):
    return (
        values * rot[0]
        + pltpu.roll(values, values.shape[1] - 8, 1) * rot[1]
        + pltpu.roll(values, 8, 1) * rot[2]
    )


def turn_back(values, rot):
    return (
        values * rot[0]
        + pltpu.roll(values * rot[1], 8, 1)
        + pltpu.roll(values * rot[2], values.shape[1] - 8, 1)
    )


def head_parts(values, head_dim):
    lane = lax.broadcasted_iota(jnp.int32, values.shape, 1)
    zero = jnp.zeros_like(values)
    return [
        jnp.where((lane >= h * head_dim) & (lane < (h + 1) * head_dim), values, zero)
        for h in range(values.shape[1] // head_dim)
    ]


def bias_slices(vec, tp, local, ff):
    width = vec.shape[1]
    b_in = vec[4:7, pl.ds(pl.multiple_of(tp * local, local), local)]
    per_row = width // ff
    row = 8 + tp // per_row
    b_up = vec[pl.ds(row, 1), pl.ds(pl.multiple_of(lax.rem(tp, per_row) * ff, ff), ff)]
    return b_in, b_up


def seq_forward(values, lengths, head_dim, w, wo, vec, b_in, b_up, rot):
    rows = values.shape[0]
    local = wo.shape[0]
    ff = b_up.shape[1]
    values = values.astype(F32)
    normed = (values * vec[0:1] + vec[1:2]).astype(BF)
    mixed = nn_dot(normed, w[:, : 3 * local])
    parts = [mixed[:, i * local : (i + 1) * local] + b_in[i : i + 1] for i in range(3)]
    queries = (turn(parts[0], rot).astype(BF).astype(F32) * head_dim ** (-0.5)).astype(BF)
    keys = turn(parts[1], rot).astype(BF)
    vals = parts[2].astype(BF)
    row = lax.broadcasted_iota(jnp.int32, (rows, rows), 0)
    col = lax.broadcasted_iota(jnp.int32, (rows, rows), 1)
    allowed = (col <= row) & (col < lengths)
    total, probs = None, []
    for q_h, v_h in zip(head_parts(queries, head_dim), head_parts(vals, head_dim)):
        scores = jnp.where(allowed, nt_dot(q_h, keys), MASKED_SCORE)
        weights = jnp.exp(scores - jnp.max(scores, -1, keepdims=True))
        probability = (weights / jnp.sum(weights, -1, keepdims=True)).astype(BF)
        probs.append(probability)
        term = nn_dot(probability, v_h)
        total = term if total is None else total + term
    context = total.astype(BF)
    normed = (values * vec[2:3] + vec[3:4]).astype(BF)
    expanded = nn_dot(normed, w[:, 3 * local : 3 * local + ff]) + b_up
    spread_to = 0.5 * (1.0 + lax.erf(expanded * 0.7071067811865476))
    active = (expanded * spread_to).astype(BF)
    slope = (spread_to + expanded * (0.3989422804014327 * jnp.exp(-0.5 * expanded * expanded))).astype(BF)
    part = nn_dot(context, wo[...]) + nt_dot(active, w[:, 3 * local + ff :])
    return part, (queries, keys, vals), probs, context, active, slope


def seq_backward(grad, qkv, probs, slope, head_dim, w, wo, vec, rot):
    local = wo.shape[0]
    ff = slope.shape[1]
    queries, keys, vals = qkv
    active_grad = nn_dot(grad, w[:, 3 * local + ff :])
    expanded_grad = (slope.astype(F32) * active_grad).astype(BF)
    total = nt_dot(expanded_grad, w[:, 3 * local : 3 * local + ff]) * vec[2:3]
    context_grad = nt_dot(grad, wo[...]).astype(BF)
    query_grad = key_grad = value_grad = 0.0
    for prob_b, c_h, q_h, k_h in zip(
        probs, head_parts(context_grad, head_dim), head_parts(queries, head_dim), head_parts(keys, head_dim)
    ):
        probability = prob_b.astype(F32)
        prob_grad = nt_dot(c_h, vals)
        value_grad = value_grad + tn_dot(prob_b, c_h)
        inner = jnp.sum(probability * prob_grad, -1, keepdims=True)
        score_grad = (probability * (prob_grad - inner)).astype(BF)
        query_grad = query_grad + nn_dot(score_grad, k_h)
        key_grad = key_grad + tn_dot(score_grad, q_h)
    query_grad = query_grad * head_dim ** (-0.5)
    pieces = [turn_back(query_grad, rot).astype(BF), turn_back(key_grad, rot).astype(BF), value_grad.astype(BF)]
    mixed_grad = jnp.concatenate(pieces, 1)
    total = total + nt_dot(mixed_grad, w[:, : 3 * local]) * vec[0:1]
    return total, mixed_grad, expanded_grad


def fold_rows(values):
    return jnp.sum(values.astype(F32).reshape(-1, 8, values.shape[1]), axis=0)


def across(chip, step):
    x = lax.rem(lax.rem(chip, 2) + lax.rem(step, 2), 2)
    y = lax.rem(chip // 2 + step // 2, 2)
    return 2 * y + x


def pick(core, other):
    return core + (1 - 2 * core) * other


CHUNK = 32


def chunks(rows, body):
    def step(i, carry):
        body(pl.ds(pl.multiple_of(i * CHUNK, CHUNK), CHUNK))
        return carry

    lax.fori_loop(0, rows // CHUNK, step, 0)


def norm_parts(values):
    centred = values - jnp.mean(values, -1, keepdims=True)
    return centred, lax.rsqrt(jnp.mean(centred * centred, -1, keepdims=True) + NORM_EPSILON)


class Exchange:
    def __init__(self, both, met, landed, sems):
        self.joined, self.mine, self.met, self.landed = both.at[0], both.at[1], met, landed
        self.ps, self.pr, self.bs, self.br = sems
        self.grp, tp = place()
        self.core, self.chip = tp // HALF, lax.rem(tp, HALF)
        self.partner = lax.rem(tp + HALF, TP)

    def to_partner(self, k):
        return remote(
            self.mine.at[k], self.met.at[k], self.ps.at[k], self.pr.at[k], (self.grp, self.partner)
        )

    def to_owner(self, k):
        owner = self.core * HALF + across(self.chip, k)
        return remote(
            self.joined.at[k], self.landed.at[k], self.bs.at[k], self.br.at[k], (self.grp, owner)
        )

    def join(self, k):
        self.to_partner(k).wait_recv()

        def add(at):
            self.joined[k, at] = (self.joined[k, at].astype(F32) + self.met[k, at].astype(F32)).astype(BF)

        chunks(self.met.shape[1], add)

    def hand_over(self, k):
        self.join(k)
        if k:
            self.to_owner(k).start()

    def total(self, at):
        value = self.joined[0, at].astype(F32)
        for k in range(1, HALF):
            value = value + self.landed[k, at].astype(F32)
        return value

    def wait_landed(self):
        for k in range(1, HALF):
            self.to_owner(k).wait_recv()

    def drain(self):
        for k in range(HALF):
            self.to_partner(k).wait_send()
        for k in range(1, HALF):
            self.to_owner(k).wait_send()


class Gather:
    def __init__(self, own, buffer, sems):
        self.own, self.buffer = own, buffer
        self.gs, self.gr, self.fs, self.fr = sems
        self.grp, self.tp = place()
        self.core, self.chip = self.tp // HALF, lax.rem(self.tp, HALF)
        self.partner = lax.rem(self.tp + HALF, TP)

    def to_peer(self, k):
        if isinstance(k, int) and k == 0:
            target = self.partner
        else:
            target = self.core * HALF + across(self.chip, k)
        return remote(self.own, self.buffer.at[self.tp], self.gs.at[k], self.gr.at[k], (self.grp, target))

    def start(self, local):
        pltpu.make_async_copy(self.own, self.buffer.at[self.tp], local).start()
        for k in (1, 2, 3, 0):
            self.to_peer(k).start()
        pltpu.make_async_copy(self.own, self.buffer.at[self.tp], local).wait()

    def pass_on(self, k):
        source = self.core * HALF + across(self.chip, k)
        block = self.buffer.at[source]
        return remote(block, block, self.fs.at[k], self.fr.at[k], (self.grp, self.partner))

    def arrived(self, source, sem):
        block = self.buffer.at[source]
        remote(block, block, sem, sem, (self.grp, self.partner)).wait_recv()

    def wait_block(self, k):
        self.arrived(self.core * HALF + across(self.chip, k), self.gr.at[k])
        self.pass_on(k).start()

    def wait_partner(self):
        self.arrived(self.partner, self.gr.at[0])

    def wait_passed(self, k):
        self.arrived((1 - self.core) * HALF + across(self.chip, k), self.fr.at[k])

    def settle(self, k, work):
        block = across(self.chip, k)
        for other in range(2):
            work[other] = self.buffer[pick(self.core, other) * HALF + block]

    def drain(self):
        for k in range(HALF):
            self.to_peer(k).wait_send()
        for k in range(1, HALF):
            self.pass_on(k).wait_send()


def greet_plane():
    grp, tp = place()
    core, chip = tp // HALF, lax.rem(tp, HALF)
    targets = [lax.rem(tp + HALF, TP)] + [core * HALF + across(chip, k) for k in range(1, HALF)]
    greet([(grp, target) for target in targets])


def first_kernel(head_dim, lens, xg, w, wo, vec, rot, own,
                 out, xnext, qkv_h, prob_h, ctx_h, act_h, slope_h,
                 qkv, prob, ctx, act, slope, both, met, landed, keep, *sems):
    grp, tp = place()
    core, chip = tp // HALF, lax.rem(tp, HALF)
    local, ff = wo.shape[0], act.shape[2]
    swap = Exchange(both, met, landed, sems)
    kept = [(qkv, qkv_h), (prob, prob_h), (ctx, ctx_h), (act, act_h), (slope, slope_h)]
    greet_plane()
    b_in, b_up = bias_slices(vec, tp, local, ff)

    def one(seq):
        part, mixed, probs, context, active, sl = seq_forward(
            xg[seq], lens[seq], head_dim, w, wo, vec, b_in, b_up, rot
        )
        for i, piece in enumerate(mixed):
            qkv[seq, :, i * local : (i + 1) * local] = piece
        for h, p in enumerate(probs):
            prob[seq, h] = p
        ctx[seq] = context
        act[seq] = active
        slope[seq] = sl
        return part

    for k in reversed(range(HALF)):
        block = across(chip, k)

        def part_of(other, carry):
            both[other, k] = one(pick(core, other) * HALF + block).astype(BF)
            return carry

        lax.fori_loop(0, 2, part_of, 0)
        swap.to_partner(k).start()
        if k + 1 < HALF:
            swap.hand_over(k + 1)
    swap.hand_over(0)
    saved = [pltpu.make_async_copy(a, b, keep.at[i]) for i, (a, b) in enumerate(kept)]
    for copy in saved:
        copy.start()
    swap.wait_landed()

    def finish(at):
        result = (own[at].astype(F32) + swap.total(at) + (vec[7:8] + vec[12:13])).astype(BF)
        out[at] = result
        centred, scale = norm_parts(result.astype(F32))
        xnext[at] = (centred * scale).astype(BF)

    chunks(own.shape[0], finish)
    swap.drain()
    for copy in saved:
        copy.wait()


def first_layer(head_dim, lens, xg, w, wo, vec, rot, own):
    seqs, rows, width = xg.shape
    local = wo.shape[0]
    ff = (w.shape[1] - 3 * local) // 2
    dma = pltpu.SemaphoreType.DMA
    kept = [
        (seqs, rows, 3 * local), (seqs, local // head_dim, rows, rows), (seqs, rows, local), (seqs, rows, ff),
        (seqs, rows, ff),
    ]
    block = pltpu.VMEM((HALF, rows, width), BF)
    pair = pltpu.VMEM((2, HALF, rows, width), BF)
    return pl.pallas_call(
        functools.partial(first_kernel, head_dim),
        out_shape=[jax.ShapeDtypeStruct((rows, width), BF)] * 2 + [jax.ShapeDtypeStruct(s, BF) for s in kept],
        in_specs=[VMEM] * 7,
        out_specs=[VMEM] * 2 + [ANY] * 5,
        scratch_shapes=[pltpu.VMEM(s, BF) for s in kept] + [pair, block, block] + [dma((5,))] + [dma((HALF,))] * 4,
        compiler_params=pltpu.CompilerParams(
            collective_id=2, has_side_effects=True, vmem_limit_bytes=VMEM_BYTES
        ),
        name="first_layer",
    )(lens, xg, w, wo, vec, rot, own)


def weight_grads(xg, gg, mixes, act, ctx, w, vec, sums, packed, out_grad, vrows, grad_rows, tp):
    local, width = out_grad.shape[0] * out_grad.shape[1], out_grad.shape[2]
    total, shard, cols = packed.shape
    ff = act.shape[2]
    split = 3 * local
    rows = xg.shape[0] * xg.shape[1]
    flat = lambda ref, cut: ref[:, :, cut].reshape(rows, -1)
    everything = slice(None)
    col_sums = jnp.sum(sums[...], axis=0, keepdims=True)
    half = width // 2
    ones = jnp.ones((8, split), F32)
    wide = jnp.ones((8, ff), F32)
    exact = lambda a, b: lax.dot_general(a, b, NT, preferred_element_type=F32, precision=lax.Precision.HIGHEST)
    for c in range(2):
        cut = slice(c * half, (c + 1) * half)
        lines = slice(c * half // shard, (c + 1) * half // shard)
        gains = vec[0:4, cut].T
        cross = tn_dot(flat(xg, cut), flat(mixes, everything))
        in_cross, up_cross = cross[:, :split], cross[:, split:]
        in_grad = gains[:, 0:1] * in_cross + gains[:, 1:2] * col_sums[:, :split]
        up_grad = gains[:, 2:3] * up_cross + gains[:, 3:4] * col_sums[:, split:]
        down_grad = tn_dot(flat(gg, cut), flat(act, everything))
        packed[lines, :, :split] = in_grad.astype(BF).reshape(-1, shard, split)
        packed[lines, :, split : split + ff] = up_grad.astype(BF).reshape(-1, shard, ff)
        packed[lines, :, split + ff :] = down_grad.astype(BF).reshape(-1, shard, ff)
        w_in = w[cut, :split].astype(F32)
        w_up = w[cut, split : split + ff].astype(F32)
        norm_rows = [
            exact(ones, w_in * in_cross)[0:1],
            exact(jnp.broadcast_to(col_sums[:, :split], (8, split)), w_in)[0:1],
            exact(wide, w_up * up_cross)[0:1],
            exact(jnp.broadcast_to(col_sums[:, split:], (8, ff)), w_up)[0:1],
        ]
        for i, line in enumerate(norm_rows):
            for j in range(half // 128):
                vrows[i * (width // 128) + c * (half // 128) + j] = line[:, j * 128 : (j + 1) * 128]
        part = tn_dot(flat(ctx, everything), flat(gg, cut)).astype(BF)
        out_grad[:, :, cut] = part.reshape(-1, shard, half)
    per = width // 128
    base = 4 * per

    def clear(i, carry):
        vrows[base + i] = jnp.zeros((1, 128), F32)
        return carry

    lax.fori_loop(0, vrows.shape[0] - base, clear, 0)
    step = local // 128
    for i in range(3):
        for j in range(step):
            vrows[base + i * per + tp * step + j] = col_sums[:, i * local + j * 128 : i * local + (j + 1) * 128]
    base = 8 * per
    for j in range(ff // 128):
        vrows[base + tp * (ff // 128) + j] = col_sums[:, split + j * 128 : split + (j + 1) * 128]
    bias = jnp.sum(grad_rows.astype(F32), axis=0, keepdims=True)
    for j in range(per):
        vrows[7 * per + j] = bias[:, j * 128 : (j + 1) * 128]
        vrows[12 * per + j] = bias[:, j * 128 : (j + 1) * 128]


def second_kernel(head_dim, lens, xown, gg, w, wo, vec, rot, hidden,
                  out, grad_next, packed, out_grad, vrows,
                  xg, work, mixes, act, ctx, sums, both, met, landed, both_e, met_e, landed_e,
                  loc, *sems):
    grp, tp = place()
    core, chip = tp // HALF, lax.rem(tp, HALF)
    local, ff = wo.shape[0], act.shape[2]
    swap = Exchange(both, met, landed, sems[0:4])
    swap_e = Exchange(both_e, met_e, landed_e, sems[4:8])
    gather = Gather(xown, xg, sems[8:12])
    greet_plane()
    gather.start(loc.at[0])
    sums[...] = jnp.zeros_like(sums)
    b_in, b_up = bias_slices(vec, tp, local, ff)

    def one(other, seq):
        part, mixed, probs, context, active, sl = seq_forward(
            work[other], lens[seq], head_dim, w, wo, vec, b_in, b_up, rot
        )
        ctx[seq] = context
        act[seq] = active
        back, mixed_grad, expanded_grad = seq_backward(
            gg[seq], mixed, probs, sl, head_dim, w, wo, vec, rot
        )
        mixes[seq, :, : 3 * local] = mixed_grad
        mixes[seq, :, 3 * local :] = expanded_grad
        sums[:, : 3 * local] += fold_rows(mixed_grad)
        sums[:, 3 * local :] += fold_rows(expanded_grad)
        return part, back

    for k in range(HALF):
        if k:
            gather.wait_block(k)
            swap_e.hand_over(k - 1)
            swap.hand_over(k - 1)
            gather.wait_passed(k)
        else:
            gather.wait_partner()
        block = across(chip, k)
        gather.settle(k, work)

        def part_of(other, carry):
            part, back = one(other, pick(core, other) * HALF + block)
            both[other, k] = part.astype(BF)
            both_e[other, k] = back.astype(BF)
            return carry

        lax.fori_loop(0, 2, part_of, 0)
        swap_e.to_partner(k).start()
        swap.to_partner(k).start()
    swap_e.hand_over(HALF - 1)
    swap.hand_over(HALF - 1)
    weight_grads(xg, gg, mixes, act, ctx, w, vec, sums, packed, out_grad, vrows, gg[tp], tp)
    swap_e.wait_landed()

    def finish_back(at):
        total = swap_e.total(at)
        centred, scale = norm_parts(hidden[at].astype(F32))
        xhat = centred * scale
        mean_one = jnp.mean(total, -1, keepdims=True)
        mean_two = jnp.mean(total * xhat, -1, keepdims=True)
        grad_next[at] = (
            gg[tp, at].astype(F32) + scale * (total - mean_one - xhat * mean_two)
        ).astype(BF)

    chunks(hidden.shape[0], finish_back)
    swap.wait_landed()

    def finish(at):
        out[at] = (hidden[at].astype(F32) + swap.total(at) + (vec[7:8] + vec[12:13])).astype(BF)

    chunks(hidden.shape[0], finish)
    gather.drain()
    swap.drain()
    swap_e.drain()


def second_layer(head_dim, owners, shard, lens, xown, gg, w, wo, vec, rot, hidden):
    seqs, rows, width = gg.shape
    local = wo.shape[0]
    ff = (w.shape[1] - 3 * local) // 2
    mix = 3 * local + ff
    dma = pltpu.SemaphoreType.DMA
    block = pltpu.VMEM((HALF, rows, width), BF)
    pair = pltpu.VMEM((2, HALF, rows, width), BF)
    return pl.pallas_call(
        functools.partial(second_kernel, head_dim),
        out_shape=[
            jax.ShapeDtypeStruct((rows, width), BF),
            jax.ShapeDtypeStruct((rows, width), BF),
            jax.ShapeDtypeStruct((width // shard, shard, w.shape[1]), BF),
            jax.ShapeDtypeStruct((owners, shard, width), BF),
            jax.ShapeDtypeStruct((13 * width // 128, 1, 128), F32),
        ],
        in_specs=[VMEM] * 8,
        out_specs=[VMEM] * 5,
        scratch_shapes=[
            pltpu.VMEM((seqs, rows, width), BF),
            pltpu.VMEM((2, rows, width), BF),
            pltpu.VMEM((seqs, rows, mix), BF),
            pltpu.VMEM((seqs, rows, ff), BF),
            pltpu.VMEM((seqs, rows, local), BF),
            pltpu.VMEM((8, mix), F32),
        ]
        + [pair, block, block] * 2
        + [dma((1,))]
        + [dma((HALF,))] * 12,
        compiler_params=pltpu.CompilerParams(
            collective_id=3, has_side_effects=True, vmem_limit_bytes=VMEM_BYTES
        ),
        name="second_layer",
    )(lens, xown, gg, w, wo, vec, rot, hidden)


def vector_rows(vec_part):
    step = 128
    while vec_part % step:
        step //= 2
    return (128 - step + vec_part + 127) // 128


def third_kernel(head_dim, groups, owners, gown, w, wo, vec, rot, tokens, xg,
                 qkv_h, prob_h, ctx_h, act_h, slope_h, packed1, out_grad1, vrows1,
                 out, r0, r1, ro, rv,
                 gg, work, mixes, sums, qkv, prob, ctx, act, slope, packed0, out_grad0, vrows0,
                 both, met, landed, loc, keep, ss, sr, os, orr, vs, vr, own_sem, *sems):
    grp, tp = place()
    me = grp * TP + tp
    total = groups * TP
    core, chip = tp // HALF, lax.rem(tp, HALF)
    local, ff = wo.shape[0], act.shape[2]
    swap = Exchange(both, met, landed, sems[0:4])
    gather = Gather(gown, gg, sems[4:8])
    kept = [(qkv_h, qkv), (prob_h, prob), (slope_h, slope), (act_h, act), (ctx_h, ctx)]
    rows_sent = rv.shape[2]
    vec_part = 13 * gown.shape[1] // total
    greet_all(groups)
    gather.start(loc.at[0])

    loads = [pltpu.make_async_copy(a, b, keep.at[i]) for i, (a, b) in enumerate(kept)]
    for copy in loads:
        copy.start()

    def to(step):
        other = lax.rem(me + step, total)
        return other // TP, lax.rem(other, TP), other

    def block_copy(layer, source, landing, step):
        g, t, other = to(step)
        return remote(source.at[other], landing.at[me], ss.at[layer, step], sr.at[layer, step], (g, t))

    def vec_copy(layer, source, step):
        g, t, other = to(step)
        first = (other * vec_part) // 128
        return remote(
            source.at[pl.ds(first, rows_sent)], rv.at[layer, me], vs.at[layer, step], vr.at[layer, step], (g, t)
        )

    def own_copies(layer, source, landing, vrows):
        first = (me * vec_part) // 128
        return [
            pltpu.make_async_copy(source.at[me], landing.at[me], own_sem.at[layer, 0]),
            pltpu.make_async_copy(vrows.at[pl.ds(first, rows_sent)], rv.at[layer, me], own_sem.at[layer, 1]),
        ]

    def out_copy(layer, source, j):
        owner = tp * owners + j
        return remote(
            source.at[j], ro.at[layer, grp], os.at[layer, j], orr.at[layer, grp], (owner // TP, lax.rem(owner, TP))
        )

    def send(layer, source, landing, out_grad, vrows):
        def start_all(step, carry):
            vec_copy(layer, vrows, step).start()
            block_copy(layer, source, landing, step).start()
            return carry

        lax.fori_loop(1, total, start_all, 0)
        for copy in own_copies(layer, source, landing, vrows):
            copy.start()
        for j in range(owners):
            owner = tp * owners + j

            @pl.when(owner != me)
            def _():
                out_copy(layer, out_grad, j).start()

            @pl.when(owner == me)
            def _():
                pltpu.make_async_copy(out_grad.at[j], ro.at[layer, grp], orr.at[layer, grp]).start()

    def collect(layer, source, landing, out_grad, vrows):
        def wait_all(step, carry):
            vec_copy(layer, vrows, step).wait()
            block_copy(layer, source, landing, step).wait()
            return carry

        lax.fori_loop(1, total, wait_all, 0)
        for copy in own_copies(layer, source, landing, vrows):
            copy.wait()
        for j in range(owners):
            owner = tp * owners + j

            @pl.when(owner != me)
            def _():
                out_copy(layer, out_grad, j).wait_send()

        for g in range(groups):
            pltpu.make_async_copy(out_grad.at[0], ro.at[layer, g], orr.at[layer, g]).wait()

    send(1, packed1, r1, out_grad1, vrows1)
    sums[...] = jnp.zeros_like(sums)
    for copy in loads[:3]:
        copy.wait()

    def one(other, seq):
        mixed = [qkv[seq, :, i * local : (i + 1) * local] for i in range(3)]
        probs = [prob[seq, h] for h in range(local // head_dim)]
        back, mixed_grad, expanded_grad = seq_backward(
            work[other], mixed, probs, slope[seq], head_dim, w, wo, vec, rot
        )
        mixes[seq, :, : 3 * local] = mixed_grad
        mixes[seq, :, 3 * local :] = expanded_grad
        sums[:, : 3 * local] += fold_rows(mixed_grad)
        sums[:, 3 * local :] += fold_rows(expanded_grad)
        return back

    for k in range(HALF):
        if k:
            gather.wait_block(k)
            swap.hand_over(k - 1)
            gather.wait_passed(k)
        else:
            gather.wait_partner()
        block = across(chip, k)
        gather.settle(k, work)

        def part_of(other, carry):
            both[other, k] = one(other, pick(core, other) * HALF + block).astype(BF)
            return carry

        lax.fori_loop(0, 2, part_of, 0)
        swap.to_partner(k).start()
    for copy in loads[3:]:
        copy.wait()
    weight_grads(xg, gg, mixes, act, ctx, w, vec, sums, packed0, out_grad0, vrows0, gg[tp], tp)
    send(0, packed0, r0, out_grad0, vrows0)
    swap.hand_over(HALF - 1)
    swap.wait_landed()

    def finish_back(at):
        value = swap.total(at)
        centred, scale = norm_parts(tokens[at].astype(F32))
        xhat = centred * scale
        mean_one = jnp.mean(value, -1, keepdims=True)
        mean_two = jnp.mean(value * xhat, -1, keepdims=True)
        out[at] = (gg[tp, at].astype(F32) + scale * (value - mean_one - xhat * mean_two)).astype(BF)

    chunks(tokens.shape[0], finish_back)
    gather.drain()
    swap.drain()
    collect(1, packed1, r1, out_grad1, vrows1)
    collect(0, packed0, r0, out_grad0, vrows0)


def third_layer(head_dim, groups, gown, w, wo, vec, rot, tokens, xg, kept, packed1, out_grad1, vrows1):
    seqs, rows, width = xg.shape
    local = wo.shape[0]
    ff = (w.shape[1] - 3 * local) // 2
    mix = 3 * local + ff
    total = groups * TP
    owners, shard = out_grad1.shape[:2]
    dma = pltpu.SemaphoreType.DMA
    block = pltpu.VMEM((HALF, rows, width), BF)
    pair = pltpu.VMEM((2, HALF, rows, width), BF)
    sent = vector_rows(13 * width // total)
    return pl.pallas_call(
        functools.partial(third_kernel, head_dim, groups, owners),
        out_shape=[
            jax.ShapeDtypeStruct((rows, width), BF),
            jax.ShapeDtypeStruct(packed1.shape, BF),
            jax.ShapeDtypeStruct(packed1.shape, BF),
            jax.ShapeDtypeStruct((LAYERS, groups, shard, width), BF),
            jax.ShapeDtypeStruct((LAYERS, total, sent, 1, 128), F32),
        ],
        in_specs=[VMEM] * 7 + [ANY] * 8,
        out_specs=[VMEM] + [ANY] * 4,
        scratch_shapes=[
            pltpu.VMEM((seqs, rows, width), BF),
            pltpu.VMEM((2, rows, width), BF),
            pltpu.VMEM((seqs, rows, mix), BF),
            pltpu.VMEM((8, mix), F32),
        ]
        + [pltpu.VMEM(a.shape, BF) for a in kept]
        + [pltpu.VMEM(packed1.shape, BF), pltpu.VMEM(out_grad1.shape, BF), pltpu.VMEM(vrows1.shape, F32)]
        + [pair, block, block]
        + [
            dma((1,)), dma((5,)), dma((LAYERS, total)), dma((LAYERS, total)),
            dma((LAYERS, owners)), dma((LAYERS, groups)), dma((LAYERS, total)), dma((LAYERS, total)),
            dma((LAYERS, 2)),
        ]
        + [dma((HALF,))] * 8,
        compiler_params=pltpu.CompilerParams(
            collective_id=4, has_side_effects=True, vmem_limit_bytes=VMEM_BYTES
        ),
        name="third_layer",
    )(gown, w, wo, vec, rot, tokens, xg, *kept, packed1, out_grad1, vrows1)


def adam_kernel(groups, local, ff, fixes, r0, r1, ro, *refs):
    params, moments, squares = refs[0:4], refs[4:8], refs[8:12]
    grads, changes, new_moments, new_squares = refs[12:16], refs[16:20], refs[20:24], refs[24:28]
    first_fix, second_fix = fixes[0], fixes[1]

    def update(which, at, gradient):
        moment = BETA_FIRST * moments[which][0, :, at] + (1.0 - BETA_FIRST) * gradient
        square = BETA_SECOND * squares[which][0, :, at] + (1.0 - BETA_SECOND) * gradient * gradient
        grads[which][0, :, at] = gradient
        new_moments[which][0, :, at] = moment
        new_squares[which][0, :, at] = square
        changes[which][0, :, at] = -LEARNING * (
            moment / first_fix / (jnp.sqrt(square / second_fix) + ADAM_EPSILON)
            + DECAY_RATE * params[which][0, :, at]
        )

    def layer(source):
        for p in range(TP):
            value = source[p].astype(F32)
            for g in range(1, groups):
                value = value + source[g * TP + p].astype(F32)
            for i in range(3):
                start = i * TP * local + p * local
                update(0, slice(start, start + local), value[:, i * local : (i + 1) * local])
            split = 3 * local
            at = slice(p * ff, (p + 1) * ff)
            update(2, at, value[:, split : split + ff])
            update(3, at, value[:, split + ff :])
        value = ro[0, 0].astype(F32)
        for g in range(1, groups):
            value = value + ro[0, g].astype(F32)
        update(1, slice(None), value)

    @pl.when(pl.program_id(0) == 0)
    def _():
        layer(r0)

    @pl.when(pl.program_id(0) == 1)
    def _():
        layer(r1)


def adam_step(groups, local, ff, fixes, r0, r1, ro, params, moments, squares):
    shard = ro.shape[2]
    part = 8
    specs = [pl.BlockSpec((1, part, a.shape[2]), lambda l, r: (l, r, 0)) for a in params]
    source = lambda layer: pl.BlockSpec(
        (r0.shape[0], part, r0.shape[2]), lambda l, r: (0, jnp.where(l == layer, r, (1 - layer) * (shard // part - 1)), 0)
    )
    outs = [jax.ShapeDtypeStruct(a.shape, F32) for a in params]
    return pl.pallas_call(
        functools.partial(adam_kernel, groups, local, ff),
        grid=(LAYERS, shard // part),
        in_specs=[SMEM, source(0), source(1), pl.BlockSpec((1, groups, part, ro.shape[3]), lambda l, r: (l, 0, r, 0))]
        + specs * 3,
        out_specs=specs * 4,
        out_shape=outs * 4,
        compiler_params=pltpu.CompilerParams(vmem_limit_bytes=VMEM_BYTES),
        name="adam_step",
    )(fixes, r0, r1, ro, *params, *moments, *squares)


def rotary(row_count, width, head_dim):
    rot_dim = head_dim // 4
    half_rot = rot_dim // 2
    column = jnp.arange(width, dtype=jnp.int32) % head_dim
    freq_slot = (column % half_rot).astype(F32)
    frequency = 10000.0 ** (-(freq_slot * 2.0) / rot_dim)
    angles = jnp.arange(row_count, dtype=F32)[:, None] * frequency[None, :]
    inside = (column < rot_dim)[None, :]
    first_half = (column < half_rot)[None, :]
    sine = jnp.sin(angles)
    return jnp.stack(
        [
            jnp.where(inside, jnp.cos(angles), 1.0),
            jnp.where(first_half, -sine, 0.0),
            jnp.where(inside & jnp.logical_not(first_half), sine, 0.0),
        ]
    )


def standard(values):
    centred = values - jnp.mean(values, -1, keepdims=True)
    return centred * lax.rsqrt(jnp.mean(centred * centred, -1, keepdims=True) + NORM_EPSILON)


def adam_update(weight, moment, square, gradient, first_fix, second_fix):
    moment = BETA_FIRST * moment + (1.0 - BETA_FIRST) * gradient
    square = BETA_SECOND * square + (1.0 - BETA_SECOND) * gradient * gradient
    change = -LEARNING * (
        moment / first_fix / (jnp.sqrt(square / second_fix) + ADAM_EPSILON) + DECAY_RATE * weight
    )
    return (change, moment, square)


def per_device(
    groups,
    tokens,
    cotangent,
    seq_lengths,
    seq_device,
    step_count,
    *state,
):
    params, moments, squares = state[0:5], state[5:10], state[10:15]
    attend_in, attend_out, expand_weight, reduce_weight, layer_vectors = params
    grp, tp = place()
    me = grp * TP + tp
    total = groups * TP
    rows, width = tokens.shape
    shard = attend_in.shape[1]
    head_dim = width // HEADS
    local = width // TP
    ff = expand_weight.shape[2] // TP
    vec_part = layer_vectors.shape[1]
    owners = local // shard
    plane_ids = grp * TP + jnp.arange(TP, dtype=jnp.int32)
    lens = jnp.sum(jnp.where(plane_ids[:, None] == seq_device[None, :], seq_lengths[None, :], 0), 1)
    lens = jnp.broadcast_to(lens[:, None, None], (TP, 1, rows))
    own_length = jnp.sum(jnp.where(seq_device == me, seq_lengths, 0))
    valid = jnp.arange(rows, dtype=jnp.int32)[:, None] < own_length
    rot = rotary(rows, local, head_dim)

    blocks = [
        jnp.concatenate(
            [
                attend_in[l].astype(BF).reshape(shard, 3, TP, local).transpose(2, 0, 1, 3).reshape(TP, shard, 3 * local),
                expand_weight[l].astype(BF).reshape(shard, TP, ff).transpose(1, 0, 2),
                reduce_weight[l].astype(BF).reshape(shard, TP, ff).transpose(1, 0, 2),
            ],
            2,
        )
        for l in range(LAYERS)
    ]
    vec = jnp.pad(layer_vectors.astype(BF).astype(F32).reshape(-1), (0, 8 * 128 - 2 * vec_part)).reshape(8, 128)
    xhat_own = standard(tokens.astype(F32)).astype(BF)
    grad_own = jnp.where(valid, cotangent, jnp.zeros_like(cotangent))
    grads_all = lax.all_gather(grad_own, "tp", axis=0)
    xg, w0, w1, wog, vecg = spread(groups, xhat_own, blocks[0], blocks[1], attend_out.astype(BF), vec)
    w1, grads_all = lax.optimization_barrier((w1, grads_all))
    w1 = lax.all_gather(w1, "grp", axis=0).reshape(width, -1)
    w0 = w0.reshape(width, -1)
    out_rows = wog.transpose(1, 0, 2, 3).reshape(LAYERS, local, width)
    vectors = vecg.reshape(total, -1)[:, : 2 * vec_part].reshape(total, LAYERS, vec_part)
    vectors = vectors.transpose(1, 0, 2).reshape(LAYERS, 13, width)
    vectors = jnp.pad(vectors, ((0, 0), (0, 3), (0, 0)))

    hidden0, xnext, *kept = first_layer(
        head_dim, lens, xg, w0, out_rows[0], vectors[0], rot, tokens
    )
    hidden1, grad0, packed1, out_grad1, vrows1 = second_layer(
        head_dim, owners, shard, lens, xnext, grads_all, w1, out_rows[1], vectors[1], rot, hidden0
    )
    input_grad, r0, r1, ro, rv = third_layer(
        head_dim, groups, grad0, w0, out_rows[0], vectors[0], rot, tokens, xg, kept, packed1, out_grad1, vrows1
    )
    step_float = step_count[0].astype(F32)
    first_fix = 1.0 - jnp.power(BETA_FIRST, step_float)
    second_fix = 1.0 - jnp.power(BETA_SECOND, step_float)
    big = adam_step(
        groups, local, ff, jnp.stack([first_fix, second_fix]), r0, r1, ro, params[:4], moments[:4], squares[:4]
    )
    vec_rows = jnp.sum(rv, 1).reshape(LAYERS, -1)
    grad_vec = lax.dynamic_slice_in_dim(vec_rows, lax.rem(me * vec_part, 128), vec_part, 1)
    small = (grad_vec,) + adam_update(params[4], moments[4], squares[4], grad_vec, first_fix, second_fix)
    results = []
    for i in range(4):
        results += list(big[4 * i : 4 * i + 4]) + [small[i]]
    return (jnp.stack([hidden0, hidden1]), input_grad, *results)


def solution(mesh):
    devices = mesh.devices.reshape(-1, TP)
    groups = devices.shape[0]
    flat = Mesh(devices, ("grp", "tp"))
    axes = ("grp", "tp")
    by_row = P(axes, None)
    by_dim = [P(None, axes, None)] * 4 + [P(None, axes)]
    return jax.shard_map(
        functools.partial(per_device, groups),
        mesh=flat,
        in_specs=(by_row, by_row, P(), P(), P(), *(by_dim * 3)),
        out_specs=(P(None, axes, None), by_row, *(by_dim * 4)),
        check_vma=False,
    )
```

```python
import functools

import jax
import jax.numpy as jnp
from jax import lax
from jax.experimental import pallas as pl
from jax.experimental.pallas import tpu as pltpu
from jax.sharding import Mesh
from jax.sharding import PartitionSpec as P

HEADS = 16
LAYERS = 2
NORM_EPSILON = 1e-05
ADAM_EPSILON = 1e-08
LEARNING = 0.02
BETA_FIRST = 0.9
BETA_SECOND = 0.95
DECAY_RATE = 0.1
MASKED_SCORE = -1e30

TP = 8
HALF = TP // 2
BF = jnp.bfloat16
F32 = jnp.float32
MESH = pl.DeviceIdType.MESH
NT = (((1,), (1,)), ((), ()))
TN = (((0,), (0,)), ((), ()))
ANY = pl.BlockSpec(memory_space=pl.ANY)
VMEM = pl.BlockSpec(memory_space=pltpu.VMEM)
SMEM = pl.BlockSpec(memory_space=pltpu.SMEM)
VMEM_BYTES = 67043328


AXES = ("far", "near", "core", "y", "x")


class Place:
    def __init__(self):
        self.far, near, core, self.y, x = (lax.axis_index(name) for name in AXES)
        self.fars, self.ys = lax.axis_size("far"), lax.axis_size("y")
        self.tp = core * HALF + near * 2 + x
        self.row = near * 2 + core
        self.x = x
        self.core, self.chip = core, near * 2 + x
        self.partner = (1 - core) * HALF + self.chip
        self.groups, self.total = self.fars * self.ys, self.fars * self.ys * TP
        self.me = self.flat(self.far, self.y, self.tp)

    def flat(self, far, y, tp):
        near, core, x = lax.rem(tp // 2, 2), tp // HALF, lax.rem(tp, 2)
        return (((far * 2 + near) * 2 + core) * self.ys + y) * 2 + x

    def device(self, tp, far=None, y=None):
        far = self.far if far is None else far
        y = self.y if y is None else y
        return far, lax.rem(tp // 2, 2), tp // HALF, y, lax.rem(tp, 2)

    def device_of(self, flat):
        rest = flat // 2
        y, rest = lax.rem(rest, self.ys), rest // self.ys
        core, rest = lax.rem(rest, 2), rest // 2
        return rest // 2, lax.rem(rest, 2), core, y, lax.rem(flat, 2)

    def tp_of(self, row, x):
        return (row % 2) * HALF + (row // 2) * 2 + x


def nn_dot(a, b):
    return jnp.dot(a, b, preferred_element_type=F32)


def nt_dot(a, b):
    return lax.dot_general(a, b, NT, preferred_element_type=F32)


def tn_dot(a, b):
    return lax.dot_general(a, b, TN, preferred_element_type=F32)


def remote(src, dst, send, recv, target):
    return pltpu.make_async_remote_copy(
        src_ref=src, dst_ref=dst, send_sem=send, recv_sem=recv, device_id=target, device_id_type=MESH
    )


def greet(targets):
    barrier = pltpu.get_barrier_semaphore()
    for target in targets:
        pl.semaphore_signal(barrier, inc=1, device_id=target, device_id_type=MESH)
    pl.semaphore_wait(barrier, len(targets))


def greet_all(here):
    barrier = pltpu.get_barrier_semaphore()

    def signal(step, carry):
        other = lax.rem(here.me + step, here.total)
        pl.semaphore_signal(barrier, inc=1, device_id=here.device_of(other), device_id_type=MESH)
        return carry

    lax.fori_loop(1, here.total, signal, 0)
    pl.semaphore_wait(barrier, here.total - 1)


def spread_kernel(owners, xh, s0, s1, wo, vec, xg, w0, w1, wog, vecg,
                  ps, pr, zs, zr, ys, yr, os, orr, vs, vr, loc, *sems):
    here = Place()
    far, y, tp, row, x = here.far, here.y, here.tp, here.row, here.x
    gather_x = Gather(here, xh, xg, sems[0:4])
    layers = ((s0, w0), (s1, w1))
    greet_all(here)

    def within(l, step):
        source, w = layers[l]
        peer = lax.rem(tp + step, TP)
        return remote(
            source.at[peer], w.at[far, row, y, x], ps.at[l, step], pr.at[l, tp], here.device(peer)
        )

    def start_layer(l):
        source, w = layers[l]
        for step in range(1, TP):
            within(l, step).start()
        pltpu.make_async_copy(source.at[tp], w.at[far, row, y, x], pr.at[l, tp]).start()

    def vec_copy(step):
        other = lax.rem(here.me + step, here.total)
        return remote(vec, vecg.at[here.me], vs.at[step], vr.at[step], here.device_of(other))

    def start_vec(step, carry):
        vec_copy(step).start()
        return carry

    def wait_vec(step, carry):
        vec_copy(step).wait()
        return carry

    start_layer(0)
    start_layer(1)
    lax.fori_loop(1, here.total, start_vec, 0)
    own_vec = pltpu.make_async_copy(vec, vecg.at[here.me], loc.at[1])
    own_vec.start()
    slot = lax.rem(here.me, owners)
    user = here.me // owners

    def out_copy(f, v):
        return remote(wo, wog.at[slot], os.at[f, v], orr.at[slot], here.device(user, f, v))

    def is_own(f, v):
        return (user == tp) & (f == far) & (v == y)

    blocks = [(f, v) for f in range(here.fars) for v in range(here.ys)]
    for f, v in blocks:

        @pl.when(jnp.logical_not(is_own(f, v)))
        def _():
            out_copy(f, v).start()

        @pl.when(is_own(f, v))
        def _():
            pltpu.make_async_copy(wo, wog.at[slot], orr.at[slot]).start()

    def along_far(l, i, r):
        part = layers[l][1].at[far, r, y]
        target = lax.rem(far + i, here.fars)
        return remote(part, part, zs.at[l, i, r], zr.at[l, i, r], here.device(tp, far=target))

    def along_y(l, j, i, r):
        part = layers[l][1].at[lax.rem(far + here.fars - i, here.fars), r, y]
        target = lax.rem(y + j, here.ys)
        return remote(part, part, ys.at[l, j, i, r], yr.at[l, j, i, r], here.device(tp, y=target))

    def landed(l, f, r, v, sem):
        part = layers[l][1].at[f, r, v]
        remote(part, part, sem, sem, here.device(here.partner)).wait_recv()

    def first_hop(l):
        source, w = layers[l]
        for r in range(HALF):
            for side in range(2):
                t = here.tp_of(r, side)
                pltpu.make_async_copy(source.at[0], w.at[far, r, y, side], pr.at[l, t]).wait()
            for i in range(1, here.fars):
                along_far(l, i, r).start()
            for j in range(1, here.ys):
                along_y(l, j, 0, r).start()

    first_hop(0)
    first_hop(1)
    gather_x.start(loc.at[0])
    for l in range(LAYERS):
        for r in range(HALF):
            for i in range(1, here.fars):
                landed(l, lax.rem(far + here.fars - i, here.fars), r, y, zr.at[l, i, r])
                for j in range(1, here.ys):
                    along_y(l, j, i, r).start()
    for k in range(1, HALF):
        gather_x.wait_block(k)
    gather_x.wait_partner()
    for k in range(1, HALF):
        gather_x.wait_passed(k)
    for l in range(LAYERS):
        for j in range(1, here.ys):
            for i in range(here.fars):
                for r in range(HALF):
                    landed(
                        l, lax.rem(far + here.fars - i, here.fars), r, lax.rem(y + here.ys - j, here.ys),
                        yr.at[l, j, i, r],
                    )
    lax.fori_loop(1, here.total, wait_vec, 0)
    own_vec.wait()
    for j in range(owners):
        pltpu.make_async_copy(wo, wog.at[j], orr.at[j]).wait()
    gather_x.drain()
    for l in range(LAYERS):
        for step in range(1, TP):
            within(l, step).wait_send()
        for r in range(HALF):
            for i in range(1, here.fars):
                along_far(l, i, r).wait_send()
            for j in range(1, here.ys):
                for i in range(here.fars):
                    along_y(l, j, i, r).wait_send()
    for f, v in blocks:

        @pl.when(jnp.logical_not(is_own(f, v)))
        def _():
            out_copy(f, v).wait_send()


def spread(here, xh, s0, s1, wo, vec):
    rows, cols = s0.shape[1:]
    owners = wo.shape[2] // TP // rows
    dma = pltpu.SemaphoreType.DMA
    whole = jax.ShapeDtypeStruct((here.fars, HALF, here.ys, 2, rows, cols), BF)
    gathered = jax.ShapeDtypeStruct((TP,) + xh.shape, BF)
    return pl.pallas_call(
        functools.partial(spread_kernel, owners),
        out_shape=(
            gathered,
            whole,
            whole,
            jax.ShapeDtypeStruct((owners,) + wo.shape, BF),
            jax.ShapeDtypeStruct((here.total,) + vec.shape, F32),
        ),
        in_specs=[VMEM] + [ANY] * 4,
        out_specs=(ANY,) * 5,
        scratch_shapes=[
            dma((LAYERS, TP)), dma((LAYERS, TP)),
            dma((LAYERS, here.fars, HALF)), dma((LAYERS, here.fars, HALF)),
            dma((LAYERS, here.ys, here.fars, HALF)), dma((LAYERS, here.ys, here.fars, HALF)),
            dma((here.fars, here.ys)), dma((owners,)), dma((here.total,)), dma((here.total,)), dma((2,)),
        ]
        + [dma((HALF,))] * 4,
        compiler_params=pltpu.CompilerParams(collective_id=1, has_side_effects=True),
        name="spread",
    )(xh, s0, s1, wo, vec)


def turn(values, rot):
    return (
        values * rot[0]
        + pltpu.roll(values, values.shape[1] - 8, 1) * rot[1]
        + pltpu.roll(values, 8, 1) * rot[2]
    )


def turn_back(values, rot):
    return (
        values * rot[0]
        + pltpu.roll(values * rot[1], 8, 1)
        + pltpu.roll(values * rot[2], values.shape[1] - 8, 1)
    )


def head_parts(values, head_dim):
    lane = lax.broadcasted_iota(jnp.int32, values.shape, 1)
    zero = jnp.zeros_like(values)
    return [
        jnp.where((lane >= h * head_dim) & (lane < (h + 1) * head_dim), values, zero)
        for h in range(values.shape[1] // head_dim)
    ]


def bias_slices(vec, tp, local, ff):
    width = vec.shape[1]
    b_in = vec[4:7, pl.ds(pl.multiple_of(tp * local, local), local)]
    per_row = width // ff
    row = 8 + tp // per_row
    b_up = vec[pl.ds(row, 1), pl.ds(pl.multiple_of(lax.rem(tp, per_row) * ff, ff), ff)]
    return b_in, b_up


def seq_forward(values, lengths, head_dim, w, wo, vec, b_in, b_up, rot):
    rows = values.shape[0]
    local = wo.shape[0]
    ff = b_up.shape[1]
    values = values.astype(F32)
    normed = (values * vec[0:1] + vec[1:2]).astype(BF)
    mixed = nn_dot(normed, w[:, : 3 * local])
    parts = [mixed[:, i * local : (i + 1) * local] + b_in[i : i + 1] for i in range(3)]
    queries = (turn(parts[0], rot).astype(BF).astype(F32) * head_dim ** (-0.5)).astype(BF)
    keys = turn(parts[1], rot).astype(BF)
    vals = parts[2].astype(BF)
    row = lax.broadcasted_iota(jnp.int32, (rows, rows), 0)
    col = lax.broadcasted_iota(jnp.int32, (rows, rows), 1)
    allowed = (col <= row) & (col < lengths)
    total, probs = None, []
    for q_h, v_h in zip(head_parts(queries, head_dim), head_parts(vals, head_dim)):
        scores = jnp.where(allowed, nt_dot(q_h, keys), MASKED_SCORE)
        weights = jnp.exp(scores - jnp.max(scores, -1, keepdims=True))
        probability = (weights / jnp.sum(weights, -1, keepdims=True)).astype(BF)
        probs.append(probability)
        term = nn_dot(probability, v_h)
        total = term if total is None else total + term
    context = total.astype(BF)
    normed = (values * vec[2:3] + vec[3:4]).astype(BF)
    expanded = nn_dot(normed, w[:, 3 * local : 3 * local + ff]) + b_up
    spread_to = 0.5 * (1.0 + lax.erf(expanded * 0.7071067811865476))
    active = (expanded * spread_to).astype(BF)
    slope = (spread_to + expanded * (0.3989422804014327 * jnp.exp(-0.5 * expanded * expanded))).astype(BF)
    part = nn_dot(context, wo[...]) + nt_dot(active, w[:, 3 * local + ff :])
    return part, (queries, keys, vals), probs, context, active, slope


def seq_backward(grad, qkv, probs, slope, head_dim, w, wo, vec, rot):
    local = wo.shape[0]
    ff = slope.shape[1]
    queries, keys, vals = qkv
    active_grad = nn_dot(grad, w[:, 3 * local + ff :])
    expanded_grad = (slope.astype(F32) * active_grad).astype(BF)
    total = nt_dot(expanded_grad, w[:, 3 * local : 3 * local + ff]) * vec[2:3]
    context_grad = nt_dot(grad, wo[...]).astype(BF)
    query_grad = key_grad = value_grad = 0.0
    for prob_b, c_h, q_h, k_h in zip(
        probs, head_parts(context_grad, head_dim), head_parts(queries, head_dim), head_parts(keys, head_dim)
    ):
        probability = prob_b.astype(F32)
        prob_grad = nt_dot(c_h, vals)
        value_grad = value_grad + tn_dot(prob_b, c_h)
        inner = jnp.sum(probability * prob_grad, -1, keepdims=True)
        score_grad = (probability * (prob_grad - inner)).astype(BF)
        query_grad = query_grad + nn_dot(score_grad, k_h)
        key_grad = key_grad + tn_dot(score_grad, q_h)
    query_grad = query_grad * head_dim ** (-0.5)
    pieces = [turn_back(query_grad, rot).astype(BF), turn_back(key_grad, rot).astype(BF), value_grad.astype(BF)]
    mixed_grad = jnp.concatenate(pieces, 1)
    total = total + nt_dot(mixed_grad, w[:, : 3 * local]) * vec[0:1]
    return total, mixed_grad, expanded_grad


def fold_rows(values):
    return jnp.sum(values.astype(F32).reshape(-1, 8, values.shape[1]), axis=0)


def across(chip, step):
    x = lax.rem(lax.rem(chip, 2) + lax.rem(step, 2), 2)
    y = lax.rem(chip // 2 + step // 2, 2)
    return 2 * y + x


def pick(core, other):
    return core + (1 - 2 * core) * other


CHUNK = 32


def chunks(rows, body):
    def step(i, carry):
        body(pl.ds(pl.multiple_of(i * CHUNK, CHUNK), CHUNK))
        return carry

    lax.fori_loop(0, rows // CHUNK, step, 0)


def norm_parts(values):
    centred = values - jnp.mean(values, -1, keepdims=True)
    return centred, lax.rsqrt(jnp.mean(centred * centred, -1, keepdims=True) + NORM_EPSILON)


class Exchange:
    def __init__(self, here, both, met, landed, sems):
        self.here = here
        self.joined, self.mine, self.met, self.landed = both.at[0], both.at[1], met, landed
        self.ps, self.pr, self.bs, self.br = sems
        self.core, self.chip, self.partner = here.core, here.chip, here.partner

    def to_partner(self, k):
        return remote(
            self.mine.at[k], self.met.at[k], self.ps.at[k], self.pr.at[k], self.here.device(self.partner)
        )

    def to_owner(self, k):
        owner = self.core * HALF + across(self.chip, k)
        return remote(
            self.joined.at[k], self.landed.at[k], self.bs.at[k], self.br.at[k], self.here.device(owner)
        )

    def join(self, k):
        self.to_partner(k).wait_recv()

        def add(at):
            self.joined[k, at] = (self.joined[k, at].astype(F32) + self.met[k, at].astype(F32)).astype(BF)

        chunks(self.met.shape[1], add)

    def hand_over(self, k):
        self.join(k)
        if k:
            self.to_owner(k).start()

    def total(self, at):
        value = self.joined[0, at].astype(F32)
        for k in range(1, HALF):
            value = value + self.landed[k, at].astype(F32)
        return value

    def wait_landed(self):
        for k in range(1, HALF):
            self.to_owner(k).wait_recv()

    def drain(self):
        for k in range(HALF):
            self.to_partner(k).wait_send()
        for k in range(1, HALF):
            self.to_owner(k).wait_send()


class Gather:
    def __init__(self, here, own, buffer, sems):
        self.here, self.own, self.buffer = here, own, buffer
        self.gs, self.gr, self.fs, self.fr = sems
        self.tp, self.core, self.chip, self.partner = here.tp, here.core, here.chip, here.partner

    def to_peer(self, k):
        if isinstance(k, int) and k == 0:
            target = self.partner
        else:
            target = self.core * HALF + across(self.chip, k)
        return remote(self.own, self.buffer.at[self.tp], self.gs.at[k], self.gr.at[k], self.here.device(target))

    def start(self, local):
        pltpu.make_async_copy(self.own, self.buffer.at[self.tp], local).start()
        for k in (1, 2, 3, 0):
            self.to_peer(k).start()
        pltpu.make_async_copy(self.own, self.buffer.at[self.tp], local).wait()

    def pass_on(self, k):
        source = self.core * HALF + across(self.chip, k)
        block = self.buffer.at[source]
        return remote(block, block, self.fs.at[k], self.fr.at[k], self.here.device(self.partner))

    def arrived(self, source, sem):
        block = self.buffer.at[source]
        remote(block, block, sem, sem, self.here.device(self.partner)).wait_recv()

    def wait_block(self, k):
        self.arrived(self.core * HALF + across(self.chip, k), self.gr.at[k])
        self.pass_on(k).start()

    def wait_partner(self):
        self.arrived(self.partner, self.gr.at[0])

    def wait_passed(self, k):
        self.arrived((1 - self.core) * HALF + across(self.chip, k), self.fr.at[k])

    def settle(self, k, work):
        block = across(self.chip, k)
        for other in range(2):
            work[other] = self.buffer[pick(self.core, other) * HALF + block]

    def drain(self):
        for k in range(HALF):
            self.to_peer(k).wait_send()
        for k in range(1, HALF):
            self.pass_on(k).wait_send()


def greet_block(here):
    targets = [here.partner] + [here.core * HALF + across(here.chip, k) for k in range(1, HALF)]
    greet([here.device(target) for target in targets])


def first_kernel(head_dim, lens, xg, w, wo, vec, rot, own, gr,
                 out, xnext, gg, qkv_h, prob_h, ctx_h, act_h, slope_h,
                 qkv, prob, ctx, act, slope, both, met, landed, keep, *sems):
    here = Place()
    tp, core, chip = here.tp, here.core, here.chip
    local, ff = wo.shape[0], act.shape[2]
    swap = Exchange(here, both, met, landed, sems[0:4])
    gather = Gather(here, gr, gg, sems[4:8])
    kept = [(qkv, qkv_h), (prob, prob_h), (ctx, ctx_h), (act, act_h), (slope, slope_h)]
    greet_block(here)
    b_in, b_up = bias_slices(vec, tp, local, ff)

    def one(seq):
        part, mixed, probs, context, active, sl = seq_forward(
            xg[seq], lens[seq], head_dim, w, wo, vec, b_in, b_up, rot
        )
        for i, piece in enumerate(mixed):
            qkv[seq, :, i * local : (i + 1) * local] = piece
        for h, p in enumerate(probs):
            prob[seq, h] = p
        ctx[seq] = context
        act[seq] = active
        slope[seq] = sl
        return part

    for k in reversed(range(HALF)):
        block = across(chip, k)

        def part_of(other, carry):
            both[other, k] = one(pick(core, other) * HALF + block).astype(BF)
            return carry

        lax.fori_loop(0, 2, part_of, 0)
        swap.to_partner(k).start()
        if k + 1 < HALF:
            swap.hand_over(k + 1)
        if k == 0:
            gather.start(keep.at[5])
    swap.hand_over(0)
    saved = [pltpu.make_async_copy(a, b, keep.at[i]) for i, (a, b) in enumerate(kept)]
    for copy in saved:
        copy.start()
    for k in range(1, HALF):
        gather.wait_block(k)
    swap.wait_landed()

    def finish(at):
        result = (own[at].astype(F32) + swap.total(at) + (vec[7:8] + vec[12:13])).astype(BF)
        out[at] = result
        centred, scale = norm_parts(result.astype(F32))
        xnext[at] = (centred * scale).astype(BF)

    chunks(own.shape[0], finish)
    gather.wait_partner()
    for k in range(1, HALF):
        gather.wait_passed(k)
    gather.drain()
    swap.drain()
    for copy in saved:
        copy.wait()


def first_layer(head_dim, lens, xg, w, wo, vec, rot, own, gr):
    seqs, rows, width = xg.shape
    local = wo.shape[0]
    ff = (w.shape[1] - 3 * local) // 2
    dma = pltpu.SemaphoreType.DMA
    kept = [
        (seqs, rows, 3 * local), (seqs, local // head_dim, rows, rows), (seqs, rows, local), (seqs, rows, ff),
        (seqs, rows, ff),
    ]
    block = pltpu.VMEM((HALF, rows, width), BF)
    pair = pltpu.VMEM((2, HALF, rows, width), BF)
    return pl.pallas_call(
        functools.partial(first_kernel, head_dim),
        out_shape=[jax.ShapeDtypeStruct((rows, width), BF)] * 2
        + [jax.ShapeDtypeStruct(s, BF) for s in [xg.shape] + kept],
        in_specs=[VMEM] * 8,
        out_specs=[VMEM] * 2 + [ANY] * 6,
        scratch_shapes=[pltpu.VMEM(s, BF) for s in kept] + [pair, block, block] + [dma((6,))] + [dma((HALF,))] * 8,
        compiler_params=pltpu.CompilerParams(
            collective_id=2, has_side_effects=True, vmem_limit_bytes=VMEM_BYTES
        ),
        name="first_layer",
    )(lens, xg, w, wo, vec, rot, own, gr)


def weight_grads(xg, gg, mixes, act, ctx, w, vec, sums, packed, out_grad, vrows, grad_rows, tp):
    local, width = out_grad.shape[0] * out_grad.shape[1], out_grad.shape[2]
    fars, _, ys, _, shard, cols = packed.shape
    ff = act.shape[2]
    split = 3 * local
    rows = xg.shape[0] * xg.shape[1]
    flat = lambda ref, cut: ref[:, :, cut].reshape(rows, -1)
    everything = slice(None)
    col_sums = jnp.sum(sums[...], axis=0, keepdims=True)
    half = width // 2
    ones = jnp.ones((8, split), F32)
    wide = jnp.ones((8, ff), F32)
    exact = lambda a, b: lax.dot_general(a, b, NT, preferred_element_type=F32, precision=lax.Precision.HIGHEST)
    for c in range(2):
        cut = slice(c * half, (c + 1) * half)
        lines = slice(c * fars // 2, (c + 1) * fars // 2)
        shape = (fars // 2, HALF, ys, 2, shard)
        gains = vec[0:4, cut].T
        cross = tn_dot(flat(xg, cut), flat(mixes, everything))
        in_cross, up_cross = cross[:, :split], cross[:, split:]
        in_grad = gains[:, 0:1] * in_cross + gains[:, 1:2] * col_sums[:, :split]
        up_grad = gains[:, 2:3] * up_cross + gains[:, 3:4] * col_sums[:, split:]
        down_grad = tn_dot(flat(gg, cut), flat(act, everything))
        packed[lines, :, :, :, :, :split] = in_grad.astype(BF).reshape(shape + (split,))
        packed[lines, :, :, :, :, split : split + ff] = up_grad.astype(BF).reshape(shape + (ff,))
        packed[lines, :, :, :, :, split + ff :] = down_grad.astype(BF).reshape(shape + (ff,))
        w_in = w[cut, :split].astype(F32)
        w_up = w[cut, split : split + ff].astype(F32)
        norm_rows = [
            exact(ones, w_in * in_cross)[0:1],
            exact(jnp.broadcast_to(col_sums[:, :split], (8, split)), w_in)[0:1],
            exact(wide, w_up * up_cross)[0:1],
            exact(jnp.broadcast_to(col_sums[:, split:], (8, ff)), w_up)[0:1],
        ]
        for i, line in enumerate(norm_rows):
            for j in range(half // 128):
                vrows[i * (width // 128) + c * (half // 128) + j] = line[:, j * 128 : (j + 1) * 128]
        part = tn_dot(flat(ctx, everything), flat(gg, cut)).astype(BF)
        out_grad[:, :, cut] = part.reshape(-1, shard, half)
    per = width // 128
    base = 4 * per

    def clear(i, carry):
        vrows[base + i] = jnp.zeros((1, 128), F32)
        return carry

    lax.fori_loop(0, vrows.shape[0] - base, clear, 0)
    step = local // 128
    for i in range(3):
        for j in range(step):
            vrows[base + i * per + tp * step + j] = col_sums[:, i * local + j * 128 : i * local + (j + 1) * 128]
    base = 8 * per
    for j in range(ff // 128):
        vrows[base + tp * (ff // 128) + j] = col_sums[:, split + j * 128 : split + (j + 1) * 128]
    bias = jnp.sum(grad_rows.astype(F32), axis=0, keepdims=True)
    for j in range(per):
        vrows[7 * per + j] = bias[:, j * 128 : (j + 1) * 128]
        vrows[12 * per + j] = bias[:, j * 128 : (j + 1) * 128]


def second_kernel(head_dim, lens, xown, gg, w, wo, vec, rot, hidden,
                  out, grad_next, packed, out_grad, vrows,
                  xg, work, mixes, act, ctx, sums, both, met, landed, both_e, met_e, landed_e,
                  loc, *sems):
    here = Place()
    tp, core, chip = here.tp, here.core, here.chip
    local, ff = wo.shape[0], act.shape[2]
    swap = Exchange(here, both, met, landed, sems[0:4])
    swap_e = Exchange(here, both_e, met_e, landed_e, sems[4:8])
    gather = Gather(here, xown, xg, sems[8:12])
    greet_block(here)
    gather.start(loc.at[0])
    sums[...] = jnp.zeros_like(sums)
    b_in, b_up = bias_slices(vec, tp, local, ff)

    def one(other, seq):
        part, mixed, probs, context, active, sl = seq_forward(
            work[other], lens[seq], head_dim, w, wo, vec, b_in, b_up, rot
        )
        ctx[seq] = context
        act[seq] = active
        back, mixed_grad, expanded_grad = seq_backward(
            gg[seq], mixed, probs, sl, head_dim, w, wo, vec, rot
        )
        mixes[seq, :, : 3 * local] = mixed_grad
        mixes[seq, :, 3 * local :] = expanded_grad
        sums[:, : 3 * local] += fold_rows(mixed_grad)
        sums[:, 3 * local :] += fold_rows(expanded_grad)
        return part, back

    for k in range(HALF):
        if k:
            gather.wait_block(k)
            swap_e.hand_over(k - 1)
            swap.hand_over(k - 1)
            gather.wait_passed(k)
        else:
            gather.wait_partner()
        block = across(chip, k)
        gather.settle(k, work)

        def part_of(other, carry):
            part, back = one(other, pick(core, other) * HALF + block)
            both[other, k] = part.astype(BF)
            both_e[other, k] = back.astype(BF)
            return carry

        lax.fori_loop(0, 2, part_of, 0)
        swap_e.to_partner(k).start()
        swap.to_partner(k).start()
    swap_e.hand_over(HALF - 1)
    swap.hand_over(HALF - 1)
    weight_grads(xg, gg, mixes, act, ctx, w, vec, sums, packed, out_grad, vrows, gg[tp], tp)
    swap_e.wait_landed()

    def finish_back(at):
        total = swap_e.total(at)
        centred, scale = norm_parts(hidden[at].astype(F32))
        xhat = centred * scale
        mean_one = jnp.mean(total, -1, keepdims=True)
        mean_two = jnp.mean(total * xhat, -1, keepdims=True)
        grad_next[at] = (
            gg[tp, at].astype(F32) + scale * (total - mean_one - xhat * mean_two)
        ).astype(BF)

    chunks(hidden.shape[0], finish_back)
    swap.wait_landed()

    def finish(at):
        out[at] = (hidden[at].astype(F32) + swap.total(at) + (vec[7:8] + vec[12:13])).astype(BF)

    chunks(hidden.shape[0], finish)
    gather.drain()
    swap.drain()
    swap_e.drain()


def second_layer(here, head_dim, owners, shard, lens, xown, gg, w, wo, vec, rot, hidden):
    seqs, rows, width = gg.shape
    local = wo.shape[0]
    ff = (w.shape[1] - 3 * local) // 2
    mix = 3 * local + ff
    dma = pltpu.SemaphoreType.DMA
    block = pltpu.VMEM((HALF, rows, width), BF)
    pair = pltpu.VMEM((2, HALF, rows, width), BF)
    return pl.pallas_call(
        functools.partial(second_kernel, head_dim),
        out_shape=[
            jax.ShapeDtypeStruct((rows, width), BF),
            jax.ShapeDtypeStruct((rows, width), BF),
            jax.ShapeDtypeStruct((here.fars, HALF, here.ys, 2, shard, w.shape[1]), BF),
            jax.ShapeDtypeStruct((owners, shard, width), BF),
            jax.ShapeDtypeStruct((13 * width // 128, 1, 128), F32),
        ],
        in_specs=[VMEM] * 8,
        out_specs=[VMEM] * 5,
        scratch_shapes=[
            pltpu.VMEM((seqs, rows, width), BF),
            pltpu.VMEM((2, rows, width), BF),
            pltpu.VMEM((seqs, rows, mix), BF),
            pltpu.VMEM((seqs, rows, ff), BF),
            pltpu.VMEM((seqs, rows, local), BF),
            pltpu.VMEM((8, mix), F32),
        ]
        + [pair, block, block] * 2
        + [dma((1,))]
        + [dma((HALF,))] * 12,
        compiler_params=pltpu.CompilerParams(
            collective_id=3, has_side_effects=True, vmem_limit_bytes=VMEM_BYTES
        ),
        name="second_layer",
    )(lens, xown, gg, w, wo, vec, rot, hidden)


def vector_rows(vec_part):
    step = 128
    while vec_part % step:
        step //= 2
    return (128 - step + vec_part + 127) // 128


class Owners:
    def __init__(self, here, packed, from_y, acc, from_far, out, sems):
        self.here, self.packed, self.from_y, self.acc, self.from_far, self.out = (
            here, packed, from_y, acc, from_far, out
        )
        self.ys, self.yr, self.zs, self.zr, self.ps, self.pr = sems

    def line(self, i):
        return lax.rem(self.here.far + i, self.here.fars)

    def to_y(self, j, i, r):
        here = self.here
        y = lax.rem(here.y + j, here.ys)
        return remote(
            self.packed.at[self.line(i), r, y], self.from_y.at[j - 1, i, r],
            self.ys.at[j, i, r], self.yr.at[j, i, r], here.device(here.tp, y=y),
        )

    def to_far(self, i, r):
        here = self.here
        return remote(
            self.acc.at[i, r], self.from_far.at[i - 1, r], self.zs.at[i, r], self.zr.at[i, r],
            here.device(here.tp, far=self.line(i)),
        )

    def start(self):
        for i in list(range(1, self.here.fars)) + [0]:
            for r in range(HALF):
                for j in range(1, self.here.ys):
                    self.to_y(j, i, r).start()

    def add(self, i, r):
        here = self.here
        value = self.packed[self.line(i), r, here.y].astype(F32)
        for j in range(1, here.ys):
            self.to_y(j, i, r).wait_recv()
            value = value + self.from_y[j - 1, i, r].astype(F32)
        if i == 0:
            for far in range(1, here.fars):
                self.to_far(far, r).wait_recv()
                value = value + self.from_far[far - 1, r].astype(F32)
        self.acc[i, r] = value.astype(BF)

    def pass_far(self):
        for i in range(1, self.here.fars):
            for r in range(HALF):
                self.add(i, r)
                self.to_far(i, r).start()

    def to_owner(self, r, x):
        here = self.here
        return remote(
            self.acc.at[0, r, x], self.out.at[here.tp], self.ps.at[r, x], self.pr.at[here.tp],
            here.device(here.tp_of(r, x)),
        )

    def hand_out(self):
        here = self.here
        for r in range(HALF):
            self.add(0, r)
            for x in range(2):
                own = here.tp == here.tp_of(r, x)

                @pl.when(jnp.logical_not(own))
                def _():
                    self.to_owner(r, x).start()

                @pl.when(own)
                def _():
                    pltpu.make_async_copy(self.acc.at[0, r, x], self.out.at[here.tp], self.pr.at[here.tp]).start()

    def drain(self):
        here = self.here
        for source in range(TP):
            pltpu.make_async_copy(self.acc.at[0, 0, 0], self.out.at[source], self.pr.at[source]).wait()
        for r in range(HALF):
            for i in range(here.fars):
                for j in range(1, here.ys):
                    self.to_y(j, i, r).wait_send()
                if i:
                    self.to_far(i, r).wait_send()
            for x in range(2):

                @pl.when(here.tp != here.tp_of(r, x))
                def _():
                    self.to_owner(r, x).wait_send()


def third_kernel(head_dim, owners, gown, w, wo, vec, rot, tokens, xg, packed1,
                 qkv_h, prob_h, ctx_h, act_h, slope_h, out_grad1, vrows1,
                 out, r0, r1, ro, rv,
                 gg, work, mixes, sums, qkv, prob, ctx, act, slope, packed0, out_grad0, vrows0,
                 both, met, landed, from_y0, acc0, from_far0, from_y1, acc1, from_far1,
                 loc, keep, os, orr, vs, vr, own_sem, *sems):
    here = Place()
    tp, core, chip, me, total = here.tp, here.core, here.chip, here.me, here.total
    local, ff = wo.shape[0], act.shape[2]
    swap = Exchange(here, both, met, landed, sems[0:4])
    gather = Gather(here, gown, gg, sems[4:8])
    settle0 = Owners(here, packed0, from_y0, acc0, from_far0, r0, sems[8:14])
    settle1 = Owners(here, packed1, from_y1, acc1, from_far1, r1, sems[14:20])
    kept = [(qkv_h, qkv), (prob_h, prob), (slope_h, slope), (act_h, act), (ctx_h, ctx)]
    rows_sent = rv.shape[2]
    vec_part = 13 * gown.shape[1] // total
    greet_all(here)
    gather.start(loc.at[0])
    settle1.start()
    loads = [pltpu.make_async_copy(a, b, keep.at[i]) for i, (a, b) in enumerate(kept)]
    for copy in loads:
        copy.start()

    def vec_copy(layer, source, step):
        other = lax.rem(me + step, total)
        first = (other * vec_part) // 128
        return remote(
            source.at[pl.ds(first, rows_sent)], rv.at[layer, me], vs.at[layer, step], vr.at[layer, step],
            here.device_of(other),
        )

    def own_vec(layer, vrows):
        first = (me * vec_part) // 128
        return pltpu.make_async_copy(vrows.at[pl.ds(first, rows_sent)], rv.at[layer, me], own_sem.at[layer])

    sender = here.far * here.ys + here.y

    def out_copy(layer, source, j):
        owner = tp * owners + j
        return remote(
            source.at[j], ro.at[layer, sender], os.at[layer, j], orr.at[layer, sender], here.device_of(owner)
        )

    def send(layer, out_grad, vrows):
        def start_all(step, carry):
            vec_copy(layer, vrows, step).start()
            return carry

        lax.fori_loop(1, total, start_all, 0)
        own_vec(layer, vrows).start()
        for j in range(owners):
            owner = tp * owners + j

            @pl.when(owner != me)
            def _():
                out_copy(layer, out_grad, j).start()

            @pl.when(owner == me)
            def _():
                pltpu.make_async_copy(out_grad.at[j], ro.at[layer, sender], orr.at[layer, sender]).start()

    def collect(layer, out_grad, vrows):
        def wait_all(step, carry):
            vec_copy(layer, vrows, step).wait()
            return carry

        lax.fori_loop(1, total, wait_all, 0)
        own_vec(layer, vrows).wait()
        for j in range(owners):
            owner = tp * owners + j

            @pl.when(owner != me)
            def _():
                out_copy(layer, out_grad, j).wait_send()

        for g in range(here.groups):
            pltpu.make_async_copy(out_grad.at[0], ro.at[layer, g], orr.at[layer, g]).wait()

    send(1, out_grad1, vrows1)
    sums[...] = jnp.zeros_like(sums)
    for copy in loads[:3]:
        copy.wait()

    def one(other, seq):
        mixed = [qkv[seq, :, i * local : (i + 1) * local] for i in range(3)]
        probs = [prob[seq, h] for h in range(local // head_dim)]
        back, mixed_grad, expanded_grad = seq_backward(
            work[other], mixed, probs, slope[seq], head_dim, w, wo, vec, rot
        )
        mixes[seq, :, : 3 * local] = mixed_grad
        mixes[seq, :, 3 * local :] = expanded_grad
        sums[:, : 3 * local] += fold_rows(mixed_grad)
        sums[:, 3 * local :] += fold_rows(expanded_grad)
        return back

    for k in range(HALF):
        if k:
            gather.wait_block(k)
            swap.hand_over(k - 1)
            gather.wait_passed(k)
        else:
            gather.wait_partner()
        block = across(chip, k)
        gather.settle(k, work)

        def part_of(other, carry):
            both[other, k] = one(other, pick(core, other) * HALF + block).astype(BF)
            return carry

        lax.fori_loop(0, 2, part_of, 0)
        swap.to_partner(k).start()
        if k == 2:
            settle1.pass_far()
    for copy in loads[3:]:
        copy.wait()
    weight_grads(xg, gg, mixes, act, ctx, w, vec, sums, packed0, out_grad0, vrows0, gg[tp], tp)
    settle0.start()
    swap.hand_over(HALF - 1)
    settle1.hand_out()
    send(0, out_grad0, vrows0)
    settle0.pass_far()
    swap.wait_landed()

    def finish_back(at):
        value = swap.total(at)
        centred, scale = norm_parts(tokens[at].astype(F32))
        xhat = centred * scale
        mean_one = jnp.mean(value, -1, keepdims=True)
        mean_two = jnp.mean(value * xhat, -1, keepdims=True)
        out[at] = (gg[tp, at].astype(F32) + scale * (value - mean_one - xhat * mean_two)).astype(BF)

    chunks(tokens.shape[0], finish_back)
    settle0.hand_out()
    gather.drain()
    swap.drain()
    collect(1, out_grad1, vrows1)
    collect(0, out_grad0, vrows0)
    settle1.drain()
    settle0.drain()


def third_layer(here, head_dim, gown, w, wo, vec, rot, tokens, xg, kept, packed1, out_grad1, vrows1):
    seqs, rows, width = xg.shape
    local = wo.shape[0]
    ff = (w.shape[1] - 3 * local) // 2
    mix = 3 * local + ff
    total, fars, ys = here.total, here.fars, here.ys
    owners, shard = out_grad1.shape[:2]
    dma = pltpu.SemaphoreType.DMA
    block = pltpu.VMEM((HALF, rows, width), BF)
    pair = pltpu.VMEM((2, HALF, rows, width), BF)
    unit = (HALF, 2, shard, w.shape[1])
    settle = [pltpu.VMEM(n + unit, BF) for n in ((ys - 1, fars), (fars,), (fars - 1,))]
    settle_sems = [dma((ys, fars, HALF))] * 2 + [dma((fars, HALF))] * 2 + [dma((HALF, 2)), dma((TP,))]
    sent = vector_rows(13 * width // total)
    owned = jax.ShapeDtypeStruct((TP, shard, w.shape[1]), BF)
    return pl.pallas_call(
        functools.partial(third_kernel, head_dim, owners),
        out_shape=[
            jax.ShapeDtypeStruct((rows, width), BF),
            owned,
            owned,
            jax.ShapeDtypeStruct((LAYERS, here.groups, shard, width), BF),
            jax.ShapeDtypeStruct((LAYERS, total, sent, 1, 128), F32),
        ],
        in_specs=[VMEM] * 8 + [ANY] * 7,
        out_specs=[VMEM] + [ANY] * 4,
        scratch_shapes=[
            pltpu.VMEM((seqs, rows, width), BF),
            pltpu.VMEM((2, rows, width), BF),
            pltpu.VMEM((seqs, rows, mix), BF),
            pltpu.VMEM((8, mix), F32),
        ]
        + [pltpu.VMEM(a.shape, BF) for a in kept]
        + [pltpu.VMEM(packed1.shape, BF), pltpu.VMEM(out_grad1.shape, BF), pltpu.VMEM(vrows1.shape, F32)]
        + [pair, block, block]
        + settle * 2
        + [
            dma((1,)), dma((5,)), dma((LAYERS, owners)), dma((LAYERS, here.groups)),
            dma((LAYERS, total)), dma((LAYERS, total)), dma((LAYERS,)),
        ]
        + [dma((HALF,))] * 8
        + settle_sems * 2,
        compiler_params=pltpu.CompilerParams(
            collective_id=4, has_side_effects=True, vmem_limit_bytes=VMEM_BYTES
        ),
        name="third_layer",
    )(gown, w, wo, vec, rot, tokens, xg, packed1, *kept, out_grad1, vrows1)


def adam_kernel(groups, local, ff, fixes, r0, r1, ro, *refs):
    params, moments, squares = refs[0:4], refs[4:8], refs[8:12]
    grads, changes, new_moments, new_squares = refs[12:16], refs[16:20], refs[20:24], refs[24:28]
    first_fix, second_fix = fixes[0], fixes[1]

    def update(which, at, gradient):
        moment = BETA_FIRST * moments[which][0, :, at] + (1.0 - BETA_FIRST) * gradient
        square = BETA_SECOND * squares[which][0, :, at] + (1.0 - BETA_SECOND) * gradient * gradient
        grads[which][0, :, at] = gradient
        new_moments[which][0, :, at] = moment
        new_squares[which][0, :, at] = square
        changes[which][0, :, at] = -LEARNING * (
            moment / first_fix / (jnp.sqrt(square / second_fix) + ADAM_EPSILON)
            + DECAY_RATE * params[which][0, :, at]
        )

    def layer(source):
        for p in range(TP):
            value = source[p].astype(F32)
            for i in range(3):
                start = i * TP * local + p * local
                update(0, slice(start, start + local), value[:, i * local : (i + 1) * local])
            split = 3 * local
            at = slice(p * ff, (p + 1) * ff)
            update(2, at, value[:, split : split + ff])
            update(3, at, value[:, split + ff :])
        value = ro[0, 0].astype(F32)
        for g in range(1, groups):
            value = value + ro[0, g].astype(F32)
        update(1, slice(None), value)

    @pl.when(pl.program_id(0) == 0)
    def _():
        layer(r0)

    @pl.when(pl.program_id(0) == 1)
    def _():
        layer(r1)


def adam_step(groups, local, ff, fixes, r0, r1, ro, params, moments, squares):
    shard = ro.shape[2]
    part = 8
    specs = [pl.BlockSpec((1, part, a.shape[2]), lambda l, r: (l, r, 0)) for a in params]
    source = lambda layer: pl.BlockSpec(
        (r0.shape[0], part, r0.shape[2]), lambda l, r: (0, jnp.where(l == layer, r, (1 - layer) * (shard // part - 1)), 0)
    )
    outs = [jax.ShapeDtypeStruct(a.shape, F32) for a in params]
    return pl.pallas_call(
        functools.partial(adam_kernel, groups, local, ff),
        grid=(LAYERS, shard // part),
        in_specs=[SMEM, source(0), source(1), pl.BlockSpec((1, groups, part, ro.shape[3]), lambda l, r: (l, 0, r, 0))]
        + specs * 3,
        out_specs=specs * 4,
        out_shape=outs * 4,
        compiler_params=pltpu.CompilerParams(vmem_limit_bytes=VMEM_BYTES),
        name="adam_step",
    )(fixes, r0, r1, ro, *params, *moments, *squares)


def rotary(row_count, width, head_dim):
    rot_dim = head_dim // 4
    half_rot = rot_dim // 2
    column = jnp.arange(width, dtype=jnp.int32) % head_dim
    freq_slot = (column % half_rot).astype(F32)
    frequency = 10000.0 ** (-(freq_slot * 2.0) / rot_dim)
    angles = jnp.arange(row_count, dtype=F32)[:, None] * frequency[None, :]
    inside = (column < rot_dim)[None, :]
    first_half = (column < half_rot)[None, :]
    sine = jnp.sin(angles)
    return jnp.stack(
        [
            jnp.where(inside, jnp.cos(angles), 1.0),
            jnp.where(first_half, -sine, 0.0),
            jnp.where(inside & jnp.logical_not(first_half), sine, 0.0),
        ]
    )


def standard(values):
    centred = values - jnp.mean(values, -1, keepdims=True)
    return centred * lax.rsqrt(jnp.mean(centred * centred, -1, keepdims=True) + NORM_EPSILON)


def adam_update(weight, moment, square, gradient, first_fix, second_fix):
    moment = BETA_FIRST * moment + (1.0 - BETA_FIRST) * gradient
    square = BETA_SECOND * square + (1.0 - BETA_SECOND) * gradient * gradient
    change = -LEARNING * (
        moment / first_fix / (jnp.sqrt(square / second_fix) + ADAM_EPSILON) + DECAY_RATE * weight
    )
    return (change, moment, square)


def per_device(tokens, cotangent, seq_lengths, seq_device, step_count, *state):
    params, moments, squares = state[0:5], state[5:10], state[10:15]
    attend_in, attend_out, expand_weight, reduce_weight, layer_vectors = params
    here = Place()
    tp, me, total, groups = here.tp, here.me, here.total, here.groups
    rows, width = tokens.shape
    shard = attend_in.shape[1]
    head_dim = width // HEADS
    local = width // TP
    ff = expand_weight.shape[2] // TP
    vec_part = layer_vectors.shape[1]
    owners = local // shard
    plane_ids = here.flat(here.far, here.y, jnp.arange(TP, dtype=jnp.int32))
    lens = jnp.sum(jnp.where(plane_ids[:, None] == seq_device[None, :], seq_lengths[None, :], 0), 1)
    lens = jnp.broadcast_to(lens[:, None, None], (TP, 1, rows))
    own_length = jnp.sum(jnp.where(seq_device == me, seq_lengths, 0))
    valid = jnp.arange(rows, dtype=jnp.int32)[:, None] < own_length
    rot = rotary(rows, local, head_dim)

    blocks = [
        jnp.concatenate(
            [
                attend_in[l].astype(BF).reshape(shard, 3, TP, local).transpose(2, 0, 1, 3).reshape(TP, shard, 3 * local),
                expand_weight[l].astype(BF).reshape(shard, TP, ff).transpose(1, 0, 2),
                reduce_weight[l].astype(BF).reshape(shard, TP, ff).transpose(1, 0, 2),
            ],
            2,
        )
        for l in range(LAYERS)
    ]
    vec = jnp.pad(layer_vectors.astype(BF).astype(F32).reshape(-1), (0, 8 * 128 - 2 * vec_part)).reshape(8, 128)
    xhat_own = standard(tokens.astype(F32)).astype(BF)
    grad_own = jnp.where(valid, cotangent, jnp.zeros_like(cotangent))
    xg, w0, w1, wog, vecg = spread(here, xhat_own, blocks[0], blocks[1], attend_out.astype(BF), vec)
    w0, w1 = w0.reshape(width, -1), w1.reshape(width, -1)
    out_rows = wog.transpose(1, 0, 2, 3).reshape(LAYERS, local, width)
    vectors = vecg.reshape(total, -1)[:, : 2 * vec_part].reshape(total, LAYERS, vec_part)
    vectors = vectors.transpose(1, 0, 2).reshape(LAYERS, 13, width)
    vectors = jnp.pad(vectors, ((0, 0), (0, 3), (0, 0)))

    hidden0, xnext, grads_all, *kept = first_layer(
        head_dim, lens, xg, w0, out_rows[0], vectors[0], rot, tokens, grad_own
    )
    hidden1, grad0, packed1, out_grad1, vrows1 = second_layer(
        here, head_dim, owners, shard, lens, xnext, grads_all, w1, out_rows[1], vectors[1], rot, hidden0
    )
    input_grad, r0, r1, ro, rv = third_layer(
        here, head_dim, grad0, w0, out_rows[0], vectors[0], rot, tokens, xg, kept, packed1, out_grad1, vrows1
    )
    step_float = step_count[0].astype(F32)
    first_fix = 1.0 - jnp.power(BETA_FIRST, step_float)
    second_fix = 1.0 - jnp.power(BETA_SECOND, step_float)
    big = adam_step(
        groups, local, ff, jnp.stack([first_fix, second_fix]), r0, r1, ro, params[:4], moments[:4], squares[:4]
    )
    vec_rows = jnp.sum(rv, 1).reshape(LAYERS, -1)
    grad_vec = lax.dynamic_slice_in_dim(vec_rows, lax.rem(me * vec_part, 128), vec_part, 1)
    small = (grad_vec,) + adam_update(params[4], moments[4], squares[4], grad_vec, first_fix, second_fix)
    results = []
    for i in range(4):
        results += list(big[4 * i : 4 * i + 4]) + [small[i]]
    return (jnp.stack([hidden0, hidden1]), input_grad, *results)


def solution(mesh):
    devices = mesh.devices.reshape(-1)
    blocks = devices.size // TP
    fars = 1 << ((blocks.bit_length()) // 2)
    flat = Mesh(devices.reshape(fars, 2, 2, blocks // fars, 2), AXES)
    by_row = P(AXES, None)
    by_dim = [P(None, AXES, None)] * 4 + [P(None, AXES)]
    return jax.shard_map(
        per_device,
        mesh=flat,
        in_specs=(by_row, by_row, P(), P(), P(), *(by_dim * 3)),
        out_specs=(P(None, AXES, None), by_row, *(by_dim * 4)),
        check_vma=False,
    )
```

```python
import functools

import jax
import jax.numpy as jnp
from jax import lax
from jax.experimental import pallas as pl
from jax.experimental.pallas import tpu as pltpu
from jax.sharding import Mesh
from jax.sharding import PartitionSpec as P

HEADS = 16
LAYERS = 2
NORM_EPSILON = 1e-05
ADAM_EPSILON = 1e-08
LEARNING = 0.02
BETA_FIRST = 0.9
BETA_SECOND = 0.95
DECAY_RATE = 0.1
MASKED_SCORE = -1e30

TP = 8
HALF = TP // 2
BF = jnp.bfloat16
F32 = jnp.float32
MESH = pl.DeviceIdType.MESH
NT = (((1,), (1,)), ((), ()))
TN = (((0,), (0,)), ((), ()))
ANY = pl.BlockSpec(memory_space=pl.ANY)
VMEM = pl.BlockSpec(memory_space=pltpu.VMEM)
SMEM = pl.BlockSpec(memory_space=pltpu.SMEM)
VMEM_BYTES = 67043328


AXES = ("far", "near", "core", "y", "x")


class Place:
    def __init__(self):
        self.far, near, core, self.y, x = (lax.axis_index(name) for name in AXES)
        self.fars, self.ys = lax.axis_size("far"), lax.axis_size("y")
        self.tp = core * HALF + near * 2 + x
        self.row = near * 2 + core
        self.x = x
        self.core, self.chip = core, near * 2 + x
        self.partner = (1 - core) * HALF + self.chip
        self.groups, self.total = self.fars * self.ys, self.fars * self.ys * TP
        self.me = self.flat(self.far, self.y, self.tp)

    def flat(self, far, y, tp):
        near, core, x = lax.rem(tp // 2, 2), tp // HALF, lax.rem(tp, 2)
        return (((far * 2 + near) * 2 + core) * self.ys + y) * 2 + x

    def device(self, tp, far=None, y=None):
        far = self.far if far is None else far
        y = self.y if y is None else y
        return far, lax.rem(tp // 2, 2), tp // HALF, y, lax.rem(tp, 2)

    def device_of(self, flat):
        rest = flat // 2
        y, rest = lax.rem(rest, self.ys), rest // self.ys
        core, rest = lax.rem(rest, 2), rest // 2
        return rest // 2, lax.rem(rest, 2), core, y, lax.rem(flat, 2)

    def tp_of(self, row, x):
        return (row % 2) * HALF + (row // 2) * 2 + x


def nn_dot(a, b):
    return jnp.dot(a, b, preferred_element_type=F32)


def nt_dot(a, b):
    return lax.dot_general(a, b, NT, preferred_element_type=F32)


def tn_dot(a, b):
    return lax.dot_general(a, b, TN, preferred_element_type=F32)


def remote(src, dst, send, recv, target):
    return pltpu.make_async_remote_copy(
        src_ref=src, dst_ref=dst, send_sem=send, recv_sem=recv, device_id=target, device_id_type=MESH
    )


def greet(targets):
    barrier = pltpu.get_barrier_semaphore()
    for target in targets:
        pl.semaphore_signal(barrier, inc=1, device_id=target, device_id_type=MESH)
    pl.semaphore_wait(barrier, len(targets))


def greet_all(here):
    barrier = pltpu.get_barrier_semaphore()

    def signal(step, carry):
        other = lax.rem(here.me + step, here.total)
        pl.semaphore_signal(barrier, inc=1, device_id=here.device_of(other), device_id_type=MESH)
        return carry

    lax.fori_loop(1, here.total, signal, 0)
    pl.semaphore_wait(barrier, here.total - 1)


def spread_kernel(owners, xh, s0, s1, wo, vec, xg, w0, w1, wog, vecg,
                  ps, pr, zs, zr, ys, yr, os, orr, vs, vr, loc, *sems):
    here = Place()
    far, y, tp, row, x = here.far, here.y, here.tp, here.row, here.x
    gather_x = Gather(here, xh, xg, sems[0:4])
    layers = ((s0, w0), (s1, w1))
    greet_all(here)

    def within(l, step):
        source, w = layers[l]
        peer = lax.rem(tp + step, TP)
        return remote(
            source.at[peer], w.at[far, row, y, x], ps.at[l, step], pr.at[l, tp], here.device(peer)
        )

    def start_layer(l):
        source, w = layers[l]
        for step in range(1, TP):
            within(l, step).start()
        pltpu.make_async_copy(source.at[tp], w.at[far, row, y, x], pr.at[l, tp]).start()

    def vec_copy(step):
        other = lax.rem(here.me + step, here.total)
        return remote(vec, vecg.at[here.me], vs.at[step], vr.at[step], here.device_of(other))

    def start_vec(step, carry):
        vec_copy(step).start()
        return carry

    def wait_vec(step, carry):
        vec_copy(step).wait()
        return carry

    start_layer(0)
    start_layer(1)
    lax.fori_loop(1, here.total, start_vec, 0)
    own_vec = pltpu.make_async_copy(vec, vecg.at[here.me], loc.at[1])
    own_vec.start()
    slot = lax.rem(here.me, owners)
    user = here.me // owners

    def out_copy(f, v):
        return remote(wo, wog.at[slot], os.at[f, v], orr.at[slot], here.device(user, f, v))

    def is_own(f, v):
        return (user == tp) & (f == far) & (v == y)

    blocks = [(f, v) for f in range(here.fars) for v in range(here.ys)]
    for f, v in blocks:

        @pl.when(jnp.logical_not(is_own(f, v)))
        def _():
            out_copy(f, v).start()

        @pl.when(is_own(f, v))
        def _():
            pltpu.make_async_copy(wo, wog.at[slot], orr.at[slot]).start()

    def along_far(l, i, r):
        part = layers[l][1].at[far, r, y]
        target = lax.rem(far + i, here.fars)
        return remote(part, part, zs.at[l, i, r], zr.at[l, i, r], here.device(tp, far=target))

    def along_y(l, j, i, r):
        part = layers[l][1].at[lax.rem(far + here.fars - i, here.fars), r, y]
        target = lax.rem(y + j, here.ys)
        return remote(part, part, ys.at[l, j, i, r], yr.at[l, j, i, r], here.device(tp, y=target))

    def landed(l, f, r, v, sem):
        part = layers[l][1].at[f, r, v]
        remote(part, part, sem, sem, here.device(here.partner)).wait_recv()

    def first_hop(l):
        source, w = layers[l]
        for r in range(HALF):
            for side in range(2):
                t = here.tp_of(r, side)
                pltpu.make_async_copy(source.at[0], w.at[far, r, y, side], pr.at[l, t]).wait()
            for i in range(1, here.fars):
                along_far(l, i, r).start()
            for j in range(1, here.ys):
                along_y(l, j, 0, r).start()

    first_hop(0)
    first_hop(1)
    gather_x.start(loc.at[0])
    for l in range(LAYERS):
        for r in range(HALF):
            for i in range(1, here.fars):
                landed(l, lax.rem(far + here.fars - i, here.fars), r, y, zr.at[l, i, r])
                for j in range(1, here.ys):
                    along_y(l, j, i, r).start()
    for k in range(1, HALF):
        gather_x.wait_block(k)
    gather_x.wait_partner()
    for k in range(1, HALF):
        gather_x.wait_passed(k)
    for l in range(LAYERS):
        for j in range(1, here.ys):
            for i in range(here.fars):
                for r in range(HALF):
                    landed(
                        l, lax.rem(far + here.fars - i, here.fars), r, lax.rem(y + here.ys - j, here.ys),
                        yr.at[l, j, i, r],
                    )
    lax.fori_loop(1, here.total, wait_vec, 0)
    own_vec.wait()
    for j in range(owners):
        pltpu.make_async_copy(wo, wog.at[j], orr.at[j]).wait()
    gather_x.drain()
    for l in range(LAYERS):
        for step in range(1, TP):
            within(l, step).wait_send()
        for r in range(HALF):
            for i in range(1, here.fars):
                along_far(l, i, r).wait_send()
            for j in range(1, here.ys):
                for i in range(here.fars):
                    along_y(l, j, i, r).wait_send()
    for f, v in blocks:

        @pl.when(jnp.logical_not(is_own(f, v)))
        def _():
            out_copy(f, v).wait_send()


def spread(here, xh, s0, s1, wo, vec):
    rows, cols = s0.shape[1:]
    owners = wo.shape[2] // TP // rows
    dma = pltpu.SemaphoreType.DMA
    whole = jax.ShapeDtypeStruct((here.fars, HALF, here.ys, 2, rows, cols), BF)
    gathered = jax.ShapeDtypeStruct((TP,) + xh.shape, BF)
    return pl.pallas_call(
        functools.partial(spread_kernel, owners),
        out_shape=(
            gathered,
            whole,
            whole,
            jax.ShapeDtypeStruct((owners,) + wo.shape, BF),
            jax.ShapeDtypeStruct((here.total,) + vec.shape, F32),
        ),
        in_specs=[VMEM] + [ANY] * 4,
        out_specs=(ANY,) * 5,
        scratch_shapes=[
            dma((LAYERS, TP)), dma((LAYERS, TP)),
            dma((LAYERS, here.fars, HALF)), dma((LAYERS, here.fars, HALF)),
            dma((LAYERS, here.ys, here.fars, HALF)), dma((LAYERS, here.ys, here.fars, HALF)),
            dma((here.fars, here.ys)), dma((owners,)), dma((here.total,)), dma((here.total,)), dma((2,)),
        ]
        + [dma((HALF,))] * 4,
        compiler_params=pltpu.CompilerParams(collective_id=1, has_side_effects=True),
        name="spread",
    )(xh, s0, s1, wo, vec)


def turn(values, rot):
    return (
        values * rot[0]
        + pltpu.roll(values, values.shape[1] - 8, 1) * rot[1]
        + pltpu.roll(values, 8, 1) * rot[2]
    )


def turn_back(values, rot):
    return (
        values * rot[0]
        + pltpu.roll(values * rot[1], 8, 1)
        + pltpu.roll(values * rot[2], values.shape[1] - 8, 1)
    )


def head_parts(values, head_dim):
    lane = lax.broadcasted_iota(jnp.int32, values.shape, 1)
    zero = jnp.zeros_like(values)
    return [
        jnp.where((lane >= h * head_dim) & (lane < (h + 1) * head_dim), values, zero)
        for h in range(values.shape[1] // head_dim)
    ]


def bias_slices(vec, tp, local, ff):
    width = vec.shape[1]
    b_in = vec[4:7, pl.ds(pl.multiple_of(tp * local, local), local)]
    per_row = width // ff
    row = 8 + tp // per_row
    b_up = vec[pl.ds(row, 1), pl.ds(pl.multiple_of(lax.rem(tp, per_row) * ff, ff), ff)]
    return b_in, b_up


def seq_forward(values, lengths, head_dim, w, wo, vec, b_in, b_up, rot):
    rows = values.shape[0]
    local = wo.shape[0]
    ff = b_up.shape[1]
    values = values.astype(F32)
    normed = (values * vec[0:1] + vec[1:2]).astype(BF)
    mixed = nn_dot(normed, w[:, : 3 * local])
    parts = [mixed[:, i * local : (i + 1) * local] + b_in[i : i + 1] for i in range(3)]
    queries = (turn(parts[0], rot).astype(BF).astype(F32) * head_dim ** (-0.5)).astype(BF)
    keys = turn(parts[1], rot).astype(BF)
    vals = parts[2].astype(BF)
    row = lax.broadcasted_iota(jnp.int32, (rows, rows), 0)
    col = lax.broadcasted_iota(jnp.int32, (rows, rows), 1)
    allowed = (col <= row) & (col < lengths)
    total, probs = None, []
    for q_h, v_h in zip(head_parts(queries, head_dim), head_parts(vals, head_dim)):
        scores = jnp.where(allowed, nt_dot(q_h, keys), MASKED_SCORE)
        weights = jnp.exp(scores - jnp.max(scores, -1, keepdims=True))
        probability = (weights / jnp.sum(weights, -1, keepdims=True)).astype(BF)
        probs.append(probability)
        term = nn_dot(probability, v_h)
        total = term if total is None else total + term
    context = total.astype(BF)
    normed = (values * vec[2:3] + vec[3:4]).astype(BF)
    expanded = nn_dot(normed, w[:, 3 * local : 3 * local + ff]) + b_up
    spread_to = 0.5 * (1.0 + lax.erf(expanded * 0.7071067811865476))
    active = (expanded * spread_to).astype(BF)
    slope = (spread_to + expanded * (0.3989422804014327 * jnp.exp(-0.5 * expanded * expanded))).astype(BF)
    part = nn_dot(context, wo[...]) + nt_dot(active, w[:, 3 * local + ff :])
    return part, (queries, keys, vals), probs, context, active, slope


def seq_backward(grad, qkv, probs, slope, head_dim, w, wo, vec, rot):
    local = wo.shape[0]
    ff = slope.shape[1]
    queries, keys, vals = qkv
    active_grad = nn_dot(grad, w[:, 3 * local + ff :])
    expanded_grad = (slope.astype(F32) * active_grad).astype(BF)
    total = nt_dot(expanded_grad, w[:, 3 * local : 3 * local + ff]) * vec[2:3]
    context_grad = nt_dot(grad, wo[...]).astype(BF)
    query_grad = key_grad = value_grad = 0.0
    for prob_b, c_h, q_h, k_h in zip(
        probs, head_parts(context_grad, head_dim), head_parts(queries, head_dim), head_parts(keys, head_dim)
    ):
        probability = prob_b.astype(F32)
        prob_grad = nt_dot(c_h, vals)
        value_grad = value_grad + tn_dot(prob_b, c_h)
        inner = jnp.sum(probability * prob_grad, -1, keepdims=True)
        score_grad = (probability * (prob_grad - inner)).astype(BF)
        query_grad = query_grad + nn_dot(score_grad, k_h)
        key_grad = key_grad + tn_dot(score_grad, q_h)
    query_grad = query_grad * head_dim ** (-0.5)
    pieces = [turn_back(query_grad, rot).astype(BF), turn_back(key_grad, rot).astype(BF), value_grad.astype(BF)]
    mixed_grad = jnp.concatenate(pieces, 1)
    total = total + nt_dot(mixed_grad, w[:, : 3 * local]) * vec[0:1]
    return total, mixed_grad, expanded_grad


def fold_rows(values):
    return jnp.sum(values.astype(F32).reshape(-1, 8, values.shape[1]), axis=0)


def across(chip, step):
    x = lax.rem(lax.rem(chip, 2) + lax.rem(step, 2), 2)
    y = lax.rem(chip // 2 + step // 2, 2)
    return 2 * y + x


def pick(core, other):
    return core + (1 - 2 * core) * other


CHUNK = 32


def chunks(rows, body):
    def step(i, carry):
        body(pl.ds(pl.multiple_of(i * CHUNK, CHUNK), CHUNK))
        return carry

    lax.fori_loop(0, rows // CHUNK, step, 0)


def norm_parts(values):
    centred = values - jnp.mean(values, -1, keepdims=True)
    return centred, lax.rsqrt(jnp.mean(centred * centred, -1, keepdims=True) + NORM_EPSILON)


class Exchange:
    def __init__(self, here, both, met, landed, sems):
        self.here = here
        self.joined, self.mine, self.met, self.landed = both.at[0], both.at[1], met, landed
        self.ps, self.pr, self.bs, self.br = sems
        self.core, self.chip, self.partner = here.core, here.chip, here.partner

    def to_partner(self, k):
        return remote(
            self.mine.at[k], self.met.at[k], self.ps.at[k], self.pr.at[k], self.here.device(self.partner)
        )

    def to_owner(self, k):
        owner = self.core * HALF + across(self.chip, k)
        return remote(
            self.joined.at[k], self.landed.at[k], self.bs.at[k], self.br.at[k], self.here.device(owner)
        )

    def join(self, k):
        self.to_partner(k).wait_recv()

        def add(at):
            self.joined[k, at] = (self.joined[k, at].astype(F32) + self.met[k, at].astype(F32)).astype(BF)

        chunks(self.met.shape[1], add)

    def hand_over(self, k):
        self.join(k)
        if k:
            self.to_owner(k).start()

    def total(self, at):
        value = self.joined[0, at].astype(F32)
        for k in range(1, HALF):
            value = value + self.landed[k, at].astype(F32)
        return value

    def wait_landed(self):
        for k in range(1, HALF):
            self.to_owner(k).wait_recv()

    def drain(self):
        for k in range(HALF):
            self.to_partner(k).wait_send()
        for k in range(1, HALF):
            self.to_owner(k).wait_send()


class Gather:
    def __init__(self, here, own, buffer, sems):
        self.here, self.own, self.buffer = here, own, buffer
        self.gs, self.gr, self.fs, self.fr = sems
        self.tp, self.core, self.chip, self.partner = here.tp, here.core, here.chip, here.partner

    def to_peer(self, k):
        if isinstance(k, int) and k == 0:
            target = self.partner
        else:
            target = self.core * HALF + across(self.chip, k)
        return remote(self.own, self.buffer.at[self.tp], self.gs.at[k], self.gr.at[k], self.here.device(target))

    def start(self, local):
        pltpu.make_async_copy(self.own, self.buffer.at[self.tp], local).start()
        for k in (1, 2, 3, 0):
            self.to_peer(k).start()
        pltpu.make_async_copy(self.own, self.buffer.at[self.tp], local).wait()

    def pass_on(self, k):
        source = self.core * HALF + across(self.chip, k)
        block = self.buffer.at[source]
        return remote(block, block, self.fs.at[k], self.fr.at[k], self.here.device(self.partner))

    def arrived(self, source, sem):
        block = self.buffer.at[source]
        remote(block, block, sem, sem, self.here.device(self.partner)).wait_recv()

    def wait_block(self, k):
        self.arrived(self.core * HALF + across(self.chip, k), self.gr.at[k])
        self.pass_on(k).start()

    def wait_partner(self):
        self.arrived(self.partner, self.gr.at[0])

    def wait_passed(self, k):
        self.arrived((1 - self.core) * HALF + across(self.chip, k), self.fr.at[k])

    def settle(self, k, work):
        block = across(self.chip, k)
        for other in range(2):
            work[other] = self.buffer[pick(self.core, other) * HALF + block]

    def drain(self):
        for k in range(HALF):
            self.to_peer(k).wait_send()
        for k in range(1, HALF):
            self.pass_on(k).wait_send()


def greet_block(here):
    targets = [here.partner] + [here.core * HALF + across(here.chip, k) for k in range(1, HALF)]
    greet([here.device(target) for target in targets])


def first_kernel(head_dim, lens, xg, w, wo, vec, rot, own, gr,
                 out, xnext, gg, qkv_h, prob_h, ctx_h, act_h, slope_h,
                 qkv, prob, ctx, act, slope, both, met, landed, keep, *sems):
    here = Place()
    tp, core, chip = here.tp, here.core, here.chip
    local, ff = wo.shape[0], act.shape[2]
    swap = Exchange(here, both, met, landed, sems[0:4])
    gather = Gather(here, gr, gg, sems[4:8])
    kept = [(qkv, qkv_h), (prob, prob_h), (ctx, ctx_h), (act, act_h), (slope, slope_h)]
    greet_block(here)
    b_in, b_up = bias_slices(vec, tp, local, ff)

    def one(seq):
        part, mixed, probs, context, active, sl = seq_forward(
            xg[seq], lens[seq], head_dim, w, wo, vec, b_in, b_up, rot
        )
        for i, piece in enumerate(mixed):
            qkv[seq, :, i * local : (i + 1) * local] = piece
        for h, p in enumerate(probs):
            prob[seq, h] = p
        ctx[seq] = context
        act[seq] = active
        slope[seq] = sl
        return part

    for k in reversed(range(HALF)):
        block = across(chip, k)

        def part_of(other, carry):
            both[other, k] = one(pick(core, other) * HALF + block).astype(BF)
            return carry

        lax.fori_loop(0, 2, part_of, 0)
        swap.to_partner(k).start()
        if k + 1 < HALF:
            swap.hand_over(k + 1)
        if k == 0:
            gather.start(keep.at[5])
    swap.hand_over(0)
    saved = [pltpu.make_async_copy(a, b, keep.at[i]) for i, (a, b) in enumerate(kept)]
    for copy in saved:
        copy.start()
    for k in range(1, HALF):
        gather.wait_block(k)
    swap.wait_landed()

    def finish(at):
        result = (own[at].astype(F32) + swap.total(at) + (vec[7:8] + vec[12:13])).astype(BF)
        out[at] = result
        centred, scale = norm_parts(result.astype(F32))
        xnext[at] = (centred * scale).astype(BF)

    chunks(own.shape[0], finish)
    gather.wait_partner()
    for k in range(1, HALF):
        gather.wait_passed(k)
    gather.drain()
    swap.drain()
    for copy in saved:
        copy.wait()


def first_layer(head_dim, lens, xg, w, wo, vec, rot, own, gr):
    seqs, rows, width = xg.shape
    local = wo.shape[0]
    ff = (w.shape[1] - 3 * local) // 2
    dma = pltpu.SemaphoreType.DMA
    kept = [
        (seqs, rows, 3 * local), (seqs, local // head_dim, rows, rows), (seqs, rows, local), (seqs, rows, ff),
        (seqs, rows, ff),
    ]
    block = pltpu.VMEM((HALF, rows, width), BF)
    pair = pltpu.VMEM((2, HALF, rows, width), BF)
    return pl.pallas_call(
        functools.partial(first_kernel, head_dim),
        out_shape=[jax.ShapeDtypeStruct((rows, width), BF)] * 2
        + [jax.ShapeDtypeStruct(s, BF) for s in [xg.shape] + kept],
        in_specs=[VMEM] * 8,
        out_specs=[VMEM] * 2 + [ANY] * 6,
        scratch_shapes=[pltpu.VMEM(s, BF) for s in kept] + [pair, block, block] + [dma((6,))] + [dma((HALF,))] * 8,
        compiler_params=pltpu.CompilerParams(
            collective_id=2, has_side_effects=True, vmem_limit_bytes=VMEM_BYTES
        ),
        name="first_layer",
    )(lens, xg, w, wo, vec, rot, own, gr)


def weight_grads(xg, gg, mixes, act, ctx, w, vec, sums, packed, out_grad, vrows, grad_rows, tp):
    local, width = out_grad.shape[0] * out_grad.shape[1], out_grad.shape[2]
    fars, _, ys, _, shard, cols = packed.shape
    ff = act.shape[2]
    split = 3 * local
    rows = xg.shape[0] * xg.shape[1]
    flat = lambda ref, cut: ref[:, :, cut].reshape(rows, -1)
    everything = slice(None)
    col_sums = jnp.sum(sums[...], axis=0, keepdims=True)
    half = width // 2
    ones = jnp.ones((8, split), F32)
    wide = jnp.ones((8, ff), F32)
    exact = lambda a, b: lax.dot_general(a, b, NT, preferred_element_type=F32, precision=lax.Precision.HIGHEST)
    for c in range(2):
        cut = slice(c * half, (c + 1) * half)
        lines = slice(c * fars // 2, (c + 1) * fars // 2)
        shape = (fars // 2, HALF, ys, 2, shard)
        gains = vec[0:4, cut].T
        cross = tn_dot(flat(xg, cut), flat(mixes, everything))
        in_cross, up_cross = cross[:, :split], cross[:, split:]
        in_grad = gains[:, 0:1] * in_cross + gains[:, 1:2] * col_sums[:, :split]
        up_grad = gains[:, 2:3] * up_cross + gains[:, 3:4] * col_sums[:, split:]
        down_grad = tn_dot(flat(gg, cut), flat(act, everything))
        packed[lines, :, :, :, :, :split] = in_grad.astype(BF).reshape(shape + (split,))
        packed[lines, :, :, :, :, split : split + ff] = up_grad.astype(BF).reshape(shape + (ff,))
        packed[lines, :, :, :, :, split + ff :] = down_grad.astype(BF).reshape(shape + (ff,))
        w_in = w[cut, :split].astype(F32)
        w_up = w[cut, split : split + ff].astype(F32)
        norm_rows = [
            exact(ones, w_in * in_cross)[0:1],
            exact(jnp.broadcast_to(col_sums[:, :split], (8, split)), w_in)[0:1],
            exact(wide, w_up * up_cross)[0:1],
            exact(jnp.broadcast_to(col_sums[:, split:], (8, ff)), w_up)[0:1],
        ]
        for i, line in enumerate(norm_rows):
            for j in range(half // 128):
                vrows[i * (width // 128) + c * (half // 128) + j] = line[:, j * 128 : (j + 1) * 128]
        part = tn_dot(flat(ctx, everything), flat(gg, cut)).astype(BF)
        out_grad[:, :, cut] = part.reshape(-1, shard, half)
    per = width // 128
    base = 4 * per

    def clear(i, carry):
        vrows[base + i] = jnp.zeros((1, 128), F32)
        return carry

    lax.fori_loop(0, vrows.shape[0] - base, clear, 0)
    step = local // 128
    for i in range(3):
        for j in range(step):
            vrows[base + i * per + tp * step + j] = col_sums[:, i * local + j * 128 : i * local + (j + 1) * 128]
    base = 8 * per
    for j in range(ff // 128):
        vrows[base + tp * (ff // 128) + j] = col_sums[:, split + j * 128 : split + (j + 1) * 128]
    bias = jnp.sum(grad_rows.astype(F32), axis=0, keepdims=True)
    for j in range(per):
        vrows[7 * per + j] = bias[:, j * 128 : (j + 1) * 128]
        vrows[12 * per + j] = bias[:, j * 128 : (j + 1) * 128]


def second_kernel(head_dim, lens, xown, gg, w, wo, vec, rot, hidden,
                  shares, grad_next, packed, out_grad, vrows,
                  xg, work, mixes, act, ctx, sums, both, met, both_e, met_e, landed_e,
                  loc, *sems):
    here = Place()
    tp, core, chip = here.tp, here.core, here.chip
    local, ff = wo.shape[0], act.shape[2]
    swap = Exchange(here, both, met, None, sems[0:4])
    swap_e = Exchange(here, both_e, met_e, landed_e, sems[4:8])
    gather = Gather(here, xown, xg, sems[8:12])
    greet_block(here)
    gather.start(loc.at[0])
    sums[...] = jnp.zeros_like(sums)
    b_in, b_up = bias_slices(vec, tp, local, ff)

    def one(other, seq):
        part, mixed, probs, context, active, sl = seq_forward(
            work[other], lens[seq], head_dim, w, wo, vec, b_in, b_up, rot
        )
        ctx[seq] = context
        act[seq] = active
        back, mixed_grad, expanded_grad = seq_backward(
            gg[seq], mixed, probs, sl, head_dim, w, wo, vec, rot
        )
        mixes[seq, :, : 3 * local] = mixed_grad
        mixes[seq, :, 3 * local :] = expanded_grad
        sums[:, : 3 * local] += fold_rows(mixed_grad)
        sums[:, 3 * local :] += fold_rows(expanded_grad)
        return part, back

    for k in range(HALF):
        if k:
            gather.wait_block(k)
            swap_e.hand_over(k - 1)
            swap.join(k - 1)
            gather.wait_passed(k)
        else:
            gather.wait_partner()
        block = across(chip, k)
        gather.settle(k, work)

        def part_of(other, carry):
            part, back = one(other, pick(core, other) * HALF + block)
            both[other, k] = part.astype(BF)
            both_e[other, k] = back.astype(BF)
            return carry

        lax.fori_loop(0, 2, part_of, 0)
        swap_e.to_partner(k).start()
        swap.to_partner(k).start()
    swap_e.hand_over(HALF - 1)
    swap.join(HALF - 1)
    saved = pltpu.make_async_copy(both.at[0], shares, loc.at[1])
    saved.start()
    weight_grads(xg, gg, mixes, act, ctx, w, vec, sums, packed, out_grad, vrows, gg[tp], tp)
    swap_e.wait_landed()

    def finish_back(at):
        total = swap_e.total(at)
        centred, scale = norm_parts(hidden[at].astype(F32))
        xhat = centred * scale
        mean_one = jnp.mean(total, -1, keepdims=True)
        mean_two = jnp.mean(total * xhat, -1, keepdims=True)
        grad_next[at] = (
            gg[tp, at].astype(F32) + scale * (total - mean_one - xhat * mean_two)
        ).astype(BF)

    chunks(hidden.shape[0], finish_back)
    gather.drain()
    for k in range(HALF):
        swap.to_partner(k).wait_send()
    swap_e.drain()
    saved.wait()


def second_layer(here, head_dim, owners, shard, lens, xown, gg, w, wo, vec, rot, hidden):
    seqs, rows, width = gg.shape
    local = wo.shape[0]
    ff = (w.shape[1] - 3 * local) // 2
    mix = 3 * local + ff
    dma = pltpu.SemaphoreType.DMA
    block = pltpu.VMEM((HALF, rows, width), BF)
    pair = pltpu.VMEM((2, HALF, rows, width), BF)
    return pl.pallas_call(
        functools.partial(second_kernel, head_dim),
        out_shape=[
            jax.ShapeDtypeStruct((HALF, rows, width), BF),
            jax.ShapeDtypeStruct((rows, width), BF),
            jax.ShapeDtypeStruct((here.fars, HALF, here.ys, 2, shard, w.shape[1]), BF),
            jax.ShapeDtypeStruct((owners, shard, width), BF),
            jax.ShapeDtypeStruct((13 * width // 128, 1, 128), F32),
        ],
        in_specs=[VMEM] * 8,
        out_specs=[ANY] + [VMEM] * 4,
        scratch_shapes=[
            pltpu.VMEM((seqs, rows, width), BF),
            pltpu.VMEM((2, rows, width), BF),
            pltpu.VMEM((seqs, rows, mix), BF),
            pltpu.VMEM((seqs, rows, ff), BF),
            pltpu.VMEM((seqs, rows, local), BF),
            pltpu.VMEM((8, mix), F32),
        ]
        + [pair, block, pair, block, block]
        + [dma((2,))]
        + [dma((HALF,))] * 12,
        compiler_params=pltpu.CompilerParams(
            collective_id=3, has_side_effects=True, vmem_limit_bytes=VMEM_BYTES
        ),
        name="second_layer",
    )(lens, xown, gg, w, wo, vec, rot, hidden)


def vector_rows(vec_part):
    step = 128
    while vec_part % step:
        step //= 2
    return (128 - step + vec_part + 127) // 128


class Owners:
    def __init__(self, here, packed, from_y, acc, from_far, out, sems):
        self.here, self.packed, self.from_y, self.acc, self.from_far, self.out = (
            here, packed, from_y, acc, from_far, out
        )
        self.ys, self.yr, self.zs, self.zr, self.ps, self.pr = sems

    def line(self, i):
        return lax.rem(self.here.far + i, self.here.fars)

    def to_y(self, j, i, r):
        here = self.here
        y = lax.rem(here.y + j, here.ys)
        return remote(
            self.packed.at[self.line(i), r, y], self.from_y.at[j - 1, i, r],
            self.ys.at[j, i, r], self.yr.at[j, i, r], here.device(here.tp, y=y),
        )

    def to_far(self, i, r):
        here = self.here
        return remote(
            self.acc.at[i, r], self.from_far.at[i - 1, r], self.zs.at[i, r], self.zr.at[i, r],
            here.device(here.tp, far=self.line(i)),
        )

    def start(self):
        for i in list(range(1, self.here.fars)) + [0]:
            for r in range(HALF):
                for j in range(1, self.here.ys):
                    self.to_y(j, i, r).start()

    def add(self, i, r):
        here = self.here
        value = self.packed[self.line(i), r, here.y].astype(F32)
        for j in range(1, here.ys):
            self.to_y(j, i, r).wait_recv()
            value = value + self.from_y[j - 1, i, r].astype(F32)
        if i == 0:
            for far in range(1, here.fars):
                self.to_far(far, r).wait_recv()
                value = value + self.from_far[far - 1, r].astype(F32)
        self.acc[i, r] = value.astype(BF)

    def pass_far(self):
        for i in range(1, self.here.fars):
            for r in range(HALF):
                self.add(i, r)
                self.to_far(i, r).start()

    def to_owner(self, r, x):
        here = self.here
        return remote(
            self.acc.at[0, r, x], self.out.at[here.tp], self.ps.at[r, x], self.pr.at[here.tp],
            here.device(here.tp_of(r, x)),
        )

    def hand_out(self):
        here = self.here
        for r in range(HALF):
            self.add(0, r)
            for x in range(2):
                own = here.tp == here.tp_of(r, x)

                @pl.when(jnp.logical_not(own))
                def _():
                    self.to_owner(r, x).start()

                @pl.when(own)
                def _():
                    pltpu.make_async_copy(self.acc.at[0, r, x], self.out.at[here.tp], self.pr.at[here.tp]).start()

    def drain(self):
        here = self.here
        for source in range(TP):
            pltpu.make_async_copy(self.acc.at[0, 0, 0], self.out.at[source], self.pr.at[source]).wait()
        for r in range(HALF):
            for i in range(here.fars):
                for j in range(1, here.ys):
                    self.to_y(j, i, r).wait_send()
                if i:
                    self.to_far(i, r).wait_send()
            for x in range(2):

                @pl.when(here.tp != here.tp_of(r, x))
                def _():
                    self.to_owner(r, x).wait_send()


def third_kernel(head_dim, owners, gown, w, wo, vec, rot, tokens, xg, packed1,
                 qkv_h, prob_h, ctx_h, act_h, slope_h, out_grad1, vrows1, shares,
                 out, r0, r1, ro, rv, rest,
                 gg, work, mixes, sums, qkv, prob, ctx, act, slope, packed0, out_grad0, vrows0,
                 both, met, landed, from_y0, acc0, from_far0, from_y1, acc1, from_far1,
                 loc, keep, os, orr, vs, vr, own_sem, *sems):
    here = Place()
    tp, core, chip, me, total = here.tp, here.core, here.chip, here.me, here.total
    local, ff = wo.shape[0], act.shape[2]
    swap = Exchange(here, both, met, landed, sems[0:4])
    gather = Gather(here, gown, gg, sems[4:8])
    settle0 = Owners(here, packed0, from_y0, acc0, from_far0, r0, sems[8:14])
    settle1 = Owners(here, packed1, from_y1, acc1, from_far1, r1, sems[14:20])
    kept = [(qkv_h, qkv), (prob_h, prob), (slope_h, slope), (act_h, act), (ctx_h, ctx)]
    rows_sent = rv.shape[2]
    vec_part = 13 * gown.shape[1] // total
    greet_all(here)
    gather.start(loc.at[0])

    def share_copy(k):
        owner = core * HALF + across(chip, k)
        return remote(shares.at[k], rest.at[k - 1], sems[20].at[k], sems[21].at[k], here.device(owner))

    for k in range(1, HALF):
        share_copy(k).start()
    settle1.start()
    loads = [pltpu.make_async_copy(a, b, keep.at[i]) for i, (a, b) in enumerate(kept)]
    for copy in loads:
        copy.start()

    def vec_copy(layer, source, step):
        other = lax.rem(me + step, total)
        first = (other * vec_part) // 128
        return remote(
            source.at[pl.ds(first, rows_sent)], rv.at[layer, me], vs.at[layer, step], vr.at[layer, step],
            here.device_of(other),
        )

    def own_vec(layer, vrows):
        first = (me * vec_part) // 128
        return pltpu.make_async_copy(vrows.at[pl.ds(first, rows_sent)], rv.at[layer, me], own_sem.at[layer])

    sender = here.far * here.ys + here.y

    def out_copy(layer, source, j):
        owner = tp * owners + j
        return remote(
            source.at[j], ro.at[layer, sender], os.at[layer, j], orr.at[layer, sender], here.device_of(owner)
        )

    def send(layer, out_grad, vrows):
        def start_all(step, carry):
            vec_copy(layer, vrows, step).start()
            return carry

        lax.fori_loop(1, total, start_all, 0)
        own_vec(layer, vrows).start()
        for j in range(owners):
            owner = tp * owners + j

            @pl.when(owner != me)
            def _():
                out_copy(layer, out_grad, j).start()

            @pl.when(owner == me)
            def _():
                pltpu.make_async_copy(out_grad.at[j], ro.at[layer, sender], orr.at[layer, sender]).start()

    def collect(layer, out_grad, vrows):
        def wait_all(step, carry):
            vec_copy(layer, vrows, step).wait()
            return carry

        lax.fori_loop(1, total, wait_all, 0)
        own_vec(layer, vrows).wait()
        for j in range(owners):
            owner = tp * owners + j

            @pl.when(owner != me)
            def _():
                out_copy(layer, out_grad, j).wait_send()

        for g in range(here.groups):
            pltpu.make_async_copy(out_grad.at[0], ro.at[layer, g], orr.at[layer, g]).wait()

    send(1, out_grad1, vrows1)
    sums[...] = jnp.zeros_like(sums)
    for copy in loads[:3]:
        copy.wait()

    def one(other, seq):
        mixed = [qkv[seq, :, i * local : (i + 1) * local] for i in range(3)]
        probs = [prob[seq, h] for h in range(local // head_dim)]
        back, mixed_grad, expanded_grad = seq_backward(
            work[other], mixed, probs, slope[seq], head_dim, w, wo, vec, rot
        )
        mixes[seq, :, : 3 * local] = mixed_grad
        mixes[seq, :, 3 * local :] = expanded_grad
        sums[:, : 3 * local] += fold_rows(mixed_grad)
        sums[:, 3 * local :] += fold_rows(expanded_grad)
        return back

    for k in range(HALF):
        if k:
            gather.wait_block(k)
            swap.hand_over(k - 1)
            gather.wait_passed(k)
        else:
            gather.wait_partner()
        block = across(chip, k)
        gather.settle(k, work)

        def part_of(other, carry):
            both[other, k] = one(other, pick(core, other) * HALF + block).astype(BF)
            return carry

        lax.fori_loop(0, 2, part_of, 0)
        swap.to_partner(k).start()
        if k == 2:
            settle1.pass_far()
    for copy in loads[3:]:
        copy.wait()
    weight_grads(xg, gg, mixes, act, ctx, w, vec, sums, packed0, out_grad0, vrows0, gg[tp], tp)
    settle0.start()
    swap.hand_over(HALF - 1)
    settle1.hand_out()
    send(0, out_grad0, vrows0)
    settle0.pass_far()
    swap.wait_landed()

    def finish_back(at):
        value = swap.total(at)
        centred, scale = norm_parts(tokens[at].astype(F32))
        xhat = centred * scale
        mean_one = jnp.mean(value, -1, keepdims=True)
        mean_two = jnp.mean(value * xhat, -1, keepdims=True)
        out[at] = (gg[tp, at].astype(F32) + scale * (value - mean_one - xhat * mean_two)).astype(BF)

    chunks(tokens.shape[0], finish_back)
    settle0.hand_out()
    gather.drain()
    swap.drain()
    collect(1, out_grad1, vrows1)
    collect(0, out_grad0, vrows0)
    settle1.drain()
    settle0.drain()
    for k in range(1, HALF):
        share_copy(k).wait()


def third_layer(here, head_dim, gown, w, wo, vec, rot, tokens, xg, kept, packed1, out_grad1, vrows1, shares):
    seqs, rows, width = xg.shape
    local = wo.shape[0]
    ff = (w.shape[1] - 3 * local) // 2
    mix = 3 * local + ff
    total, fars, ys = here.total, here.fars, here.ys
    owners, shard = out_grad1.shape[:2]
    dma = pltpu.SemaphoreType.DMA
    block = pltpu.VMEM((HALF, rows, width), BF)
    pair = pltpu.VMEM((2, HALF, rows, width), BF)
    unit = (HALF, 2, shard, w.shape[1])
    settle = [pltpu.VMEM(n + unit, BF) for n in ((ys - 1, fars), (fars,), (fars - 1,))]
    settle_sems = [dma((ys, fars, HALF))] * 2 + [dma((fars, HALF))] * 2 + [dma((HALF, 2)), dma((TP,))]
    sent = vector_rows(13 * width // total)
    owned = jax.ShapeDtypeStruct((TP, shard, w.shape[1]), BF)
    return pl.pallas_call(
        functools.partial(third_kernel, head_dim, owners),
        out_shape=[
            jax.ShapeDtypeStruct((rows, width), BF),
            owned,
            owned,
            jax.ShapeDtypeStruct((LAYERS, here.groups, shard, width), BF),
            jax.ShapeDtypeStruct((LAYERS, total, sent, 1, 128), F32),
            jax.ShapeDtypeStruct((HALF - 1, rows, width), BF),
        ],
        in_specs=[VMEM] * 8 + [ANY] * 8,
        out_specs=[VMEM] + [ANY] * 5,
        scratch_shapes=[
            pltpu.VMEM((seqs, rows, width), BF),
            pltpu.VMEM((2, rows, width), BF),
            pltpu.VMEM((seqs, rows, mix), BF),
            pltpu.VMEM((8, mix), F32),
        ]
        + [pltpu.VMEM(a.shape, BF) for a in kept]
        + [pltpu.VMEM(packed1.shape, BF), pltpu.VMEM(out_grad1.shape, BF), pltpu.VMEM(vrows1.shape, F32)]
        + [pair, block, block]
        + settle * 2
        + [
            dma((1,)), dma((5,)), dma((LAYERS, owners)), dma((LAYERS, here.groups)),
            dma((LAYERS, total)), dma((LAYERS, total)), dma((LAYERS,)),
        ]
        + [dma((HALF,))] * 8
        + settle_sems * 2
        + [dma((HALF,))] * 2,
        compiler_params=pltpu.CompilerParams(
            collective_id=4, has_side_effects=True, vmem_limit_bytes=VMEM_BYTES
        ),
        name="third_layer",
    )(gown, w, wo, vec, rot, tokens, xg, packed1, *kept, out_grad1, vrows1, shares)


def adam_kernel(groups, local, ff, fixes, r0, r1, ro, *refs):
    params, moments, squares = refs[0:4], refs[4:8], refs[8:12]
    grads, changes, new_moments, new_squares = refs[12:16], refs[16:20], refs[20:24], refs[24:28]
    first_fix, second_fix = fixes[0], fixes[1]

    def update(which, at, gradient):
        moment = BETA_FIRST * moments[which][0, :, at] + (1.0 - BETA_FIRST) * gradient
        square = BETA_SECOND * squares[which][0, :, at] + (1.0 - BETA_SECOND) * gradient * gradient
        grads[which][0, :, at] = gradient
        new_moments[which][0, :, at] = moment
        new_squares[which][0, :, at] = square
        changes[which][0, :, at] = -LEARNING * (
            moment / first_fix / (jnp.sqrt(square / second_fix) + ADAM_EPSILON)
            + DECAY_RATE * params[which][0, :, at]
        )

    def layer(source):
        for p in range(TP):
            value = source[p].astype(F32)
            for i in range(3):
                start = i * TP * local + p * local
                update(0, slice(start, start + local), value[:, i * local : (i + 1) * local])
            split = 3 * local
            at = slice(p * ff, (p + 1) * ff)
            update(2, at, value[:, split : split + ff])
            update(3, at, value[:, split + ff :])
        value = ro[0, 0].astype(F32)
        for g in range(1, groups):
            value = value + ro[0, g].astype(F32)
        update(1, slice(None), value)

    @pl.when(pl.program_id(0) == 0)
    def _():
        layer(r0)

    @pl.when(pl.program_id(0) == 1)
    def _():
        layer(r1)


def adam_step(groups, local, ff, fixes, r0, r1, ro, params, moments, squares):
    shard = ro.shape[2]
    part = 8
    specs = [pl.BlockSpec((1, part, a.shape[2]), lambda l, r: (l, r, 0)) for a in params]
    source = lambda layer: pl.BlockSpec(
        (r0.shape[0], part, r0.shape[2]), lambda l, r: (0, jnp.where(l == layer, r, (1 - layer) * (shard // part - 1)), 0)
    )
    outs = [jax.ShapeDtypeStruct(a.shape, F32) for a in params]
    return pl.pallas_call(
        functools.partial(adam_kernel, groups, local, ff),
        grid=(LAYERS, shard // part),
        in_specs=[SMEM, source(0), source(1), pl.BlockSpec((1, groups, part, ro.shape[3]), lambda l, r: (l, 0, r, 0))]
        + specs * 3,
        out_specs=specs * 4,
        out_shape=outs * 4,
        compiler_params=pltpu.CompilerParams(vmem_limit_bytes=VMEM_BYTES),
        name="adam_step",
    )(fixes, r0, r1, ro, *params, *moments, *squares)


def rotary(row_count, width, head_dim):
    rot_dim = head_dim // 4
    half_rot = rot_dim // 2
    column = jnp.arange(width, dtype=jnp.int32) % head_dim
    freq_slot = (column % half_rot).astype(F32)
    frequency = 10000.0 ** (-(freq_slot * 2.0) / rot_dim)
    angles = jnp.arange(row_count, dtype=F32)[:, None] * frequency[None, :]
    inside = (column < rot_dim)[None, :]
    first_half = (column < half_rot)[None, :]
    sine = jnp.sin(angles)
    return jnp.stack(
        [
            jnp.where(inside, jnp.cos(angles), 1.0),
            jnp.where(first_half, -sine, 0.0),
            jnp.where(inside & jnp.logical_not(first_half), sine, 0.0),
        ]
    )


def standard(values):
    centred = values - jnp.mean(values, -1, keepdims=True)
    return centred * lax.rsqrt(jnp.mean(centred * centred, -1, keepdims=True) + NORM_EPSILON)


def adam_update(weight, moment, square, gradient, first_fix, second_fix):
    moment = BETA_FIRST * moment + (1.0 - BETA_FIRST) * gradient
    square = BETA_SECOND * square + (1.0 - BETA_SECOND) * gradient * gradient
    change = -LEARNING * (
        moment / first_fix / (jnp.sqrt(square / second_fix) + ADAM_EPSILON) + DECAY_RATE * weight
    )
    return (change, moment, square)


def per_device(tokens, cotangent, seq_lengths, seq_device, step_count, *state):
    params, moments, squares = state[0:5], state[5:10], state[10:15]
    attend_in, attend_out, expand_weight, reduce_weight, layer_vectors = params
    here = Place()
    tp, me, total, groups = here.tp, here.me, here.total, here.groups
    rows, width = tokens.shape
    shard = attend_in.shape[1]
    head_dim = width // HEADS
    local = width // TP
    ff = expand_weight.shape[2] // TP
    vec_part = layer_vectors.shape[1]
    owners = local // shard
    plane_ids = here.flat(here.far, here.y, jnp.arange(TP, dtype=jnp.int32))
    lens = jnp.sum(jnp.where(plane_ids[:, None] == seq_device[None, :], seq_lengths[None, :], 0), 1)
    lens = jnp.broadcast_to(lens[:, None, None], (TP, 1, rows))
    own_length = jnp.sum(jnp.where(seq_device == me, seq_lengths, 0))
    valid = jnp.arange(rows, dtype=jnp.int32)[:, None] < own_length
    rot = rotary(rows, local, head_dim)

    blocks = [
        jnp.concatenate(
            [
                attend_in[l].astype(BF).reshape(shard, 3, TP, local).transpose(2, 0, 1, 3).reshape(TP, shard, 3 * local),
                expand_weight[l].astype(BF).reshape(shard, TP, ff).transpose(1, 0, 2),
                reduce_weight[l].astype(BF).reshape(shard, TP, ff).transpose(1, 0, 2),
            ],
            2,
        )
        for l in range(LAYERS)
    ]
    vec = jnp.pad(layer_vectors.astype(BF).astype(F32).reshape(-1), (0, 8 * 128 - 2 * vec_part)).reshape(8, 128)
    xhat_own = standard(tokens.astype(F32)).astype(BF)
    grad_own = jnp.where(valid, cotangent, jnp.zeros_like(cotangent))
    xg, w0, w1, wog, vecg = spread(here, xhat_own, blocks[0], blocks[1], attend_out.astype(BF), vec)
    w0, w1 = w0.reshape(width, -1), w1.reshape(width, -1)
    out_rows = wog.transpose(1, 0, 2, 3).reshape(LAYERS, local, width)
    vectors = vecg.reshape(total, -1)[:, : 2 * vec_part].reshape(total, LAYERS, vec_part)
    vectors = vectors.transpose(1, 0, 2).reshape(LAYERS, 13, width)
    vectors = jnp.pad(vectors, ((0, 0), (0, 3), (0, 0)))

    hidden0, xnext, grads_all, *kept = first_layer(
        head_dim, lens, xg, w0, out_rows[0], vectors[0], rot, tokens, grad_own
    )
    shares, grad0, packed1, out_grad1, vrows1 = second_layer(
        here, head_dim, owners, shard, lens, xnext, grads_all, w1, out_rows[1], vectors[1], rot, hidden0
    )
    input_grad, r0, r1, ro, rv, rest = third_layer(
        here, head_dim, grad0, w0, out_rows[0], vectors[0], rot, tokens, xg, kept, packed1, out_grad1, vrows1, shares
    )
    hidden1 = hidden0.astype(F32) + (vectors[1, 7:8] + vectors[1, 12:13]) + shares[0].astype(F32)
    hidden1 = (hidden1 + jnp.sum(rest.astype(F32), 0)).astype(BF)
    step_float = step_count[0].astype(F32)
    first_fix = 1.0 - jnp.power(BETA_FIRST, step_float)
    second_fix = 1.0 - jnp.power(BETA_SECOND, step_float)
    big = adam_step(
        groups, local, ff, jnp.stack([first_fix, second_fix]), r0, r1, ro, params[:4], moments[:4], squares[:4]
    )
    vec_rows = jnp.sum(rv, 1).reshape(LAYERS, -1)
    grad_vec = lax.dynamic_slice_in_dim(vec_rows, lax.rem(me * vec_part, 128), vec_part, 1)
    small = (grad_vec,) + adam_update(params[4], moments[4], squares[4], grad_vec, first_fix, second_fix)
    results = []
    for i in range(4):
        results += list(big[4 * i : 4 * i + 4]) + [small[i]]
    return (jnp.stack([hidden0, hidden1]), input_grad, *results)


def solution(mesh):
    devices = mesh.devices.reshape(-1)
    blocks = devices.size // TP
    fars = 1 << ((blocks.bit_length()) // 2)
    flat = Mesh(devices.reshape(fars, 2, 2, blocks // fars, 2), AXES)
    by_row = P(AXES, None)
    by_dim = [P(None, AXES, None)] * 4 + [P(None, AXES)]
    return jax.shard_map(
        per_device,
        mesh=flat,
        in_specs=(by_row, by_row, P(), P(), P(), *(by_dim * 3)),
        out_specs=(P(None, AXES, None), by_row, *(by_dim * 4)),
        check_vma=False,
    )
```

```python
import functools

import jax
import jax.numpy as jnp
from jax import lax
from jax.experimental import pallas as pl
from jax.experimental.pallas import tpu as pltpu
from jax.sharding import Mesh
from jax.sharding import PartitionSpec as P

HEADS = 16
LAYERS = 2
NORM_EPSILON = 1e-05
ADAM_EPSILON = 1e-08
LEARNING = 0.02
BETA_FIRST = 0.9
BETA_SECOND = 0.95
DECAY_RATE = 0.1
MASKED_SCORE = -1e30

TP = 8
HALF = TP // 2
BF = jnp.bfloat16
F32 = jnp.float32
MESH = pl.DeviceIdType.MESH
NT = (((1,), (1,)), ((), ()))
TN = (((0,), (0,)), ((), ()))
ANY = pl.BlockSpec(memory_space=pl.ANY)
VMEM = pl.BlockSpec(memory_space=pltpu.VMEM)
SMEM = pl.BlockSpec(memory_space=pltpu.SMEM)
VMEM_BYTES = 67043328


AXES = ("far", "near", "core", "y", "x")


class Place:
    def __init__(self):
        self.far, near, core, self.y, x = (lax.axis_index(name) for name in AXES)
        self.fars, self.ys = lax.axis_size("far"), lax.axis_size("y")
        self.tp = core * HALF + near * 2 + x
        self.row = near * 2 + core
        self.x = x
        self.core, self.chip = core, near * 2 + x
        self.partner = (1 - core) * HALF + self.chip
        self.groups, self.total = self.fars * self.ys, self.fars * self.ys * TP
        self.me = self.flat(self.far, self.y, self.tp)

    def flat(self, far, y, tp):
        near, core, x = lax.rem(tp // 2, 2), tp // HALF, lax.rem(tp, 2)
        return (((far * 2 + near) * 2 + core) * self.ys + y) * 2 + x

    def device(self, tp, far=None, y=None):
        far = self.far if far is None else far
        y = self.y if y is None else y
        return far, lax.rem(tp // 2, 2), tp // HALF, y, lax.rem(tp, 2)

    def device_of(self, flat):
        rest = flat // 2
        y, rest = lax.rem(rest, self.ys), rest // self.ys
        core, rest = lax.rem(rest, 2), rest // 2
        return rest // 2, lax.rem(rest, 2), core, y, lax.rem(flat, 2)

    def tp_of(self, row, x):
        return (row % 2) * HALF + (row // 2) * 2 + x


def nn_dot(a, b):
    return jnp.dot(a, b, preferred_element_type=F32)


def nt_dot(a, b):
    return lax.dot_general(a, b, NT, preferred_element_type=F32)


def tn_dot(a, b):
    return lax.dot_general(a, b, TN, preferred_element_type=F32)


def remote(src, dst, send, recv, target):
    return pltpu.make_async_remote_copy(
        src_ref=src, dst_ref=dst, send_sem=send, recv_sem=recv, device_id=target, device_id_type=MESH
    )


def greet(targets):
    barrier = pltpu.get_barrier_semaphore()
    for target in targets:
        pl.semaphore_signal(barrier, inc=1, device_id=target, device_id_type=MESH)
    pl.semaphore_wait(barrier, len(targets))


def greet_all(here):
    barrier = pltpu.get_barrier_semaphore()

    def signal(step, carry):
        other = lax.rem(here.me + step, here.total)
        pl.semaphore_signal(barrier, inc=1, device_id=here.device_of(other), device_id_type=MESH)
        return carry

    lax.fori_loop(1, here.total, signal, 0)
    pl.semaphore_wait(barrier, here.total - 1)


def spread_kernel(owners, xh, gr, s0, s1, wo, vec, xg, gg, w0, w1, wog, vecg,
                  ps, pr, zs, zr, ys, yr, os, orr, vs, vr, loc, *sems):
    here = Place()
    far, y, tp, row, x = here.far, here.y, here.tp, here.row, here.x
    gather_x = Gather(here, xh, xg, sems[0:4])
    gather_g = Gather(here, gr, gg, sems[4:8])
    layers = ((s0, w0), (s1, w1))
    greet_all(here)

    def within(l, step):
        source, w = layers[l]
        peer = lax.rem(tp + step, TP)
        return remote(
            source.at[peer], w.at[far, row, y, x], ps.at[l, step], pr.at[l, tp], here.device(peer)
        )

    def start_layer(l):
        source, w = layers[l]
        for step in range(1, TP):
            within(l, step).start()
        pltpu.make_async_copy(source.at[tp], w.at[far, row, y, x], pr.at[l, tp]).start()

    def vec_copy(step):
        other = lax.rem(here.me + step, here.total)
        return remote(vec, vecg.at[here.me], vs.at[step], vr.at[step], here.device_of(other))

    def start_vec(step, carry):
        vec_copy(step).start()
        return carry

    def wait_vec(step, carry):
        vec_copy(step).wait()
        return carry

    start_layer(0)
    start_layer(1)
    lax.fori_loop(1, here.total, start_vec, 0)
    own_vec = pltpu.make_async_copy(vec, vecg.at[here.me], loc.at[1])
    own_vec.start()
    slot = lax.rem(here.me, owners)
    user = here.me // owners

    def out_copy(f, v):
        return remote(wo, wog.at[slot], os.at[f, v], orr.at[slot], here.device(user, f, v))

    def is_own(f, v):
        return (user == tp) & (f == far) & (v == y)

    blocks = [(f, v) for f in range(here.fars) for v in range(here.ys)]
    for f, v in blocks:

        @pl.when(jnp.logical_not(is_own(f, v)))
        def _():
            out_copy(f, v).start()

        @pl.when(is_own(f, v))
        def _():
            pltpu.make_async_copy(wo, wog.at[slot], orr.at[slot]).start()

    def along_far(l, i, r):
        part = layers[l][1].at[far, r, y]
        target = lax.rem(far + i, here.fars)
        return remote(part, part, zs.at[l, i, r], zr.at[l, i, r], here.device(tp, far=target))

    def along_y(l, j, i, r):
        part = layers[l][1].at[lax.rem(far + here.fars - i, here.fars), r, y]
        target = lax.rem(y + j, here.ys)
        return remote(part, part, ys.at[l, j, i, r], yr.at[l, j, i, r], here.device(tp, y=target))

    def landed(l, f, r, v, sem):
        part = layers[l][1].at[f, r, v]
        remote(part, part, sem, sem, here.device(here.partner)).wait_recv()

    def first_hop(l):
        source, w = layers[l]
        for r in range(HALF):
            for side in range(2):
                t = here.tp_of(r, side)
                pltpu.make_async_copy(source.at[0], w.at[far, r, y, side], pr.at[l, t]).wait()
            for i in range(1, here.fars):
                along_far(l, i, r).start()
            for j in range(1, here.ys):
                along_y(l, j, 0, r).start()

    first_hop(0)
    first_hop(1)
    gather_x.start(loc.at[0])
    gather_g.start(loc.at[2])
    for l in range(LAYERS):
        for r in range(HALF):
            for i in range(1, here.fars):
                landed(l, lax.rem(far + here.fars - i, here.fars), r, y, zr.at[l, i, r])
                for j in range(1, here.ys):
                    along_y(l, j, i, r).start()
    for gather in (gather_x, gather_g):
        for k in range(1, HALF):
            gather.wait_block(k)
    for gather in (gather_x, gather_g):
        gather.wait_partner()
        for k in range(1, HALF):
            gather.wait_passed(k)
    for l in range(LAYERS):
        for j in range(1, here.ys):
            for i in range(here.fars):
                for r in range(HALF):
                    landed(
                        l, lax.rem(far + here.fars - i, here.fars), r, lax.rem(y + here.ys - j, here.ys),
                        yr.at[l, j, i, r],
                    )
    lax.fori_loop(1, here.total, wait_vec, 0)
    own_vec.wait()
    for j in range(owners):
        pltpu.make_async_copy(wo, wog.at[j], orr.at[j]).wait()
    gather_x.drain()
    gather_g.drain()
    for l in range(LAYERS):
        for step in range(1, TP):
            within(l, step).wait_send()
        for r in range(HALF):
            for i in range(1, here.fars):
                along_far(l, i, r).wait_send()
            for j in range(1, here.ys):
                for i in range(here.fars):
                    along_y(l, j, i, r).wait_send()
    for f, v in blocks:

        @pl.when(jnp.logical_not(is_own(f, v)))
        def _():
            out_copy(f, v).wait_send()


def spread(here, xh, gr, s0, s1, wo, vec):
    rows, cols = s0.shape[1:]
    owners = wo.shape[2] // TP // rows
    dma = pltpu.SemaphoreType.DMA
    whole = jax.ShapeDtypeStruct((here.fars, HALF, here.ys, 2, rows, cols), BF)
    gathered = jax.ShapeDtypeStruct((TP,) + xh.shape, BF)
    return pl.pallas_call(
        functools.partial(spread_kernel, owners),
        out_shape=(
            gathered,
            gathered,
            whole,
            whole,
            jax.ShapeDtypeStruct((owners,) + wo.shape, BF),
            jax.ShapeDtypeStruct((here.total,) + vec.shape, F32),
        ),
        in_specs=[VMEM] * 2 + [ANY] * 4,
        out_specs=(ANY,) * 6,
        scratch_shapes=[
            dma((LAYERS, TP)), dma((LAYERS, TP)),
            dma((LAYERS, here.fars, HALF)), dma((LAYERS, here.fars, HALF)),
            dma((LAYERS, here.ys, here.fars, HALF)), dma((LAYERS, here.ys, here.fars, HALF)),
            dma((here.fars, here.ys)), dma((owners,)), dma((here.total,)), dma((here.total,)), dma((3,)),
        ]
        + [dma((HALF,))] * 8,
        compiler_params=pltpu.CompilerParams(collective_id=1, has_side_effects=True),
        name="spread",
    )(xh, gr, s0, s1, wo, vec)


def turn(values, rot):
    return (
        values * rot[0]
        + pltpu.roll(values, values.shape[1] - 8, 1) * rot[1]
        + pltpu.roll(values, 8, 1) * rot[2]
    )


def turn_back(values, rot):
    return (
        values * rot[0]
        + pltpu.roll(values * rot[1], 8, 1)
        + pltpu.roll(values * rot[2], values.shape[1] - 8, 1)
    )


def head_parts(values, head_dim):
    lane = lax.broadcasted_iota(jnp.int32, values.shape, 1)
    zero = jnp.zeros_like(values)
    return [
        jnp.where((lane >= h * head_dim) & (lane < (h + 1) * head_dim), values, zero)
        for h in range(values.shape[1] // head_dim)
    ]


def bias_slices(vec, tp, local, ff):
    width = vec.shape[1]
    b_in = vec[4:7, pl.ds(pl.multiple_of(tp * local, local), local)]
    per_row = width // ff
    row = 8 + tp // per_row
    b_up = vec[pl.ds(row, 1), pl.ds(pl.multiple_of(lax.rem(tp, per_row) * ff, ff), ff)]
    return b_in, b_up


def seq_forward(values, lengths, head_dim, w, wo, vec, b_in, b_up, rot):
    rows = values.shape[0]
    local = wo.shape[0]
    ff = b_up.shape[1]
    values = values.astype(F32)
    normed = (values * vec[0:1] + vec[1:2]).astype(BF)
    mixed = nn_dot(normed, w[:, : 3 * local])
    parts = [mixed[:, i * local : (i + 1) * local] + b_in[i : i + 1] for i in range(3)]
    queries = (turn(parts[0], rot).astype(BF).astype(F32) * head_dim ** (-0.5)).astype(BF)
    keys = turn(parts[1], rot).astype(BF)
    vals = parts[2].astype(BF)
    row = lax.broadcasted_iota(jnp.int32, (rows, rows), 0)
    col = lax.broadcasted_iota(jnp.int32, (rows, rows), 1)
    allowed = (col <= row) & (col < lengths)
    total, probs = None, []
    for q_h, v_h in zip(head_parts(queries, head_dim), head_parts(vals, head_dim)):
        scores = jnp.where(allowed, nt_dot(q_h, keys), MASKED_SCORE)
        weights = jnp.exp(scores - jnp.max(scores, -1, keepdims=True))
        probability = (weights / jnp.sum(weights, -1, keepdims=True)).astype(BF)
        probs.append(probability)
        term = nn_dot(probability, v_h)
        total = term if total is None else total + term
    context = total.astype(BF)
    normed = (values * vec[2:3] + vec[3:4]).astype(BF)
    expanded = nn_dot(normed, w[:, 3 * local : 3 * local + ff]) + b_up
    spread_to = 0.5 * (1.0 + lax.erf(expanded * 0.7071067811865476))
    active = (expanded * spread_to).astype(BF)
    slope = (spread_to + expanded * (0.3989422804014327 * jnp.exp(-0.5 * expanded * expanded))).astype(BF)
    part = nn_dot(context, wo[...]) + nt_dot(active, w[:, 3 * local + ff :])
    return part, (queries, keys, vals), probs, context, active, slope


def seq_backward(grad, qkv, probs, slope, head_dim, w, wo, vec, rot):
    local = wo.shape[0]
    ff = slope.shape[1]
    queries, keys, vals = qkv
    active_grad = nn_dot(grad, w[:, 3 * local + ff :])
    expanded_grad = (slope.astype(F32) * active_grad).astype(BF)
    total = nt_dot(expanded_grad, w[:, 3 * local : 3 * local + ff]) * vec[2:3]
    context_grad = nt_dot(grad, wo[...]).astype(BF)
    query_grad = key_grad = value_grad = 0.0
    for prob_b, c_h, q_h, k_h in zip(
        probs, head_parts(context_grad, head_dim), head_parts(queries, head_dim), head_parts(keys, head_dim)
    ):
        probability = prob_b.astype(F32)
        prob_grad = nt_dot(c_h, vals)
        value_grad = value_grad + tn_dot(prob_b, c_h)
        inner = jnp.sum(probability * prob_grad, -1, keepdims=True)
        score_grad = (probability * (prob_grad - inner)).astype(BF)
        query_grad = query_grad + nn_dot(score_grad, k_h)
        key_grad = key_grad + tn_dot(score_grad, q_h)
    query_grad = query_grad * head_dim ** (-0.5)
    pieces = [turn_back(query_grad, rot).astype(BF), turn_back(key_grad, rot).astype(BF), value_grad.astype(BF)]
    mixed_grad = jnp.concatenate(pieces, 1)
    total = total + nt_dot(mixed_grad, w[:, : 3 * local]) * vec[0:1]
    return total, mixed_grad, expanded_grad


def fold_rows(values):
    return jnp.sum(values.astype(F32).reshape(-1, 8, values.shape[1]), axis=0)


def across(chip, step):
    x = lax.rem(lax.rem(chip, 2) + lax.rem(step, 2), 2)
    y = lax.rem(chip // 2 + step // 2, 2)
    return 2 * y + x


def pick(core, other):
    return core + (1 - 2 * core) * other


CHUNK = 32
ORDER = (0, 3, 1, 2)


def chunks(rows, body):
    def step(i, carry):
        body(pl.ds(pl.multiple_of(i * CHUNK, CHUNK), CHUNK))
        return carry

    lax.fori_loop(0, rows // CHUNK, step, 0)


def norm_parts(values):
    centred = values - jnp.mean(values, -1, keepdims=True)
    return centred, lax.rsqrt(jnp.mean(centred * centred, -1, keepdims=True) + NORM_EPSILON)


class Exchange:
    def __init__(self, here, both, met, landed, sems):
        self.here = here
        self.joined, self.mine, self.met, self.landed = both.at[0], both.at[1], met, landed
        self.ps, self.pr, self.bs, self.br = sems
        self.core, self.chip, self.partner = here.core, here.chip, here.partner

    def to_partner(self, k):
        return remote(
            self.mine.at[k], self.met.at[k], self.ps.at[k], self.pr.at[k], self.here.device(self.partner)
        )

    def to_owner(self, k):
        owner = self.core * HALF + across(self.chip, k)
        return remote(
            self.joined.at[k], self.landed.at[k], self.bs.at[k], self.br.at[k], self.here.device(owner)
        )

    def join(self, k):
        self.to_partner(k).wait_recv()

        def add(at):
            self.joined[k, at] = (self.joined[k, at].astype(F32) + self.met[k, at].astype(F32)).astype(BF)

        chunks(self.met.shape[1], add)

    def hand_over(self, k):
        self.join(k)
        if k:
            self.to_owner(k).start()

    def total(self, at):
        value = self.joined[0, at].astype(F32)
        for k in range(1, HALF):
            value = value + self.landed[k, at].astype(F32)
        return value

    def wait_landed(self):
        for k in range(1, HALF):
            self.to_owner(k).wait_recv()

    def drain(self):
        for k in range(HALF):
            self.to_partner(k).wait_send()
        for k in range(1, HALF):
            self.to_owner(k).wait_send()


class Gather:
    def __init__(self, here, own, buffer, sems):
        self.here, self.own, self.buffer = here, own, buffer
        self.gs, self.gr, self.fs, self.fr = sems
        self.tp, self.core, self.chip, self.partner = here.tp, here.core, here.chip, here.partner

    def to_peer(self, k):
        if isinstance(k, int) and k == 0:
            target = self.partner
        else:
            target = self.core * HALF + across(self.chip, k)
        return remote(self.own, self.buffer.at[self.tp], self.gs.at[k], self.gr.at[k], self.here.device(target))

    def start(self, local):
        pltpu.make_async_copy(self.own, self.buffer.at[self.tp], local).start()
        for k in ORDER[1:] + ORDER[:1]:
            self.to_peer(k).start()
        pltpu.make_async_copy(self.own, self.buffer.at[self.tp], local).wait()

    def pass_on(self, k):
        source = self.core * HALF + across(self.chip, k)
        block = self.buffer.at[source]
        return remote(block, block, self.fs.at[k], self.fr.at[k], self.here.device(self.partner))

    def arrived(self, source, sem):
        block = self.buffer.at[source]
        remote(block, block, sem, sem, self.here.device(self.partner)).wait_recv()

    def wait_block(self, k):
        self.arrived(self.core * HALF + across(self.chip, k), self.gr.at[k])
        self.pass_on(k).start()

    def wait_partner(self):
        self.arrived(self.partner, self.gr.at[0])

    def wait_passed(self, k):
        self.arrived((1 - self.core) * HALF + across(self.chip, k), self.fr.at[k])

    def settle(self, k, work):
        block = across(self.chip, k)
        for other in range(2):
            work[other] = self.buffer[pick(self.core, other) * HALF + block]

    def drain(self):
        for k in range(HALF):
            self.to_peer(k).wait_send()
        for k in range(1, HALF):
            self.pass_on(k).wait_send()


def greet_block(here):
    targets = [here.partner] + [here.core * HALF + across(here.chip, k) for k in range(1, HALF)]
    greet([here.device(target) for target in targets])


def first_kernel(head_dim, lens, xg, w, wo, vec, rot, own,
                 out, xnext, qkv_h, prob_h, ctx_h, act_h, slope_h,
                 qkv, prob, ctx, act, slope, both, met, landed, keep, *sems):
    here = Place()
    tp, core, chip = here.tp, here.core, here.chip
    local, ff = wo.shape[0], act.shape[2]
    swap = Exchange(here, both, met, landed, sems)
    kept = [(qkv, qkv_h), (prob, prob_h), (ctx, ctx_h), (act, act_h), (slope, slope_h)]
    greet_block(here)
    b_in, b_up = bias_slices(vec, tp, local, ff)

    def one(seq):
        part, mixed, probs, context, active, sl = seq_forward(
            xg[seq], lens[seq], head_dim, w, wo, vec, b_in, b_up, rot
        )
        for i, piece in enumerate(mixed):
            qkv[seq, :, i * local : (i + 1) * local] = piece
        for h, p in enumerate(probs):
            prob[seq, h] = p
        ctx[seq] = context
        act[seq] = active
        slope[seq] = sl
        return part

    for k in reversed(range(HALF)):
        block = across(chip, k)

        def part_of(other, carry):
            both[other, k] = one(pick(core, other) * HALF + block).astype(BF)
            return carry

        lax.fori_loop(0, 2, part_of, 0)
        swap.to_partner(k).start()
        if k + 1 < HALF:
            swap.hand_over(k + 1)
    swap.hand_over(0)
    saved = [pltpu.make_async_copy(a, b, keep.at[i]) for i, (a, b) in enumerate(kept)]
    for copy in saved:
        copy.start()
    swap.wait_landed()

    def finish(at):
        result = (own[at].astype(F32) + swap.total(at) + (vec[7:8] + vec[12:13])).astype(BF)
        out[at] = result
        centred, scale = norm_parts(result.astype(F32))
        xnext[at] = (centred * scale).astype(BF)

    chunks(own.shape[0], finish)
    swap.drain()
    for copy in saved:
        copy.wait()


def first_layer(head_dim, lens, xg, w, wo, vec, rot, own):
    seqs, rows, width = xg.shape
    local = wo.shape[0]
    ff = (w.shape[1] - 3 * local) // 2
    dma = pltpu.SemaphoreType.DMA
    kept = [
        (seqs, rows, 3 * local), (seqs, local // head_dim, rows, rows), (seqs, rows, local), (seqs, rows, ff),
        (seqs, rows, ff),
    ]
    block = pltpu.VMEM((HALF, rows, width), BF)
    pair = pltpu.VMEM((2, HALF, rows, width), BF)
    return pl.pallas_call(
        functools.partial(first_kernel, head_dim),
        out_shape=[jax.ShapeDtypeStruct((rows, width), BF)] * 2
        + [jax.ShapeDtypeStruct(s, BF) for s in kept],
        in_specs=[VMEM] * 7,
        out_specs=[VMEM] * 2 + [ANY] * 5,
        scratch_shapes=[pltpu.VMEM(s, BF) for s in kept] + [pair, block, block] + [dma((5,))] + [dma((HALF,))] * 4,
        compiler_params=pltpu.CompilerParams(
            collective_id=2, has_side_effects=True, vmem_limit_bytes=VMEM_BYTES
        ),
        name="first_layer",
    )(lens, xg, w, wo, vec, rot, own)


def weight_grads(xg, gg, mixes, act, ctx, w, vec, sums, packed, out_grad, vrows, grad_rows, tp):
    local, width = out_grad.shape[0] * out_grad.shape[1], out_grad.shape[2]
    fars, _, ys, _, shard, cols = packed.shape
    ff = act.shape[2]
    split = 3 * local
    rows = xg.shape[0] * xg.shape[1]
    flat = lambda ref, cut: ref[:, :, cut].reshape(rows, -1)
    everything = slice(None)
    col_sums = jnp.sum(sums[...], axis=0, keepdims=True)
    half = width // 2
    ones = jnp.ones((8, split), F32)
    wide = jnp.ones((8, ff), F32)
    exact = lambda a, b: lax.dot_general(a, b, NT, preferred_element_type=F32, precision=lax.Precision.HIGHEST)
    for c in range(2):
        cut = slice(c * half, (c + 1) * half)
        lines = slice(c * fars // 2, (c + 1) * fars // 2)
        shape = (fars // 2, HALF, ys, 2, shard)
        gains = vec[0:4, cut].T
        cross = tn_dot(flat(xg, cut), flat(mixes, everything))
        in_cross, up_cross = cross[:, :split], cross[:, split:]
        in_grad = gains[:, 0:1] * in_cross + gains[:, 1:2] * col_sums[:, :split]
        up_grad = gains[:, 2:3] * up_cross + gains[:, 3:4] * col_sums[:, split:]
        down_grad = tn_dot(flat(gg, cut), flat(act, everything))
        packed[lines, :, :, :, :, :split] = in_grad.astype(BF).reshape(shape + (split,))
        packed[lines, :, :, :, :, split : split + ff] = up_grad.astype(BF).reshape(shape + (ff,))
        packed[lines, :, :, :, :, split + ff :] = down_grad.astype(BF).reshape(shape + (ff,))
        w_in = w[cut, :split].astype(F32)
        w_up = w[cut, split : split + ff].astype(F32)
        norm_rows = [
            exact(ones, w_in * in_cross)[0:1],
            exact(jnp.broadcast_to(col_sums[:, :split], (8, split)), w_in)[0:1],
            exact(wide, w_up * up_cross)[0:1],
            exact(jnp.broadcast_to(col_sums[:, split:], (8, ff)), w_up)[0:1],
        ]
        for i, line in enumerate(norm_rows):
            for j in range(half // 128):
                vrows[i * (width // 128) + c * (half // 128) + j] = line[:, j * 128 : (j + 1) * 128]
        part = tn_dot(flat(ctx, everything), flat(gg, cut)).astype(BF)
        out_grad[:, :, cut] = part.reshape(-1, shard, half)
    per = width // 128
    base = 4 * per

    def clear(i, carry):
        vrows[base + i] = jnp.zeros((1, 128), F32)
        return carry

    lax.fori_loop(0, vrows.shape[0] - base, clear, 0)
    step = local // 128
    for i in range(3):
        for j in range(step):
            vrows[base + i * per + tp * step + j] = col_sums[:, i * local + j * 128 : i * local + (j + 1) * 128]
    base = 8 * per
    for j in range(ff // 128):
        vrows[base + tp * (ff // 128) + j] = col_sums[:, split + j * 128 : split + (j + 1) * 128]
    bias = jnp.sum(grad_rows.astype(F32), axis=0, keepdims=True)
    for j in range(per):
        vrows[7 * per + j] = bias[:, j * 128 : (j + 1) * 128]
        vrows[12 * per + j] = bias[:, j * 128 : (j + 1) * 128]


def second_kernel(head_dim, lens, xown, gg, w, wo, vec, rot, hidden,
                  out, grad_next, packed, out_grad, vrows,
                  xg, work, mixes, act, ctx, sums, both, met, landed, both_e, met_e, landed_e,
                  loc, *sems):
    here = Place()
    tp, core, chip = here.tp, here.core, here.chip
    local, ff = wo.shape[0], act.shape[2]
    swap = Exchange(here, both, met, landed, sems[0:4])
    swap_e = Exchange(here, both_e, met_e, landed_e, sems[4:8])
    gather = Gather(here, xown, xg, sems[8:12])
    greet_block(here)
    gather.start(loc.at[0])
    sums[...] = jnp.zeros_like(sums)
    b_in, b_up = bias_slices(vec, tp, local, ff)

    def one(other, seq):
        part, mixed, probs, context, active, sl = seq_forward(
            work[other], lens[seq], head_dim, w, wo, vec, b_in, b_up, rot
        )
        ctx[seq] = context
        act[seq] = active
        back, mixed_grad, expanded_grad = seq_backward(
            gg[seq], mixed, probs, sl, head_dim, w, wo, vec, rot
        )
        mixes[seq, :, : 3 * local] = mixed_grad
        mixes[seq, :, 3 * local :] = expanded_grad
        sums[:, : 3 * local] += fold_rows(mixed_grad)
        sums[:, 3 * local :] += fold_rows(expanded_grad)
        return part, back

    for n, k in enumerate(ORDER):
        if k:
            gather.wait_block(k)
            swap_e.hand_over(ORDER[n - 1])
            swap.hand_over(ORDER[n - 1])
            gather.wait_passed(k)
        else:
            gather.wait_partner()
        block = across(chip, k)
        gather.settle(k, work)

        def part_of(other, carry):
            part, back = one(other, pick(core, other) * HALF + block)
            both[other, k] = part.astype(BF)
            both_e[other, k] = back.astype(BF)
            return carry

        lax.fori_loop(0, 2, part_of, 0)
        swap_e.to_partner(k).start()
        swap.to_partner(k).start()
    swap_e.hand_over(ORDER[-1])
    swap.hand_over(ORDER[-1])
    weight_grads(xg, gg, mixes, act, ctx, w, vec, sums, packed, out_grad, vrows, gg[tp], tp)
    swap_e.wait_landed()

    def finish_back(at):
        total = swap_e.total(at)
        centred, scale = norm_parts(hidden[at].astype(F32))
        xhat = centred * scale
        mean_one = jnp.mean(total, -1, keepdims=True)
        mean_two = jnp.mean(total * xhat, -1, keepdims=True)
        grad_next[at] = (
            gg[tp, at].astype(F32) + scale * (total - mean_one - xhat * mean_two)
        ).astype(BF)

    chunks(hidden.shape[0], finish_back)
    swap.wait_landed()

    def finish(at):
        out[at] = (hidden[at].astype(F32) + swap.total(at) + (vec[7:8] + vec[12:13])).astype(BF)

    chunks(hidden.shape[0], finish)
    gather.drain()
    swap.drain()
    swap_e.drain()


def second_layer(here, head_dim, owners, shard, lens, xown, gg, w, wo, vec, rot, hidden):
    seqs, rows, width = gg.shape
    local = wo.shape[0]
    ff = (w.shape[1] - 3 * local) // 2
    mix = 3 * local + ff
    dma = pltpu.SemaphoreType.DMA
    block = pltpu.VMEM((HALF, rows, width), BF)
    pair = pltpu.VMEM((2, HALF, rows, width), BF)
    return pl.pallas_call(
        functools.partial(second_kernel, head_dim),
        out_shape=[
            jax.ShapeDtypeStruct((rows, width), BF),
            jax.ShapeDtypeStruct((rows, width), BF),
            jax.ShapeDtypeStruct((here.fars, HALF, here.ys, 2, shard, w.shape[1]), BF),
            jax.ShapeDtypeStruct((owners, shard, width), BF),
            jax.ShapeDtypeStruct((13 * width // 128, 1, 128), F32),
        ],
        in_specs=[VMEM] * 8,
        out_specs=[VMEM] * 5,
        scratch_shapes=[
            pltpu.VMEM((seqs, rows, width), BF),
            pltpu.VMEM((2, rows, width), BF),
            pltpu.VMEM((seqs, rows, mix), BF),
            pltpu.VMEM((seqs, rows, ff), BF),
            pltpu.VMEM((seqs, rows, local), BF),
            pltpu.VMEM((8, mix), F32),
        ]
        + [pair, block, block] * 2
        + [dma((1,))]
        + [dma((HALF,))] * 12,
        compiler_params=pltpu.CompilerParams(
            collective_id=3, has_side_effects=True, vmem_limit_bytes=VMEM_BYTES
        ),
        name="second_layer",
    )(lens, xown, gg, w, wo, vec, rot, hidden)


def vector_rows(vec_part):
    step = 128
    while vec_part % step:
        step //= 2
    return (128 - step + vec_part + 127) // 128


class Owners:
    def __init__(self, here, packed, from_y, acc, from_far, out, sems):
        self.here, self.packed, self.from_y, self.acc, self.from_far, self.out = (
            here, packed, from_y, acc, from_far, out
        )
        self.ys, self.yr, self.zs, self.zr, self.ps, self.pr = sems

    def line(self, i):
        return lax.rem(self.here.far + i, self.here.fars)

    def to_y(self, j, i, r):
        here = self.here
        y = lax.rem(here.y + j, here.ys)
        return remote(
            self.packed.at[self.line(i), r, y], self.from_y.at[j - 1, i, r],
            self.ys.at[j, i, r], self.yr.at[j, i, r], here.device(here.tp, y=y),
        )

    def to_far(self, i, r):
        here = self.here
        return remote(
            self.acc.at[i, r], self.from_far.at[i - 1, r], self.zs.at[i, r], self.zr.at[i, r],
            here.device(here.tp, far=self.line(i)),
        )

    def start(self):
        for i in list(range(1, self.here.fars)) + [0]:
            for r in range(HALF):
                for j in range(1, self.here.ys):
                    self.to_y(j, i, r).start()

    def add(self, i, r):
        here = self.here
        value = self.packed[self.line(i), r, here.y].astype(F32)
        for j in range(1, here.ys):
            self.to_y(j, i, r).wait_recv()
            value = value + self.from_y[j - 1, i, r].astype(F32)
        if i == 0:
            for far in range(1, here.fars):
                self.to_far(far, r).wait_recv()
                value = value + self.from_far[far - 1, r].astype(F32)
        self.acc[i, r] = value.astype(BF)

    def pass_far(self):
        for i in range(1, self.here.fars):
            for r in range(HALF):
                self.add(i, r)
                self.to_far(i, r).start()

    def to_owner(self, r, x):
        here = self.here
        return remote(
            self.acc.at[0, r, x], self.out.at[here.tp], self.ps.at[r, x], self.pr.at[here.tp],
            here.device(here.tp_of(r, x)),
        )

    def hand_out(self):
        here = self.here
        for r in range(HALF):
            self.add(0, r)
            for x in range(2):
                own = here.tp == here.tp_of(r, x)

                @pl.when(jnp.logical_not(own))
                def _():
                    self.to_owner(r, x).start()

                @pl.when(own)
                def _():
                    pltpu.make_async_copy(self.acc.at[0, r, x], self.out.at[here.tp], self.pr.at[here.tp]).start()

    def drain(self):
        here = self.here
        for source in range(TP):
            pltpu.make_async_copy(self.acc.at[0, 0, 0], self.out.at[source], self.pr.at[source]).wait()
        for r in range(HALF):
            for i in range(here.fars):
                for j in range(1, here.ys):
                    self.to_y(j, i, r).wait_send()
                if i:
                    self.to_far(i, r).wait_send()
            for x in range(2):

                @pl.when(here.tp != here.tp_of(r, x))
                def _():
                    self.to_owner(r, x).wait_send()


def third_kernel(head_dim, owners, gown, w, wo, vec, rot, tokens, xg, packed1,
                 qkv_h, prob_h, ctx_h, act_h, slope_h, out_grad1, vrows1,
                 out, r0, r1, ro, rv,
                 gg, work, mixes, sums, qkv, prob, ctx, act, slope, packed0, out_grad0, vrows0,
                 both, met, landed, from_y0, acc0, from_far0, from_y1, acc1, from_far1,
                 loc, keep, os, orr, vs, vr, own_sem, *sems):
    here = Place()
    tp, core, chip, me, total = here.tp, here.core, here.chip, here.me, here.total
    local, ff = wo.shape[0], act.shape[2]
    swap = Exchange(here, both, met, landed, sems[0:4])
    gather = Gather(here, gown, gg, sems[4:8])
    settle0 = Owners(here, packed0, from_y0, acc0, from_far0, r0, sems[8:14])
    settle1 = Owners(here, packed1, from_y1, acc1, from_far1, r1, sems[14:20])
    kept = [(qkv_h, qkv), (prob_h, prob), (slope_h, slope), (act_h, act), (ctx_h, ctx)]
    rows_sent = rv.shape[2]
    vec_part = 13 * gown.shape[1] // total
    greet_all(here)
    gather.start(loc.at[0])
    settle1.start()
    loads = [pltpu.make_async_copy(a, b, keep.at[i]) for i, (a, b) in enumerate(kept)]
    for copy in loads:
        copy.start()

    def vec_copy(layer, source, step):
        other = lax.rem(me + step, total)
        first = (other * vec_part) // 128
        return remote(
            source.at[pl.ds(first, rows_sent)], rv.at[layer, me], vs.at[layer, step], vr.at[layer, step],
            here.device_of(other),
        )

    def own_vec(layer, vrows):
        first = (me * vec_part) // 128
        return pltpu.make_async_copy(vrows.at[pl.ds(first, rows_sent)], rv.at[layer, me], own_sem.at[layer])

    sender = here.far * here.ys + here.y

    def out_copy(layer, source, j):
        owner = tp * owners + j
        return remote(
            source.at[j], ro.at[layer, sender], os.at[layer, j], orr.at[layer, sender], here.device_of(owner)
        )

    def send(layer, out_grad, vrows):
        def start_all(step, carry):
            vec_copy(layer, vrows, step).start()
            return carry

        lax.fori_loop(1, total, start_all, 0)
        own_vec(layer, vrows).start()
        for j in range(owners):
            owner = tp * owners + j

            @pl.when(owner != me)
            def _():
                out_copy(layer, out_grad, j).start()

            @pl.when(owner == me)
            def _():
                pltpu.make_async_copy(out_grad.at[j], ro.at[layer, sender], orr.at[layer, sender]).start()

    def collect(layer, out_grad, vrows):
        def wait_all(step, carry):
            vec_copy(layer, vrows, step).wait()
            return carry

        lax.fori_loop(1, total, wait_all, 0)
        own_vec(layer, vrows).wait()
        for j in range(owners):
            owner = tp * owners + j

            @pl.when(owner != me)
            def _():
                out_copy(layer, out_grad, j).wait_send()

        for g in range(here.groups):
            pltpu.make_async_copy(out_grad.at[0], ro.at[layer, g], orr.at[layer, g]).wait()

    send(1, out_grad1, vrows1)
    sums[...] = jnp.zeros_like(sums)
    for copy in loads[:3]:
        copy.wait()

    def one(other, seq):
        mixed = [qkv[seq, :, i * local : (i + 1) * local] for i in range(3)]
        probs = [prob[seq, h] for h in range(local // head_dim)]
        back, mixed_grad, expanded_grad = seq_backward(
            work[other], mixed, probs, slope[seq], head_dim, w, wo, vec, rot
        )
        mixes[seq, :, : 3 * local] = mixed_grad
        mixes[seq, :, 3 * local :] = expanded_grad
        sums[:, : 3 * local] += fold_rows(mixed_grad)
        sums[:, 3 * local :] += fold_rows(expanded_grad)
        return back

    for n, k in enumerate(ORDER):
        if k:
            gather.wait_block(k)
            swap.hand_over(ORDER[n - 1])
            gather.wait_passed(k)
        else:
            gather.wait_partner()
        block = across(chip, k)
        gather.settle(k, work)

        def part_of(other, carry):
            both[other, k] = one(other, pick(core, other) * HALF + block).astype(BF)
            return carry

        lax.fori_loop(0, 2, part_of, 0)
        swap.to_partner(k).start()
        if n == 2:
            settle1.pass_far()
    for copy in loads[3:]:
        copy.wait()
    weight_grads(xg, gg, mixes, act, ctx, w, vec, sums, packed0, out_grad0, vrows0, gg[tp], tp)
    settle0.start()
    swap.hand_over(ORDER[-1])
    settle1.hand_out()
    send(0, out_grad0, vrows0)
    settle0.pass_far()
    swap.wait_landed()

    def finish_back(at):
        value = swap.total(at)
        centred, scale = norm_parts(tokens[at].astype(F32))
        xhat = centred * scale
        mean_one = jnp.mean(value, -1, keepdims=True)
        mean_two = jnp.mean(value * xhat, -1, keepdims=True)
        out[at] = (gg[tp, at].astype(F32) + scale * (value - mean_one - xhat * mean_two)).astype(BF)

    chunks(tokens.shape[0], finish_back)
    settle0.hand_out()
    gather.drain()
    swap.drain()
    collect(1, out_grad1, vrows1)
    collect(0, out_grad0, vrows0)
    settle1.drain()
    settle0.drain()


def third_layer(here, head_dim, gown, w, wo, vec, rot, tokens, xg, kept, packed1, out_grad1, vrows1):
    seqs, rows, width = xg.shape
    local = wo.shape[0]
    ff = (w.shape[1] - 3 * local) // 2
    mix = 3 * local + ff
    total, fars, ys = here.total, here.fars, here.ys
    owners, shard = out_grad1.shape[:2]
    dma = pltpu.SemaphoreType.DMA
    block = pltpu.VMEM((HALF, rows, width), BF)
    pair = pltpu.VMEM((2, HALF, rows, width), BF)
    unit = (HALF, 2, shard, w.shape[1])
    settle = [pltpu.VMEM(n + unit, BF) for n in ((ys - 1, fars), (fars,), (fars - 1,))]
    settle_sems = [dma((ys, fars, HALF))] * 2 + [dma((fars, HALF))] * 2 + [dma((HALF, 2)), dma((TP,))]
    sent = vector_rows(13 * width // total)
    owned = jax.ShapeDtypeStruct((TP, shard, w.shape[1]), BF)
    return pl.pallas_call(
        functools.partial(third_kernel, head_dim, owners),
        out_shape=[
            jax.ShapeDtypeStruct((rows, width), BF),
            owned,
            owned,
            jax.ShapeDtypeStruct((LAYERS, here.groups, shard, width), BF),
            jax.ShapeDtypeStruct((LAYERS, total, sent, 1, 128), F32),
        ],
        in_specs=[VMEM] * 8 + [ANY] * 7,
        out_specs=[VMEM] + [ANY] * 4,
        scratch_shapes=[
            pltpu.VMEM((seqs, rows, width), BF),
            pltpu.VMEM((2, rows, width), BF),
            pltpu.VMEM((seqs, rows, mix), BF),
            pltpu.VMEM((8, mix), F32),
        ]
        + [pltpu.VMEM(a.shape, BF) for a in kept]
        + [pltpu.VMEM(packed1.shape, BF), pltpu.VMEM(out_grad1.shape, BF), pltpu.VMEM(vrows1.shape, F32)]
        + [pair, block, block]
        + settle * 2
        + [
            dma((1,)), dma((5,)), dma((LAYERS, owners)), dma((LAYERS, here.groups)),
            dma((LAYERS, total)), dma((LAYERS, total)), dma((LAYERS,)),
        ]
        + [dma((HALF,))] * 8
        + settle_sems * 2,
        compiler_params=pltpu.CompilerParams(
            collective_id=4, has_side_effects=True, vmem_limit_bytes=VMEM_BYTES
        ),
        name="third_layer",
    )(gown, w, wo, vec, rot, tokens, xg, packed1, *kept, out_grad1, vrows1)


def adam_kernel(groups, local, ff, fixes, r0, r1, ro, *refs):
    params, moments, squares = refs[0:4], refs[4:8], refs[8:12]
    grads, changes, new_moments, new_squares = refs[12:16], refs[16:20], refs[20:24], refs[24:28]
    first_fix, second_fix = fixes[0], fixes[1]

    def update(which, at, gradient):
        moment = BETA_FIRST * moments[which][0, :, at] + (1.0 - BETA_FIRST) * gradient
        square = BETA_SECOND * squares[which][0, :, at] + (1.0 - BETA_SECOND) * gradient * gradient
        grads[which][0, :, at] = gradient
        new_moments[which][0, :, at] = moment
        new_squares[which][0, :, at] = square
        changes[which][0, :, at] = -LEARNING * (
            moment / first_fix / (jnp.sqrt(square / second_fix) + ADAM_EPSILON)
            + DECAY_RATE * params[which][0, :, at]
        )

    def layer(source):
        for p in range(TP):
            value = source[p].astype(F32)
            for i in range(3):
                start = i * TP * local + p * local
                update(0, slice(start, start + local), value[:, i * local : (i + 1) * local])
            split = 3 * local
            at = slice(p * ff, (p + 1) * ff)
            update(2, at, value[:, split : split + ff])
            update(3, at, value[:, split + ff :])
        value = ro[0, 0].astype(F32)
        for g in range(1, groups):
            value = value + ro[0, g].astype(F32)
        update(1, slice(None), value)

    @pl.when(pl.program_id(0) == 0)
    def _():
        layer(r0)

    @pl.when(pl.program_id(0) == 1)
    def _():
        layer(r1)


def adam_step(groups, local, ff, fixes, r0, r1, ro, params, moments, squares):
    shard = ro.shape[2]
    part = 8
    specs = [pl.BlockSpec((1, part, a.shape[2]), lambda l, r: (l, r, 0)) for a in params]
    source = lambda layer: pl.BlockSpec(
        (r0.shape[0], part, r0.shape[2]), lambda l, r: (0, jnp.where(l == layer, r, (1 - layer) * (shard // part - 1)), 0)
    )
    outs = [jax.ShapeDtypeStruct(a.shape, F32) for a in params]
    return pl.pallas_call(
        functools.partial(adam_kernel, groups, local, ff),
        grid=(LAYERS, shard // part),
        in_specs=[SMEM, source(0), source(1), pl.BlockSpec((1, groups, part, ro.shape[3]), lambda l, r: (l, 0, r, 0))]
        + specs * 3,
        out_specs=specs * 4,
        out_shape=outs * 4,
        compiler_params=pltpu.CompilerParams(vmem_limit_bytes=VMEM_BYTES),
        name="adam_step",
    )(fixes, r0, r1, ro, *params, *moments, *squares)


def rotary(row_count, width, head_dim):
    rot_dim = head_dim // 4
    half_rot = rot_dim // 2
    column = jnp.arange(width, dtype=jnp.int32) % head_dim
    freq_slot = (column % half_rot).astype(F32)
    frequency = 10000.0 ** (-(freq_slot * 2.0) / rot_dim)
    angles = jnp.arange(row_count, dtype=F32)[:, None] * frequency[None, :]
    inside = (column < rot_dim)[None, :]
    first_half = (column < half_rot)[None, :]
    sine = jnp.sin(angles)
    return jnp.stack(
        [
            jnp.where(inside, jnp.cos(angles), 1.0),
            jnp.where(first_half, -sine, 0.0),
            jnp.where(inside & jnp.logical_not(first_half), sine, 0.0),
        ]
    )


def standard(values):
    centred = values - jnp.mean(values, -1, keepdims=True)
    return centred * lax.rsqrt(jnp.mean(centred * centred, -1, keepdims=True) + NORM_EPSILON)


def adam_update(weight, moment, square, gradient, first_fix, second_fix):
    moment = BETA_FIRST * moment + (1.0 - BETA_FIRST) * gradient
    square = BETA_SECOND * square + (1.0 - BETA_SECOND) * gradient * gradient
    change = -LEARNING * (
        moment / first_fix / (jnp.sqrt(square / second_fix) + ADAM_EPSILON) + DECAY_RATE * weight
    )
    return (change, moment, square)


def per_device(tokens, cotangent, seq_lengths, seq_device, step_count, *state):
    params, moments, squares = state[0:5], state[5:10], state[10:15]
    attend_in, attend_out, expand_weight, reduce_weight, layer_vectors = params
    here = Place()
    tp, me, total, groups = here.tp, here.me, here.total, here.groups
    rows, width = tokens.shape
    shard = attend_in.shape[1]
    head_dim = width // HEADS
    local = width // TP
    ff = expand_weight.shape[2] // TP
    vec_part = layer_vectors.shape[1]
    owners = local // shard
    plane_ids = here.flat(here.far, here.y, jnp.arange(TP, dtype=jnp.int32))
    lens = jnp.sum(jnp.where(plane_ids[:, None] == seq_device[None, :], seq_lengths[None, :], 0), 1)
    lens = jnp.broadcast_to(lens[:, None, None], (TP, 1, rows))
    own_length = jnp.sum(jnp.where(seq_device == me, seq_lengths, 0))
    valid = jnp.arange(rows, dtype=jnp.int32)[:, None] < own_length
    rot = rotary(rows, local, head_dim)

    blocks = [
        jnp.concatenate(
            [
                attend_in[l].astype(BF).reshape(shard, 3, TP, local).transpose(2, 0, 1, 3).reshape(TP, shard, 3 * local),
                expand_weight[l].astype(BF).reshape(shard, TP, ff).transpose(1, 0, 2),
                reduce_weight[l].astype(BF).reshape(shard, TP, ff).transpose(1, 0, 2),
            ],
            2,
        )
        for l in range(LAYERS)
    ]
    vec = jnp.pad(layer_vectors.astype(BF).astype(F32).reshape(-1), (0, 8 * 128 - 2 * vec_part)).reshape(8, 128)
    xhat_own = standard(tokens.astype(F32)).astype(BF)
    grad_own = jnp.where(valid, cotangent, jnp.zeros_like(cotangent))
    xg, grads_all, w0, w1, wog, vecg = spread(
        here, xhat_own, grad_own, blocks[0], blocks[1], attend_out.astype(BF), vec
    )
    w0, w1 = w0.reshape(width, -1), w1.reshape(width, -1)
    out_rows = wog.transpose(1, 0, 2, 3).reshape(LAYERS, local, width)
    vectors = vecg.reshape(total, -1)[:, : 2 * vec_part].reshape(total, LAYERS, vec_part)
    vectors = vectors.transpose(1, 0, 2).reshape(LAYERS, 13, width)
    vectors = jnp.pad(vectors, ((0, 0), (0, 3), (0, 0)))

    hidden0, xnext, *kept = first_layer(
        head_dim, lens, xg, w0, out_rows[0], vectors[0], rot, tokens
    )
    hidden1, grad0, packed1, out_grad1, vrows1 = second_layer(
        here, head_dim, owners, shard, lens, xnext, grads_all, w1, out_rows[1], vectors[1], rot, hidden0
    )
    input_grad, r0, r1, ro, rv = third_layer(
        here, head_dim, grad0, w0, out_rows[0], vectors[0], rot, tokens, xg, kept, packed1, out_grad1, vrows1
    )
    step_float = step_count[0].astype(F32)
    first_fix = 1.0 - jnp.power(BETA_FIRST, step_float)
    second_fix = 1.0 - jnp.power(BETA_SECOND, step_float)
    big = adam_step(
        groups, local, ff, jnp.stack([first_fix, second_fix]), r0, r1, ro, params[:4], moments[:4], squares[:4]
    )
    vec_rows = jnp.sum(rv, 1).reshape(LAYERS, -1)
    grad_vec = lax.dynamic_slice_in_dim(vec_rows, lax.rem(me * vec_part, 128), vec_part, 1)
    small = (grad_vec,) + adam_update(params[4], moments[4], squares[4], grad_vec, first_fix, second_fix)
    results = []
    for i in range(4):
        results += list(big[4 * i : 4 * i + 4]) + [small[i]]
    return (jnp.stack([hidden0, hidden1]), input_grad, *results)


def solution(mesh):
    devices = mesh.devices.reshape(-1)
    blocks = devices.size // TP
    fars = 1 << ((blocks.bit_length()) // 2)
    flat = Mesh(devices.reshape(fars, 2, 2, blocks // fars, 2), AXES)
    by_row = P(AXES, None)
    by_dim = [P(None, AXES, None)] * 4 + [P(None, AXES)]
    return jax.shard_map(
        per_device,
        mesh=flat,
        in_specs=(by_row, by_row, P(), P(), P(), *(by_dim * 3)),
        out_specs=(P(None, AXES, None), by_row, *(by_dim * 4)),
        check_vma=False,
    )
```
